256 devices in a mesh: band: 8 (over z_lo, x), vis: 32 (over y, z_hi, core).
Axes of the slice: x: 4, y: 4, z: 8 (z_hi: 4, z_lo: 2; z = z_hi * 2 + z_lo), core: 2. Of those that a mesh axis runs over, the one named last changes fastest.
Arguments:
- sky_image: float32 [4096, 4096], P(('band', 'vis')), as said below
- coef_dual: float32 [4, 2048, 2048], P(None, ('band', 'vis')), may hold values from -12 to 12
- vis_dual: float32 [8, 32, 32, 4, 2, 32], P('band', 'vis'), may hold values from -12 to 12
- visibilities: float32 [8, 32, 32, 4, 2, 32], P('band', 'vis')
- kernel_blocks: bfloat16 [8, 32, 32, 4, 2, 32, 128], P('band', 'vis'), may hold values from -0.5 to 0.5
- tile_rows: int32 [8, 32, 32, 4], P('band', 'vis'), may hold values from 0 to 511
- tile_counts: int32 [8, 32, 32], P('band', 'vis'), may hold values from 1 to 4, as said below
Outputs:
- new_image: float32 [4096, 4096], P(('band', 'vis'))
- new_coef_dual: float32 [4, 2048, 2048], P(None, ('band', 'vis'))
- new_vis_dual: float32 [8, 32, 32, 4, 2, 32], P('band', 'vis')
The draws below stay inside these ranges and needn't reach their ends.
Inputs may be any that keep to these rules, and one draw needn't show every extreme that they name: `sky_image`: nonnegative. `tile_counts`: in every band some owner q has all 4 slots live from every device of that band.
All inputs are finite; a program needn't handle non-finite values.
Results may differ from the reference program's by a relative error of at most 0.0018.
Values may be sent and summed in bfloat16 or wider, within the bound.
A program may use at most 64 MiB of HBM per device.

```python
import jax
import jax.numpy as jnp
from jax import lax

IMG = 4096
VT = 32
SLOTS = 4
ITERS = 1
STRIPE = 512
PIECE_ROWS = 128
HALF = 2048
N_BAND = 8
N_VIS = 32


def draw_sky_image(key, part):
    row_key, col_key, base_key = jax.random.split(key, 3)
    row_scale = jnp.exp(jax.random.uniform(row_key, (IMG, 1), jnp.float32) * jnp.log(10.0))
    col_scale = jnp.exp(jax.random.uniform(col_key, (1, IMG), jnp.float32) * jnp.log(10.0))
    rising = 1.0 + 2.0 * jnp.arange(IMG, dtype=jnp.float32)[:, None] / IMG
    base_values = jax.random.uniform(base_key, (IMG, IMG), jnp.float32)
    return 0.2 * base_values * row_scale * col_scale * rising


def draw_visibilities(key, part):
    full_shape = (N_BAND, N_VIS, N_VIS, SLOTS, 2, VT)
    scale_key, value_key = jax.random.split(key)
    tile_scale = jnp.exp(jax.random.uniform(scale_key, (N_BAND, N_VIS, N_VIS, SLOTS, 1, 1), jnp.float32) * jnp.log(10.0))
    position = (jnp.arange(N_BAND * N_VIS, dtype=jnp.float32) / (N_BAND * N_VIS - 1)).reshape(N_BAND, N_VIS, 1, 1, 1, 1)
    values = jax.random.normal(value_key, full_shape, jnp.float32)
    rising = 1.0 + 2.0 * position
    return values * tile_scale * rising


def draw_tile_counts(key, part):
    count_key, owner_key = jax.random.split(jax.random.fold_in(key, 11))
    counts = jax.random.randint(count_key, (N_BAND, N_VIS, N_VIS), 1, SLOTS + 1)
    full_owner = jax.random.randint(owner_key, (N_BAND, 1, 1), 0, N_VIS)
    owners = jnp.arange(N_VIS, dtype=jnp.int32)[None, None, :]
    return jnp.where(owners == full_owner, SLOTS, counts).astype(jnp.int32)


def plant(values, key, low, largest):
    extent = values.shape
    spot = [jax.random.randint(jax.random.fold_in(key, axis), (), 0, extent[axis]) for axis in range(len(extent))]
    values = values.at[tuple(spot)].set(low)
    longest = extent.index(max(extent))
    spot[longest] = (spot[longest] + 1) % extent[longest]
    return values.at[tuple(spot)].set(largest)


def block_levels(rng, shape, cuts, least, largest):
    loudness, own = 1.0, jax.random.fold_in(rng, 6)
    for dim, shards_of in cuts:
        heights = jnp.exp(jax.random.uniform(jax.random.fold_in(own, dim), (shards_of,), jnp.float32, least / len(cuts), largest / len(cuts)))
        loudness = loudness * jnp.repeat(heights, shape[dim] // shards_of).reshape([-1 if axis == dim else 1 for axis in range(len(shape))])
    return loudness


def centred(own_key, extent, width, limit, cuts=(), held_as=jnp.bfloat16):
    entries = width * jax.random.normal(own_key, extent, jnp.float32)
    if cuts:
        entries = entries * block_levels(own_key, extent, cuts, -0.22, 0.18)
    return jnp.clip(entries, -limit, limit).astype(held_as)


def setup_inputs(seed: int = 0) -> dict:
    splits = jax.random.split(jax.random.key(seed), 8)
    sky_image = draw_sky_image(jax.random.fold_in(splits[7], 71), 0)
    coef_dual = centred(splits[1], (4, HALF, HALF), 2.0, 12.0, ((1, 256),), jnp.float32)
    vis_dual = centred(splits[2], (N_BAND, N_VIS, N_VIS, SLOTS, 2, VT), 2.0, 12.0, ((0, 8), (1, 32)), jnp.float32)
    visibilities = draw_visibilities(jax.random.fold_in(splits[7], 71), 0)
    kernel_blocks = centred(splits[4], (N_BAND, N_VIS, N_VIS, SLOTS, 2, VT, PIECE_ROWS), PIECE_ROWS ** -0.5, 0.5, ((0, 8), (1, 32)))
    tile_rows = plant(jax.random.randint(splits[5], (N_BAND, N_VIS, N_VIS, SLOTS), 0, STRIPE), jax.random.fold_in(splits[5], 1), 0, STRIPE - 1).astype(jnp.int32)
    tile_counts = draw_tile_counts(jax.random.fold_in(splits[7], 71), 0)
    return dict(sky_image=sky_image, coef_dual=coef_dual, vis_dual=vis_dual, visibilities=visibilities, kernel_blocks=kernel_blocks, tile_rows=tile_rows, tile_counts=tile_counts)


low_taps = (-0.010597401784997278, 0.032883011666982945, 0.030841381835986965, -0.18703481171888114, -0.02798376941698385, 0.6308807679295904, 0.7148465705525415, 0.23037781330885523)
high_taps = tuple(((-1.0) ** offset * low_taps[7 - offset] for offset in range(8)))
highest = lax.Precision.HIGHEST

def analyse_axis(field, axis):
    length = field.shape[axis]
    low_part = 0.0
    high_part = 0.0
    for offset in range(8):
        taken = lax.slice_in_dim(jnp.roll(field, -offset, axis=axis), 0, length, 2, axis)
        low_part = low_part + low_taps[offset] * taken
        high_part = high_part + high_taps[offset] * taken
    return (low_part, high_part)

def synthesise_axis(low_part, high_part, axis):
    halves = []
    for parity in range(2):
        summed = 0.0
        for delay in range(4):
            summed = summed + low_taps[parity + 2 * delay] * jnp.roll(low_part, delay, axis=axis)
            summed = summed + high_taps[parity + 2 * delay] * jnp.roll(high_part, delay, axis=axis)
        halves.append(summed)
    joined = jnp.stack(halves, axis=axis + 1)
    new_shape = list(low_part.shape)
    new_shape[axis] = 2 * new_shape[axis]
    return joined.reshape(new_shape)

def analysis(field):
    rows_low, rows_high = analyse_axis(field, 0)
    low_low, low_high = analyse_axis(rows_low, 1)
    high_low, high_high = analyse_axis(rows_high, 1)
    return jnp.stack([low_low, low_high, high_low, high_high])

def synthesis(coeffs):
    rows_low = synthesise_axis(coeffs[0], coeffs[1], 1)
    rows_high = synthesise_axis(coeffs[2], coeffs[3], 1)
    return synthesise_axis(rows_low, rows_high, 0)

def forward_map(extrap, kernel_blocks, tile_rows):
    spectrum = jnp.fft.fft2(extrap) / IMG
    flipped = spectrum.T.reshape(N_BAND, STRIPE, N_VIS, PIECE_ROWS)
    real_grid = lax.optimization_barrier(jnp.real(flipped).astype(jnp.bfloat16))
    imag_grid = lax.optimization_barrier(jnp.imag(flipped).astype(jnp.bfloat16))
    owners = jnp.arange(N_VIS, dtype=jnp.int32)[None, :, None]

    def per_band(inputs):
        kernels, rows_band, real_band, imag_band = inputs
        tile_real = real_band[rows_band, owners].astype(jnp.float32)
        tile_imag = imag_band[rows_band, owners].astype(jnp.float32)
        kernel_real = kernels[:, :, :, 0].astype(jnp.float32)
        kernel_imag = kernels[:, :, :, 1].astype(jnp.float32)
        out_real = jnp.einsum('vqsat,vqst->vqsa', kernel_real, tile_real, precision=highest) - jnp.einsum('vqsat,vqst->vqsa', kernel_imag, tile_imag, precision=highest)
        out_imag = jnp.einsum('vqsat,vqst->vqsa', kernel_real, tile_imag, precision=highest) + jnp.einsum('vqsat,vqst->vqsa', kernel_imag, tile_real, precision=highest)
        return jnp.stack([out_real, out_imag], axis=3)
    return lax.map(per_band, (kernel_blocks, tile_rows, real_grid, imag_grid))

def adjoint_map(weights, kernel_blocks, tile_rows):
    rounded = lax.optimization_barrier(weights.astype(jnp.bfloat16))
    owners = jnp.arange(N_VIS, dtype=jnp.int32)[None, :, None]

    def per_band(inputs):
        kernels, rows_band, vis_band = inputs
        kernel_real = kernels[:, :, :, 0].astype(jnp.float32)
        kernel_imag = kernels[:, :, :, 1].astype(jnp.float32)
        weight_real = vis_band[:, :, :, 0].astype(jnp.float32)
        weight_imag = vis_band[:, :, :, 1].astype(jnp.float32)
        grid_real = jnp.einsum('vqsat,vqsa->vqst', kernel_real, weight_real, precision=highest) + jnp.einsum('vqsat,vqsa->vqst', kernel_imag, weight_imag, precision=highest)
        grid_imag = jnp.einsum('vqsat,vqsa->vqst', kernel_real, weight_imag, precision=highest) - jnp.einsum('vqsat,vqsa->vqst', kernel_imag, weight_real, precision=highest)
        stacked = jnp.stack([grid_real, grid_imag], axis=3)
        segment = (owners * STRIPE + rows_band).astype(jnp.int32)
        summed = jax.ops.segment_sum(stacked.reshape(-1, 2, PIECE_ROWS), segment.reshape(-1), num_segments=N_VIS * STRIPE)
        return summed.reshape(N_VIS, STRIPE, 2, PIECE_ROWS)
    grids = lax.map(per_band, (kernel_blocks, tile_rows, rounded))
    ordered = jnp.transpose(grids, (3, 1, 4, 0, 2)).reshape(2, IMG, IMG)
    spectrum = lax.complex(ordered[0], ordered[1])
    return jnp.real(jnp.fft.ifft2(spectrum)) * IMG

def reference(sky_image, coef_dual, vis_dual, visibilities, kernel_blocks, tile_rows, tile_counts):
    slot_index = jnp.arange(SLOTS, dtype=jnp.int32)
    live_slots = (slot_index < tile_counts[..., None]).astype(jnp.float32)[..., None, None]
    data_square = jnp.sum(live_slots * visibilities * visibilities)
    radius = 0.5 * jnp.sqrt(data_square + 1e-06)
    for iteration in range(ITERS):
        adjoint_part = adjoint_map(live_slots * vis_dual, kernel_blocks, tile_rows)
        smooth = synthesis(coef_dual)
        new_image = jnp.maximum(sky_image - smooth - adjoint_part, 0.0)
        extrap = 2.0 * new_image - sky_image
        coeffs = analysis(extrap)
        threshold = 0.5 * jnp.sum(jnp.abs(coeffs)) / (IMG * IMG)
        coef_dual = jnp.clip(coef_dual + coeffs, -threshold, threshold)
        predicted = forward_map(extrap, kernel_blocks, tile_rows)
        residual = live_slots * (vis_dual + predicted - visibilities)
        size_value = jnp.sqrt(jnp.sum(residual * residual) + 1e-06)
        vis_dual = residual * (1.0 - jnp.minimum(1.0, radius / size_value))
        sky_image = new_image
    return (sky_image, coef_dual, vis_dual)
```

```python
import functools
import math

import jax
import jax.numpy as jnp
import numpy as np
from jax import lax
from jax.experimental import pallas as pl
from jax.experimental.pallas import tpu as pltpu
from jax.sharding import PartitionSpec as P

IMG = 4096
NB = 8
NV = 32
MESH_ID = pl.DeviceIdType.MESH
highest = lax.Precision.HIGHEST
f32 = jnp.float32
bf16 = jnp.bfloat16

low_taps = (
    -0.010597401784997278,
    0.032883011666982945,
    0.030841381835986965,
    -0.18703481171888114,
    -0.02798376941698385,
    0.6308807679295904,
    0.7148465705525415,
    0.23037781330885523,
)
high_taps = tuple(((-1.0) ** offset * low_taps[7 - offset] for offset in range(8)))


def halves_of(table):
    high = table.astype(bf16)
    low = (table - high.astype(np.float64)).astype(bf16)
    return high, low


def dft512_tables():
    index = np.arange(512)
    angle = 2.0 * np.pi / 512 * (index[:, None] * index[None, :] % 512)
    return halves_of(np.concatenate([np.cos(angle), np.sin(angle)], axis=0))


def dft128_table():
    index = np.arange(128)
    angle = 2.0 * np.pi / 128 * (index[:, None] * index[None, :] % 128)
    return (np.concatenate([np.cos(angle), np.sin(angle)], axis=1) / IMG).astype(np.float32)


def row_twist():
    angle = 2.0 * np.pi / IMG * (np.arange(32)[:, None] * np.arange(128)[None, :] % IMG)
    return np.stack([np.cos(angle), np.sin(angle)], axis=1).astype(np.float32)


def lane_order():
    place = np.zeros((128, 128), np.float32)
    for t in range(128):
        place[(t % 8) * 16 + t // 8, t] = 1.0
    return place.astype(bf16)


def times(pair, cosine, sine):
    re, im = pair
    if abs(sine) < 1e-12:
        if cosine > 0:
            return pair
        return (-re, None if im is None else -im)
    if abs(cosine) < 1e-12:
        if im is None:
            return (None, re if sine > 0 else -re)
        return (-im, re) if sine > 0 else (im, -re)
    cosine, sine = np.float32(cosine), np.float32(sine)
    if im is None:
        return (re * cosine, re * sine)
    return (re * cosine - im * sine, re * sine + im * cosine)


def plus(a, b):
    if a is None:
        return b
    return a if b is None else a + b


def minus(a, b):
    if b is None:
        return a
    return -b if a is None else a - b


def small_dft(values, sign):
    count = len(values)
    if count == 1:
        return values
    even = small_dft(values[0::2], sign)
    odd = small_dft(values[1::2], sign)
    out = [None] * count
    for k in range(count // 2):
        angle = sign * 2.0 * math.pi * k / count
        turned = times(odd[k], math.cos(angle), math.sin(angle))
        out[k] = (plus(even[k][0], turned[0]), plus(even[k][1], turned[1]))
        out[k + count // 2] = (minus(even[k][0], turned[0]), minus(even[k][1], turned[1]))
    return out


def swap_groups(arrays):
    arrays = list(arrays)
    lane = lax.broadcasted_iota(jnp.int32, arrays[0].shape, arrays[0].ndim - 1)
    axis = arrays[0].ndim - 1
    for bit in range(3):
        shift = 16 << bit
        upper = (lane // shift) % 2 == 1
        for j in range(8):
            other = j | (1 << bit)
            if other == j:
                continue
            low, high = arrays[j], arrays[other]
            arrays[j] = jnp.where(upper, pltpu.roll(high, shift, axis), low)
            arrays[other] = jnp.where(upper, high, pltpu.roll(low, 128 - shift, axis))
    return arrays


def greet(vis_me, band_me):
    barrier = pltpu.get_barrier_semaphore()

    def vis_signal(d, carry):
        pl.semaphore_signal(
            barrier, inc=1, device_id={"vis": vis_me ^ d}, device_id_type=MESH_ID
        )
        return carry

    def band_signal(d, carry):
        pl.semaphore_signal(
            barrier, inc=1, device_id={"band": band_me ^ d}, device_id_type=MESH_ID
        )
        return carry

    lax.fori_loop(1, NV, vis_signal, 0)
    lax.fori_loop(1, NB, band_signal, 0)
    return barrier


def launch(sent, landed, sems, axis, count, me):
    def body(d, carry):
        peer = me ^ d
        pltpu.make_async_remote_copy(
            src_ref=sent.at[peer],
            dst_ref=landed.at[me],
            send_sem=sems.at[0],
            recv_sem=sems.at[1],
            device_id={axis: peer},
            device_id_type=MESH_ID,
        ).start()
        return carry

    lax.fori_loop(1, count, body, 0)
    landed[me] = sent[me]


def arrived(landed, sems, count):
    part = landed.at[pl.ds(0, count - 1)]
    pltpu.make_async_copy(part, part, sems.at[1]).wait()


def drained(sent, sems, count):
    part = sent.at[pl.ds(0, count - 1)]
    pltpu.make_async_copy(part, part, sems.at[0]).wait()


def adjoint_kernel(
    weights, places, kernels, table_hi, table_lo, table128, twist_row, twist_col, order,
    image, onehot,
    sent_a, got_a, sent_b, got_b, sent_c, got_c, sent_d, got_d, mid,
    sem_a, sem_b, sem_c, sem_d,
):
    vis_me, band_me = lax.axis_index("vis"), lax.axis_index("band")
    barrier = greet(vis_me, band_me)
    for q in range(NV):
        part = jnp.dot(weights[q], kernels[q], preferred_element_type=f32)
        sent_a[q] = jnp.concatenate([part, places[q]], axis=0).astype(bf16)
    pl.semaphore_wait(barrier, NV + NB - 2)
    launch(sent_a, got_a, sem_a, "vis", NV, vis_me)
    arrived(got_a, sem_a, NV)

    contrib = got_a[:, 0:8, :].astype(f32).reshape(256, 128).astype(bf16)
    where_to = got_a[:, 8:16, :].astype(f32).reshape(256, 128)
    lane = lax.broadcasted_iota(jnp.int32, (256, 128), 1).astype(f32)
    is_imag = lax.broadcasted_iota(jnp.int32, (256, 128), 0) % 2 == 1
    hots = [(where_to == lane + float(128 * g - 256)).astype(f32) for g in range(4)]
    for g in range(4):
        onehot[:, 128 * g : 128 * g + 128] = hots[g].astype(bf16)
    real_hots = [jnp.where(is_imag, 0.0, h).astype(bf16) for h in hots]
    imag_hots = [jnp.where(is_imag, h, 0.0).astype(bf16) for h in hots]
    turned = lax.dot_general(
        order[...], contrib, (((1,), (1,)), ((), ())), preferred_element_type=f32
    ).astype(bf16)
    for c, some in ((0, real_hots), (1, imag_hots)):
        for g in range(4):
            grid = jnp.dot(turned, some[g], preferred_element_type=f32).astype(bf16)
            for low in range(8):
                sent_b[low * 4 + g, c] = grid[16 * low : 16 * low + 16]
    launch(sent_b, got_b, sem_b, "vis", NV, vis_me)
    arrived(got_b, sem_b, NV)

    spread = jnp.concatenate(
        [got_b[:, 0].reshape(512, 128), got_b[:, 1].reshape(512, 128)], axis=1
    )
    both = jnp.dot(table_hi[...], spread, preferred_element_type=f32)
    both = both + jnp.dot(table_lo[...], spread, preferred_element_type=f32)
    sent_c[:, 0] = (both[:512, :128] - both[512:, 128:]).astype(bf16).reshape(NV, 16, 128)
    sent_c[:, 1] = (both[512:, :128] + both[:512, 128:]).astype(bf16).reshape(NV, 16, 128)
    launch(sent_c, got_c, sem_c, "vis", NV, vis_me)
    arrived(got_c, sem_c, NV)

    for g in range(4):
        values = []
        for low in range(8):
            re = got_c[low * 4 + g, 0].astype(f32)
            im = got_c[low * 4 + g, 1].astype(f32)
            cosine, sine = twist_col[low, 0], twist_col[low, 1]
            values.append((re * cosine - im * sine, re * sine + im * cosine))
        values = small_dft(values, 1.0)
        for b in range(NB):
            for c in range(2):
                sent_d[b, c, :, 128 * g : 128 * g + 128] = values[b][c].astype(sent_d.dtype)
    launch(sent_d, got_d, sem_d, "band", NB, band_me)
    arrived(got_d, sem_d, NB)

    for g in range(4):
        for c in range(2):
            parts = swap_groups(
                [got_d[b, c, :, 128 * g : 128 * g + 128].astype(f32) for b in range(NB)]
            )
            for a in range(8):
                mid[g * 8 + a, c] = parts[a]
    lanes = jnp.dot(
        mid[...].reshape(1024, 128), table128[...], precision=highest, preferred_element_type=f32
    ).reshape(32, 2, 16, 256)
    for half in range(2):
        rows = slice(8 * half, 8 * half + 8)
        values = []
        for a in range(32):
            re = lanes[a, 0, rows, :128] - lanes[a, 1, rows, 128:]
            im = lanes[a, 0, rows, 128:] + lanes[a, 1, rows, :128]
            cosine, sine = twist_row[a, 0:1], twist_row[a, 1:2]
            values.append((re * cosine - im * sine, re * sine + im * cosine))
        values = small_dft(values, 1.0)
        for n in range(32):
            image[rows, 128 * n : 128 * n + 128] = values[n][0]

    drained(sent_a, sem_a, NV)
    drained(sent_b, sem_b, NV)
    drained(sent_c, sem_c, NV)
    drained(sent_d, sem_d, NB)


def forward_kernel(
    image, onehot, kernels, table_hi, table_lo, table128, twist_row, twist_col, order,
    predicted,
    mid, sent_a, got_a, sent_b, got_b, sent_c, got_c, sent_d, got_d,
    sem_a, sem_b, sem_c, sem_d,
):
    vis_me, band_me = lax.axis_index("vis"), lax.axis_index("band")
    barrier = greet(vis_me, band_me)
    for half in range(2):
        rows = slice(8 * half, 8 * half + 8)
        values = [(image[rows, 128 * n : 128 * n + 128], None) for n in range(32)]
        values = small_dft(values, -1.0)
        for a in range(32):
            re, im = values[a]
            cosine, sine = twist_row[a, 0:1], twist_row[a, 1:2]
            if im is None:
                mid[a, 0, rows] = re * cosine
                mid[a, 1, rows] = -re * sine
            else:
                mid[a, 0, rows] = re * cosine + im * sine
                mid[a, 1, rows] = im * cosine - re * sine
    lanes = jnp.dot(
        mid[...].reshape(1024, 128), table128[...], precision=highest, preferred_element_type=f32
    ).reshape(32, 2, 16, 256)
    for g in range(4):
        for c in range(2):
            parts = []
            for a in range(8):
                re, im = lanes[g * 8 + a, 0], lanes[g * 8 + a, 1]
                if c == 0:
                    parts.append(re[:, :128] + im[:, 128:])
                else:
                    parts.append(im[:, :128] - re[:, 128:])
            parts = swap_groups(parts)
            for b in range(NB):
                sent_a[b, c, :, 128 * g : 128 * g + 128] = parts[b].astype(sent_a.dtype)
    pl.semaphore_wait(barrier, NV + NB - 2)
    launch(sent_a, got_a, sem_a, "band", NB, band_me)
    arrived(got_a, sem_a, NB)

    for g in range(4):
        values = []
        for b in range(NB):
            values.append(
                tuple(
                    got_a[b, c, :, 128 * g : 128 * g + 128].astype(f32) for c in range(2)
                )
            )
        values = small_dft(values, -1.0)
        for low in range(8):
            re, im = values[low]
            cosine, sine = twist_col[low, 0], twist_col[low, 1]
            sent_b[low * 4 + g, 0] = (re * cosine + im * sine).astype(sent_b.dtype)
            sent_b[low * 4 + g, 1] = (im * cosine - re * sine).astype(sent_b.dtype)
    launch(sent_b, got_b, sem_b, "vis", NV, vis_me)
    arrived(got_b, sem_b, NV)

    spread = jnp.concatenate(
        [got_b[:, 0].reshape(512, 128), got_b[:, 1].reshape(512, 128)], axis=1
    )
    high = spread.astype(bf16)
    both = jnp.dot(table_hi[...], high, preferred_element_type=f32)
    both = both + jnp.dot(table_lo[...], high, preferred_element_type=f32)
    if spread.dtype == f32:
        low_part = (spread - high.astype(f32)).astype(bf16)
        both = both + jnp.dot(table_hi[...], low_part, preferred_element_type=f32)
    sent_c[:, 0] = (both[:512, :128] + both[512:, 128:]).astype(bf16).reshape(NV, 16, 128)
    sent_c[:, 1] = (both[:512, 128:] - both[512:, :128]).astype(bf16).reshape(NV, 16, 128)
    launch(sent_c, got_c, sem_c, "vis", NV, vis_me)
    arrived(got_c, sem_c, NV)

    picked = []
    for c in range(2):
        total = 0.0
        for g in range(4):
            piece = jnp.concatenate([got_c[low * 4 + g, c] for low in range(8)], axis=0)
            total = total + lax.dot_general(
                onehot[:, 128 * g : 128 * g + 128],
                piece,
                (((1,), (1,)), ((), ())),
                preferred_element_type=f32,
            )
        picked.append(total)
    is_imag = lax.broadcasted_iota(jnp.int32, (256, 128), 0) % 2 == 1
    tiles = jnp.where(is_imag, picked[1], picked[0]).astype(bf16)
    tiles = jnp.dot(tiles, order[...], preferred_element_type=f32)
    sent_d[...] = tiles.reshape(NV, 8, 128).astype(bf16)
    launch(sent_d, got_d, sem_d, "vis", NV, vis_me)
    arrived(got_d, sem_d, NV)

    row = lax.broadcasted_iota(jnp.int32, (8, 256), 0)
    slot = lax.broadcasted_iota(jnp.int32, (8, 256), 1) // 64
    on_real = row == 2 * slot
    on_imag = row == 2 * slot + 1
    from_real, from_imag = [], []
    for q in range(NV):
        product = lax.dot_general(
            got_d[q], kernels[q], (((1,), (1,)), ((), ())), preferred_element_type=f32
        )
        from_real.append(jnp.sum(jnp.where(on_real, product, 0.0), axis=0, keepdims=True))
        from_imag.append(jnp.sum(jnp.where(on_imag, product, 0.0), axis=0, keepdims=True))
    from_real = jnp.concatenate(from_real, axis=0)
    from_imag = jnp.concatenate(from_imag, axis=0)
    imag_lane = (lax.broadcasted_iota(jnp.int32, (NV, 256), 1) // 32) % 2 == 1
    predicted[...] = from_real + jnp.where(
        imag_lane, pltpu.roll(from_imag, 32, 1), -pltpu.roll(from_imag, 256 - 32, 1)
    )

    drained(sent_a, sem_a, NB)
    drained(sent_b, sem_b, NV)
    drained(sent_c, sem_c, NV)
    drained(sent_d, sem_d, NV)


VM = pl.BlockSpec(memory_space=pltpu.VMEM)


def call(kernel, inputs, outs, scratch, collective_id):
    return pl.pallas_call(
        kernel,
        out_shape=outs,
        in_specs=[VM] * len(inputs),
        out_specs=tuple([VM] * len(outs)),
        scratch_shapes=scratch,
        compiler_params=pltpu.CompilerParams(
            collective_id=collective_id, has_side_effects=True, vmem_limit_bytes=48 * 2**20
        ),
    )(*inputs)


def pair(shape, dtype):
    return [pltpu.VMEM(shape, dtype), pltpu.VMEM(shape, dtype)]


def adjoint_map(weights, places, kernels, tables):
    vis_tile = (NV, 2, 16, 128)
    scratch = (
        pair((NV, 16, 128), bf16)
        + pair(vis_tile, bf16)
        + pair(vis_tile, bf16)
        + pair((NB, 2, 16, 512), bf16)
        + [pltpu.VMEM((32, 2, 16, 128), f32)]
        + [pltpu.SemaphoreType.DMA((2,))] * 4
    )
    outs = (
        jax.ShapeDtypeStruct((16, IMG), f32),
        jax.ShapeDtypeStruct((256, 512), bf16),
    )
    return call(adjoint_kernel, (weights, places, kernels) + tables, outs, scratch, 0)


def forward_map(image, onehot, kernels, tables):
    vis_tile = (NV, 2, 16, 128)
    scratch = (
        [pltpu.VMEM((32, 2, 16, 128), f32)]
        + pair((NB, 2, 16, 512), f32)
        + pair(vis_tile, f32)
        + pair(vis_tile, bf16)
        + pair((NV, 8, 128), bf16)
        + [pltpu.SemaphoreType.DMA((2,))] * 4
    )
    outs = (jax.ShapeDtypeStruct((NV, 256), f32),)
    return call(forward_kernel, (image, onehot, kernels) + tables, outs, scratch, 1)[0]


def shifted(block, axis, distance):
    devices = range(lax.axis_size(axis))
    route = [((i - distance) % len(devices), i) for i in devices]
    return lax.ppermute(block, axis, route)


def cols_down(field):
    image_width = field.shape[1]
    extended = jnp.concatenate([field, field[:, :6]], axis=1)
    low_part = 0.0
    high_part = 0.0
    for offset in range(8):
        taken = extended[:, offset : offset + image_width : 2]
        low_part = low_part + low_taps[offset] * taken
        high_part = high_part + high_taps[offset] * taken
    return (low_part, high_part)


def cols_up(low_part, high_part):
    halves = []
    for parity in range(2):
        summed = 0.0
        for delay in range(4):
            summed = summed + low_taps[parity + 2 * delay] * jnp.roll(low_part, delay, axis=1)
            summed = summed + high_taps[parity + 2 * delay] * jnp.roll(high_part, delay, axis=1)
        halves.append(summed)
    return jnp.stack(halves, axis=2).reshape(low_part.shape[0], 2 * low_part.shape[1])


def rows_up(low_ext, high_ext, half_rows):
    halves = []
    for parity in range(2):
        summed = 0.0
        for delay in range(4):
            begin = 3 - delay
            summed = summed + low_taps[parity + 2 * delay] * low_ext[begin : begin + half_rows]
            summed = summed + high_taps[parity + 2 * delay] * high_ext[begin : begin + half_rows]
        halves.append(summed)
    return jnp.stack(halves, axis=1).reshape(2 * half_rows, low_ext.shape[1])


def analysis(extrap):
    rows_dev = extrap.shape[0]
    extended = jnp.concatenate([extrap, shifted(extrap[:6], ("band", "vis"), -1)], axis=0)
    half_rows = rows_dev // 2
    rows_low = 0.0
    rows_high = 0.0
    for offset in range(8):
        taken = extended[offset : offset + 2 * half_rows : 2]
        rows_low = rows_low + low_taps[offset] * taken
        rows_high = rows_high + high_taps[offset] * taken
    low_low, low_high = cols_down(rows_low)
    high_low, high_high = cols_down(rows_high)
    return jnp.stack([low_low, low_high, high_low, high_high])


def synthesis(coef_dual):
    half_rows = coef_dual.shape[1]
    halo = shifted(coef_dual[:, half_rows - 3 :, :], ("band", "vis"), 1)
    joined = jnp.concatenate([halo, coef_dual], axis=1)
    cols_low = rows_up(joined[0], joined[2], half_rows)
    cols_high = rows_up(joined[1], joined[3], half_rows)
    return cols_up(cols_low, cols_high)


def local(sky_image, coef_dual, vis_dual, visibilities, kernel_blocks, tile_rows, tile_counts):
    kernels = kernel_blocks.reshape(NV, 256, 128)
    rows_here = tile_rows.reshape(NV, 4)
    counts = tile_counts.reshape(NV, 1)
    live = (jnp.arange(256, dtype=jnp.int32)[None, :] // 64 < counts).astype(f32)
    vis_data = visibilities.reshape(NV, 256)
    vis_state = vis_dual.reshape(NV, 256)

    wb = live * vis_state
    lane = jnp.arange(256, dtype=jnp.int32)
    imag_lane = (lane // 32) % 2 == 1
    crossed = jnp.where(imag_lane, -jnp.roll(wb, 32, axis=1), jnp.roll(wb, -32, axis=1))
    slot_row = jnp.arange(8, dtype=jnp.int32)
    same = (slot_row[:, None] // 2 == lane[None, :] // 64)[None]
    chosen = jnp.where((slot_row % 2 == 1)[None, :, None], crossed[:, None, :], wb[:, None, :])
    weights = jnp.where(same, chosen, 0.0).astype(bf16)

    place = (rows_here % 32) * 16 + rows_here // 32 - 256
    places = jnp.broadcast_to(
        jnp.repeat(place.astype(f32), 2, axis=1)[:, :, None], (NV, 8, 128)
    )

    low = jnp.arange(8, dtype=jnp.int32)[:, None]
    mu = lax.axis_index("vis") * 16 + jnp.arange(16, dtype=jnp.int32)[None, :]
    angle = (2.0 * math.pi / IMG) * (low * mu).astype(f32)
    twist_col = jnp.broadcast_to(
        jnp.stack([jnp.cos(angle), jnp.sin(angle)], axis=1)[..., None], (8, 2, 16, 128)
    )
    table_hi, table_lo = dft512_tables()
    tables = (
        jnp.asarray(table_hi),
        jnp.asarray(table_lo),
        jnp.asarray(dft128_table()),
        jnp.asarray(row_twist()),
        twist_col,
        jnp.asarray(lane_order()),
    )

    data_part = jnp.sum(live * vis_data * vis_data)
    adjoint_part, onehot = adjoint_map(weights, places, kernels, tables)
    smooth = synthesis(coef_dual)
    new_image = jnp.maximum(sky_image - smooth - adjoint_part, 0.0)
    extrap = 2.0 * new_image - sky_image
    coeffs = analysis(extrap)
    abs_total = jnp.sum(jnp.abs(coeffs))
    predicted = forward_map(extrap, onehot, kernels, tables)
    residual = live * (vis_state + predicted - vis_data)
    resid_square = jnp.sum(residual * residual)
    totals = lax.psum(jnp.stack([abs_total, resid_square, data_part]), ("band", "vis"))
    threshold = 0.5 * totals[0] / (IMG * IMG)
    coef_dual = jnp.clip(coef_dual + coeffs, -threshold, threshold)
    radius = 0.5 * jnp.sqrt(totals[2] + 1e-06)
    size_value = jnp.sqrt(totals[1] + 1e-06)
    vis_state = residual * (1.0 - jnp.minimum(1.0, radius / size_value))
    return (new_image, coef_dual, vis_state.reshape(1, 1, NV, 4, 2, 32))


def solution(mesh):
    return jax.shard_map(
        local,
        mesh=mesh,
        in_specs=(
            P(("band", "vis"), None),
            P(None, ("band", "vis"), None),
            P("band", "vis", None, None, None, None),
            P("band", "vis", None, None, None, None),
            P("band", "vis", None, None, None, None, None),
            P("band", "vis", None, None),
            P("band", "vis", None),
        ),
        out_specs=(
            P(("band", "vis"), None),
            P(None, ("band", "vis"), None),
            P("band", "vis", None, None, None, None),
        ),
        check_vma=False,
    )
```

```python
import functools
import math

import jax
import jax.numpy as jnp
import numpy as np
from jax import lax
from jax.experimental import pallas as pl
from jax.experimental.pallas import tpu as pltpu
from jax.sharding import PartitionSpec as P

IMG = 4096
NB = 8
NV = 32
MESH_ID = pl.DeviceIdType.MESH
highest = lax.Precision.HIGHEST
f32 = jnp.float32
bf16 = jnp.bfloat16

low_taps = (
    -0.010597401784997278,
    0.032883011666982945,
    0.030841381835986965,
    -0.18703481171888114,
    -0.02798376941698385,
    0.6308807679295904,
    0.7148465705525415,
    0.23037781330885523,
)
high_taps = tuple(((-1.0) ** offset * low_taps[7 - offset] for offset in range(8)))


def halves_of(table):
    high = table.astype(bf16)
    low = (table - high.astype(np.float64)).astype(bf16)
    return high, low


def dft512_tables():
    index = np.arange(512)
    angle = 2.0 * np.pi / 512 * (index[:, None] * index[None, :] % 512)
    return halves_of(np.concatenate([np.cos(angle), np.sin(angle)], axis=0))


def dft128_table():
    index = np.arange(128)
    angle = 2.0 * np.pi / 128 * (index[:, None] * index[None, :] % 128)
    return (np.concatenate([np.cos(angle), np.sin(angle)], axis=1) / IMG).astype(np.float32)


def row_twist():
    angle = 2.0 * np.pi / IMG * (np.arange(32)[:, None] * np.arange(128)[None, :] % IMG)
    return np.stack([np.cos(angle), np.sin(angle)], axis=1).astype(np.float32)


def wavelet_tables():
    up = np.zeros((512, 256))
    down = np.zeros((384, 256))
    rows_up = np.zeros((2, 16, 32))
    rows_down = np.zeros((16, 24))
    for tap in range(8):
        for side, taps in ((0, low_taps), (1, high_taps)):
            for k in range(128):
                down[2 * k + tap, 128 * side + k] = taps[tap]
            for k in range(-128, 128):
                if 0 <= 2 * k + tap < 256:
                    up[256 * side + 128 + k, 2 * k + tap] = taps[tap]
            for k in range(8):
                rows_down[8 * side + k, 2 * k + tap] = taps[tap]
            for k in range(-3, 8):
                if 0 <= 2 * k + tap < 16:
                    for part in range(2):
                        spot = 8 * side + k if k >= 0 else 16 + 3 * (part + 2 * side) + k + 3
                        rows_up[part, 2 * k + tap, spot] = taps[tap]
    sides = np.zeros((48, 32))
    sides[0:32] = rows_up.reshape(32, 32)
    sides[32:48, 0:24] = rows_down
    return tuple(part for table in (up, down, sides) for part in halves_of(table))


def lane_order():
    place = np.zeros((128, 128), np.float32)
    for t in range(128):
        place[(t % 8) * 16 + t // 8, t] = 1.0
    return place.astype(bf16)


def times(pair, cosine, sine):
    re, im = pair
    if abs(sine) < 1e-12:
        if cosine > 0:
            return pair
        return (-re, None if im is None else -im)
    if abs(cosine) < 1e-12:
        if im is None:
            return (None, re if sine > 0 else -re)
        return (-im, re) if sine > 0 else (im, -re)
    cosine, sine = np.float32(cosine), np.float32(sine)
    if im is None:
        return (re * cosine, re * sine)
    return (re * cosine - im * sine, re * sine + im * cosine)


def plus(a, b):
    if a is None:
        return b
    return a if b is None else a + b


def minus(a, b):
    if b is None:
        return a
    return -b if a is None else a - b


def small_dft(values, sign):
    count = len(values)
    if count == 1:
        return values
    even = small_dft(values[0::2], sign)
    odd = small_dft(values[1::2], sign)
    out = [None] * count
    for k in range(count // 2):
        angle = sign * 2.0 * math.pi * k / count
        turned = times(odd[k], math.cos(angle), math.sin(angle))
        out[k] = (plus(even[k][0], turned[0]), plus(even[k][1], turned[1]))
        out[k + count // 2] = (minus(even[k][0], turned[0]), minus(even[k][1], turned[1]))
    return out


def swap_groups(arrays):
    arrays = list(arrays)
    lane = lax.broadcasted_iota(jnp.int32, arrays[0].shape, arrays[0].ndim - 1)
    axis = arrays[0].ndim - 1
    for bit in range(3):
        shift = 16 << bit
        upper = (lane // shift) % 2 == 1
        for j in range(8):
            other = j | (1 << bit)
            if other == j:
                continue
            low, high = arrays[j], arrays[other]
            arrays[j] = jnp.where(upper, pltpu.roll(high, shift, axis), low)
            arrays[other] = jnp.where(upper, high, pltpu.roll(low, 128 - shift, axis))
    return arrays


def dot(a, b):
    return jnp.dot(a, b, preferred_element_type=f32)


def dot_nt(a, b):
    return lax.dot_general(a, b, (((1,), (1,)), ((), ())), preferred_element_type=f32)


def halves(value):
    high = value.astype(bf16)
    return high, (value - high.astype(f32)).astype(bf16)


def by_table(value, high, low):
    value_high, value_low = halves(value)
    return dot(value_high, high) + dot(value_low, high) + dot(value_high, low)


def table_by(high, low, value):
    value_high, value_low = halves(value)
    return dot(high, value_high) + dot(high, value_low) + dot(low, value_high)


def greet(vis_me, band_me, neighbours):
    barrier = pltpu.get_barrier_semaphore()

    def vis_signal(d, carry):
        pl.semaphore_signal(
            barrier, inc=1, device_id={"vis": vis_me ^ d}, device_id_type=MESH_ID
        )
        return carry

    def band_signal(d, carry):
        pl.semaphore_signal(
            barrier, inc=1, device_id={"band": band_me ^ d}, device_id_type=MESH_ID
        )
        return carry

    for neighbour in neighbours:
        pl.semaphore_signal(barrier, inc=1, device_id=neighbour, device_id_type=MESH_ID)
    lax.fori_loop(1, NV, vis_signal, 0)
    lax.fori_loop(1, NB, band_signal, 0)
    return barrier


def launch(sent, landed, sems, axis, count, me, same=False):
    def body(d, carry):
        peer = me ^ d
        pltpu.make_async_remote_copy(
            src_ref=sent if same else sent.at[peer],
            dst_ref=landed.at[me],
            send_sem=sems.at[0],
            recv_sem=sems.at[1],
            device_id={axis: peer},
            device_id_type=MESH_ID,
        ).start()
        return carry

    lax.fori_loop(1, count, body, 0)
    landed[me] = sent[...] if same else sent[me]


def to_neighbour(sent, landed, sems, neighbour):
    copy = pltpu.make_async_remote_copy(
        src_ref=sent,
        dst_ref=landed,
        send_sem=sems.at[0],
        recv_sem=sems.at[1],
        device_id=neighbour,
        device_id_type=MESH_ID,
    )
    copy.start()
    return copy


def arrived(landed, sems, count):
    part = landed.at[pl.ds(0, count - 1)]
    pltpu.make_async_copy(part, part, sems.at[1]).wait()


def drained(landed, sems, count):
    part = landed.at[pl.ds(0, count - 1)]
    pltpu.make_async_copy(part, part, sems.at[0]).wait()


def step_kernel(*refs):
    names = INPUTS + OUTPUTS + list(SCRATCH)
    r = dict(zip(names, refs))
    vis_me, band_me = lax.axis_index("vis"), lax.axis_index("band")
    me = band_me * NV + vis_me
    following = (me + 1) % (NB * NV)
    preceding = (me + NB * NV - 1) % (NB * NV)
    following = {"band": following // NV, "vis": following % NV}
    preceding = {"band": preceding // NV, "vis": preceding % NV}
    copies = {}
    for place, name in enumerate(STAGED):
        copies[name] = pltpu.make_async_copy(r[name], r["here_" + name], r["sem_in"].at[place])
        copies[name].start()

    def staged(name):
        if name in copies:
            copies.pop(name).wait()
        return r["here_" + name]

    barrier = greet(vis_me, band_me, (following, preceding))

    weights, places, sent_a, got_a = r["weights"], r["places"], r["sent_a"], r["got_a"]
    kernels = staged("kernels")
    for q in range(NV):
        part = dot(weights[q], kernels[q])
        sent_a[q] = jnp.concatenate([part, places[q]], axis=0).astype(bf16)
    pl.semaphore_wait(barrier, NV + NB)
    launch(sent_a, got_a, r["sem_a"], "vis", NV, vis_me)
    coef_copy = to_neighbour(r["coef_rows"], r["got_coef"], r["sem_coef"], following)

    coef, sky = staged("coef"), staged("sky")
    sides_hi, sides_lo = r["sides_hi"], r["sides_lo"]
    up_hi, up_lo = staged("up_hi"), staged("up_lo")
    coef_copy.wait_recv()
    rows_up = []
    for part in range(2):
        rows = slice(16 * part, 16 * part + 16)
        stack = jnp.concatenate([coef[part], coef[part + 2], r["got_coef"][...]], axis=0)
        rows_up.append(table_by(sides_hi[rows, :], sides_lo[rows, :], stack))
    stack = []
    for n in range(16):
        parts = []
        for field in rows_up:
            for block in ((n + 15) % 16, n):
                parts.append(field[:, 128 * block : 128 * block + 128])
        stack.append(jnp.concatenate(parts, axis=1))
    smooth = by_table(jnp.concatenate(stack, axis=0), up_hi[...], up_lo[...])
    raw = r["raw_here"]
    for n in range(16):
        cols = slice(256 * n, 256 * n + 256)
        raw[:, cols] = sky[:, cols] - smooth[16 * n : 16 * n + 16]
    arrived(got_a, r["sem_a"], NV)

    order, onehot, sent_b, got_b = r["order"], r["onehot"], r["sent_b"], r["got_b"]
    contrib = got_a[:, 0:8, :].astype(f32).reshape(256, 128).astype(bf16)
    where_to = got_a[:, 8:16, :].astype(f32).reshape(256, 128)
    lane = lax.broadcasted_iota(jnp.int32, (256, 128), 1).astype(f32)
    is_imag = lax.broadcasted_iota(jnp.int32, (256, 128), 0) % 2 == 1
    hots = [(where_to == lane + float(128 * g - 256)).astype(f32) for g in range(4)]
    for g in range(4):
        onehot[:, 128 * g : 128 * g + 128] = hots[g].astype(bf16)
    real_hots = [jnp.where(is_imag, 0.0, h).astype(bf16) for h in hots]
    imag_hots = [jnp.where(is_imag, h, 0.0).astype(bf16) for h in hots]
    turned = dot_nt(order[...], contrib).astype(bf16)
    for c, some in ((0, real_hots), (1, imag_hots)):
        for g in range(4):
            grid = dot(turned, some[g]).astype(bf16)
            for low in range(8):
                sent_b[low * 4 + g, c] = grid[16 * low : 16 * low + 16]
    launch(sent_b, got_b, r["sem_b"], "vis", NV, vis_me)
    table_hi, table_lo = staged("table_hi"), staged("table_lo")
    arrived(got_b, r["sem_b"], NV)

    sent_c, got_c = r["sent_c"], r["got_c"]
    spread = jnp.concatenate(
        [got_b[:, 0].reshape(512, 128), got_b[:, 1].reshape(512, 128)], axis=1
    )
    both = dot(table_hi[...], spread) + dot(table_lo[...], spread)
    sent_c[:, 0] = (both[:512, :128] - both[512:, 128:]).astype(bf16).reshape(NV, 16, 128)
    sent_c[:, 1] = (both[512:, :128] + both[:512, 128:]).astype(bf16).reshape(NV, 16, 128)
    launch(sent_c, got_c, r["sem_c"], "vis", NV, vis_me)
    arrived(got_c, r["sem_c"], NV)

    sent_d, got_d, twist_col = r["sent_d"], r["got_d"], r["twist_col"]
    for g in range(4):
        values = []
        for low in range(8):
            re = got_c[low * 4 + g, 0].astype(f32)
            im = got_c[low * 4 + g, 1].astype(f32)
            cosine, sine = twist_col[low, 0], twist_col[low, 1]
            values.append((re * cosine - im * sine, re * sine + im * cosine))
        values = small_dft(values, 1.0)
        for b in range(NB):
            for c in range(2):
                sent_d[b, c, :, 128 * g : 128 * g + 128] = values[b][c].astype(sent_d.dtype)
    launch(sent_d, got_d, r["sem_d"], "band", NB, band_me)
    arrived(got_d, r["sem_d"], NB)

    mid, table128, twist_row = r["mid"], r["table128"], r["twist_row"]
    for g in range(4):
        for c in range(2):
            parts = swap_groups(
                [got_d[b, c, :, 128 * g : 128 * g + 128].astype(f32) for b in range(NB)]
            )
            for a in range(8):
                mid[g * 8 + a, c] = parts[a]
    lanes = jnp.dot(
        mid[...].reshape(1024, 128), table128[...], precision=highest, preferred_element_type=f32
    ).reshape(32, 2, 16, 256)
    extrap = r["extrap"]
    for half in range(2):
        rows = slice(8 * half, 8 * half + 8)
        values = []
        for a in range(32):
            re = lanes[a, 0, rows, :128] - lanes[a, 1, rows, 128:]
            im = lanes[a, 0, rows, 128:] + lanes[a, 1, rows, :128]
            cosine, sine = twist_row[a, 0:1], twist_row[a, 1:2]
            values.append((re * cosine - im * sine, re * sine + im * cosine))
        values = small_dft(values, 1.0)
        for n in range(32):
            cols = slice(128 * n, 128 * n + 128)
            now = raw[rows, cols] - values[n][0]
            raw[rows, cols] = now
            extrap[rows, cols] = 2.0 * jnp.maximum(now, 0.0) - sky[rows, cols]
    image_copy = to_neighbour(extrap.at[pl.ds(0, 8)], r["got_rows"], r["sem_rows"], preceding)
    out_raw = pltpu.make_async_copy(raw, r["raw"], r["sem_out"].at[0])
    out_raw.start()

    sent_e, got_e = r["sent_e"], r["got_e"]
    for half in range(2):
        rows = slice(8 * half, 8 * half + 8)
        values = [(extrap[rows, 128 * n : 128 * n + 128], None) for n in range(32)]
        values = small_dft(values, -1.0)
        for a in range(32):
            re, im = values[a]
            cosine, sine = twist_row[a, 0:1], twist_row[a, 1:2]
            if im is None:
                mid[a, 0, rows] = re * cosine
                mid[a, 1, rows] = -re * sine
            else:
                mid[a, 0, rows] = re * cosine + im * sine
                mid[a, 1, rows] = im * cosine - re * sine
    lanes = jnp.dot(
        mid[...].reshape(1024, 128), table128[...], precision=highest, preferred_element_type=f32
    ).reshape(32, 2, 16, 256)
    for g in range(4):
        for c in range(2):
            parts = []
            for a in range(8):
                re, im = lanes[g * 8 + a, 0], lanes[g * 8 + a, 1]
                if c == 0:
                    parts.append(re[:, :128] + im[:, 128:])
                else:
                    parts.append(im[:, :128] - re[:, 128:])
            parts = swap_groups(parts)
            for b in range(NB):
                sent_e[b, c, :, 128 * g : 128 * g + 128] = parts[b].astype(sent_e.dtype)
    launch(sent_e, got_e, r["sem_e"], "band", NB, band_me)

    down_hi, down_lo = staged("down_hi"), staged("down_lo")
    image_copy.wait_recv()
    fields = jnp.concatenate([extrap[...], r["got_rows"][...]], axis=0)
    fields = table_by(sides_hi[32:48, 0:24], sides_lo[32:48, 0:24], fields)
    stack = []
    for n in range(16):
        if n < 15:
            stack.append(fields[:, 256 * n : 256 * n + 384])
        else:
            stack.append(jnp.concatenate([fields[:, 3840:4096], fields[:, 0:128]], axis=1))
    found = by_table(jnp.concatenate(stack, axis=0), down_hi[...], down_lo[...])
    coeffs = r["coeffs_here"]
    for n in range(16):
        cols = slice(128 * n, 128 * n + 128)
        block = found[16 * n : 16 * n + 16]
        coeffs[0, :, cols] = block[0:8, :128]
        coeffs[1, :, cols] = block[0:8, 128:]
        coeffs[2, :, cols] = block[8:16, :128]
        coeffs[3, :, cols] = block[8:16, 128:]
    abs_total = jnp.sum(jnp.abs(found))
    out_coeffs = pltpu.make_async_copy(coeffs, r["coeffs"], r["sem_out"].at[1])
    out_coeffs.start()
    arrived(got_e, r["sem_e"], NB)

    sent_f, got_f = r["sent_f"], r["got_f"]
    for g in range(4):
        values = []
        for b in range(NB):
            values.append(
                tuple(
                    got_e[b, c, :, 128 * g : 128 * g + 128].astype(f32) for c in range(2)
                )
            )
        values = small_dft(values, -1.0)
        for low in range(8):
            re, im = values[low]
            cosine, sine = twist_col[low, 0], twist_col[low, 1]
            sent_f[low * 4 + g, 0] = (re * cosine + im * sine).astype(sent_f.dtype)
            sent_f[low * 4 + g, 1] = (im * cosine - re * sine).astype(sent_f.dtype)
    launch(sent_f, got_f, r["sem_f"], "vis", NV, vis_me)
    arrived(got_f, r["sem_f"], NV)

    sent_g, got_g = r["sent_g"], r["got_g"]
    spread = jnp.concatenate(
        [got_f[:, 0].reshape(512, 128), got_f[:, 1].reshape(512, 128)], axis=1
    )
    if spread.dtype == f32:
        both = table_by(table_hi[...], table_lo[...], spread)
    else:
        both = dot(table_hi[...], spread) + dot(table_lo[...], spread)
    sent_g[:, 0] = (both[:512, :128] + both[512:, 128:]).astype(bf16).reshape(NV, 16, 128)
    sent_g[:, 1] = (both[:512, 128:] - both[512:, :128]).astype(bf16).reshape(NV, 16, 128)
    launch(sent_g, got_g, r["sem_g"], "vis", NV, vis_me)
    arrived(got_g, r["sem_g"], NV)

    sent_h, got_h = r["sent_h"], r["got_h"]
    picked = []
    for c in range(2):
        total = 0.0
        for g in range(4):
            piece = jnp.concatenate([got_g[low * 4 + g, c] for low in range(8)], axis=0)
            total = total + dot_nt(onehot[:, 128 * g : 128 * g + 128], piece)
        picked.append(total)
    tiles = jnp.where(is_imag, picked[1], picked[0]).astype(bf16)
    tiles = dot(tiles, order[...])
    sent_h[...] = tiles.reshape(NV, 8, 128).astype(bf16)
    launch(sent_h, got_h, r["sem_h"], "vis", NV, vis_me)
    data_square = jnp.sum(r["live"][...] * r["vis_data"][...] * r["vis_data"][...])
    arrived(got_h, r["sem_h"], NV)

    row = lax.broadcasted_iota(jnp.int32, (8, 256), 0)
    slot = lax.broadcasted_iota(jnp.int32, (8, 256), 1) // 64
    on_real = row == 2 * slot
    on_imag = row == 2 * slot + 1
    from_real, from_imag = [], []
    for q in range(NV):
        product = dot_nt(got_h[q], kernels[q])
        from_real.append(jnp.sum(jnp.where(on_real, product, 0.0), axis=0, keepdims=True))
        from_imag.append(jnp.sum(jnp.where(on_imag, product, 0.0), axis=0, keepdims=True))
    from_real = jnp.concatenate(from_real, axis=0)
    from_imag = jnp.concatenate(from_imag, axis=0)
    imag_lane = (lax.broadcasted_iota(jnp.int32, (NV, 256), 1) // 32) % 2 == 1
    predicted = from_real + jnp.where(
        imag_lane, pltpu.roll(from_imag, 32, 1), -pltpu.roll(from_imag, 256 - 32, 1)
    )
    residual = r["live"][...] * (r["vis_state"][...] + predicted - r["vis_data"][...])
    resid_square = jnp.sum(residual * residual)

    sent_t, got_t, sent_u, got_u = r["sent_t"], r["got_t"], r["sent_u"], r["got_u"]
    spot = lax.broadcasted_iota(jnp.int32, (8, 128), 0)
    sent_t[...] = jnp.where(
        spot == 0, abs_total, jnp.where(spot == 1, resid_square, data_square)
    )
    launch(sent_t, got_t, r["sem_t"], "vis", NV, vis_me, same=True)
    arrived(got_t, r["sem_t"], NV)
    sent_u[...] = jnp.sum(got_t[...], axis=0)
    launch(sent_u, got_u, r["sem_u"], "band", NB, band_me, same=True)
    arrived(got_u, r["sem_u"], NB)
    totals = jnp.sum(got_u[...], axis=0)
    r["totals"][...] = totals
    radius = 0.5 * jnp.sqrt(totals[2:3, :] + 1e-06)
    size = jnp.sqrt(totals[1:2, :] + 1e-06)
    factor = 1.0 - jnp.minimum(1.0, radius / size)
    r["vis_new"][:, 0:128] = residual[:, 0:128] * factor
    r["vis_new"][:, 128:256] = residual[:, 128:256] * factor

    for copy in (coef_copy, image_copy):
        copy.wait_send()
    out_raw.wait()
    out_coeffs.wait()
    for name, landed, count in (
        ("a", got_a, NV), ("b", got_b, NV), ("c", got_c, NV), ("d", got_d, NB),
        ("e", got_e, NB), ("f", got_f, NV), ("g", got_g, NV), ("h", got_h, NV),
        ("t", got_t, NV), ("u", got_u, NB),
    ):
        drained(landed, r["sem_" + name], count)


STAGED = ["kernels", "coef", "sky", "up_hi", "up_lo", "table_hi", "table_lo", "down_hi", "down_lo"]
INPUTS = STAGED + [
    "coef_rows", "weights", "places", "live", "vis_state", "vis_data",
    "table128", "twist_row", "twist_col", "order", "sides_hi", "sides_lo",
]
OUTPUTS = ["raw", "coeffs", "vis_new", "totals"]
VIS_TILE = (NV, 2, 16, 128)
BAND_TILE = (NB, 2, 16, 512)
SCRATCH = dict(
    here_kernels=((NV, 256, 128), bf16),
    here_coef=((4, 8, 2048), f32),
    here_sky=((16, IMG), f32),
    here_up_hi=((512, 256), bf16),
    here_up_lo=((512, 256), bf16),
    here_table_hi=((1024, 512), bf16),
    here_table_lo=((1024, 512), bf16),
    here_down_hi=((384, 256), bf16),
    here_down_lo=((384, 256), bf16),
    sent_a=((NV, 16, 128), bf16), got_a=((NV, 16, 128), bf16),
    sent_b=(VIS_TILE, bf16), got_b=(VIS_TILE, bf16),
    sent_c=(VIS_TILE, bf16), got_c=(VIS_TILE, bf16),
    sent_d=(BAND_TILE, bf16), got_d=(BAND_TILE, bf16),
    sent_e=(BAND_TILE, f32), got_e=(BAND_TILE, f32),
    sent_f=(VIS_TILE, f32), got_f=(VIS_TILE, f32),
    sent_g=(VIS_TILE, bf16), got_g=(VIS_TILE, bf16),
    sent_h=((NV, 8, 128), bf16), got_h=((NV, 8, 128), bf16),
    sent_t=((8, 128), f32), got_t=((NV, 8, 128), f32),
    sent_u=((8, 128), f32), got_u=((NB, 8, 128), f32),
    got_coef=((16, 2048), f32), got_rows=((8, IMG), f32),
    raw_here=((16, IMG), f32), extrap=((16, IMG), f32), coeffs_here=((4, 8, 2048), f32),
    onehot=((256, 512), bf16), mid=((32, 2, 16, 128), f32),
    **{"sem_" + n: 2 for n in list("abcdefghtu") + ["coef", "rows", "out"]},
    sem_in=len(STAGED),
)


def step(inputs):
    anywhere = pl.BlockSpec(memory_space=pl.ANY)
    vmem = pl.BlockSpec(memory_space=pltpu.VMEM)
    scratch = []
    for what in SCRATCH.values():
        if isinstance(what, int):
            scratch.append(pltpu.SemaphoreType.DMA((what,)))
        else:
            scratch.append(pltpu.VMEM(*what))
    return pl.pallas_call(
        step_kernel,
        out_shape=(
            jax.ShapeDtypeStruct((16, IMG), f32),
            jax.ShapeDtypeStruct((4, 8, 2048), f32),
            jax.ShapeDtypeStruct((NV, 256), f32),
            jax.ShapeDtypeStruct((8, 128), f32),
        ),
        in_specs=[anywhere if name in STAGED else vmem for name in INPUTS],
        out_specs=(anywhere, anywhere, vmem, vmem),
        scratch_shapes=scratch,
        compiler_params=pltpu.CompilerParams(
            collective_id=0, has_side_effects=True, vmem_limit_bytes=56 * 2**20
        ),
    )(*[inputs[name] for name in INPUTS])


def local(sky_image, coef_dual, vis_dual, visibilities, kernel_blocks, tile_rows, tile_counts):
    kernels = kernel_blocks.reshape(NV, 256, 128)
    rows_here = tile_rows.reshape(NV, 4)
    counts = tile_counts.reshape(NV, 1)
    live = (jnp.arange(256, dtype=jnp.int32)[None, :] // 64 < counts).astype(f32)
    vis_data = visibilities.reshape(NV, 256)
    vis_state = vis_dual.reshape(NV, 256)

    wb = live * vis_state
    lane = jnp.arange(256, dtype=jnp.int32)
    imag_lane = (lane // 32) % 2 == 1
    crossed = jnp.where(imag_lane, -jnp.roll(wb, 32, axis=1), jnp.roll(wb, -32, axis=1))
    slot_row = jnp.arange(8, dtype=jnp.int32)
    same = (slot_row[:, None] // 2 == lane[None, :] // 64)[None]
    chosen = jnp.where((slot_row % 2 == 1)[None, :, None], crossed[:, None, :], wb[:, None, :])
    weights = jnp.where(same, chosen, 0.0).astype(bf16)

    place = (rows_here % 32) * 16 + rows_here // 32 - 256
    places = jnp.broadcast_to(
        jnp.repeat(place.astype(f32), 2, axis=1)[:, :, None], (NV, 8, 128)
    )

    low = jnp.arange(8, dtype=jnp.int32)[:, None]
    mu = lax.axis_index("vis") * 16 + jnp.arange(16, dtype=jnp.int32)[None, :]
    angle = (2.0 * math.pi / IMG) * (low * mu).astype(f32)
    twist_col = jnp.broadcast_to(
        jnp.stack([jnp.cos(angle), jnp.sin(angle)], axis=1)[..., None], (8, 2, 16, 128)
    )
    inputs = dict(zip(
        ("table_hi", "table_lo", "up_hi", "up_lo", "down_hi", "down_lo", "sides_hi", "sides_lo"),
        dft512_tables() + wavelet_tables(),
    ))
    inputs = {name: jnp.asarray(table) for name, table in inputs.items()}
    inputs.update(
        table128=jnp.asarray(dft128_table()), twist_row=jnp.asarray(row_twist()),
        twist_col=twist_col, order=jnp.asarray(lane_order()),
        kernels=kernels, coef=coef_dual, sky=sky_image,
        coef_rows=jnp.pad(coef_dual[:, 5:8].reshape(12, 2048), ((0, 4), (0, 0))),
        weights=weights, places=places, live=live, vis_state=vis_state, vis_data=vis_data,
    )
    raw, coeffs, vis_new, totals = step(inputs)
    threshold = 0.5 * totals[0, 0] / (IMG * IMG)
    new_image = jnp.maximum(raw, 0.0)
    new_coef = jnp.clip(coef_dual + coeffs, -threshold, threshold)
    return (new_image, new_coef, vis_new.reshape(1, 1, NV, 4, 2, 32))


def solution(mesh):
    return jax.shard_map(
        local,
        mesh=mesh,
        in_specs=(
            P(("band", "vis"), None),
            P(None, ("band", "vis"), None),
            P("band", "vis", None, None, None, None),
            P("band", "vis", None, None, None, None),
            P("band", "vis", None, None, None, None, None),
            P("band", "vis", None, None),
            P("band", "vis", None),
        ),
        out_specs=(
            P(("band", "vis"), None),
            P(None, ("band", "vis"), None),
            P("band", "vis", None, None, None, None),
        ),
        check_vma=False,
    )
```

```python
import functools
import math

import jax
import jax.numpy as jnp
import numpy as np
from jax import lax
from jax.experimental import pallas as pl
from jax.experimental.pallas import tpu as pltpu
from jax.sharding import PartitionSpec as P

IMG = 4096
NB = 8
NV = 32
MESH_ID = pl.DeviceIdType.MESH
f32 = jnp.float32
bf16 = jnp.bfloat16

low_taps = (
    -0.010597401784997278,
    0.032883011666982945,
    0.030841381835986965,
    -0.18703481171888114,
    -0.02798376941698385,
    0.6308807679295904,
    0.7148465705525415,
    0.23037781330885523,
)
high_taps = tuple(((-1.0) ** offset * low_taps[7 - offset] for offset in range(8)))


def halves_of(table):
    high = table.astype(bf16)
    low = (table - high.astype(np.float64)).astype(bf16)
    return high, low


def dft512_tables():
    index = np.arange(512)
    angle = 2.0 * np.pi / 512 * (index[:, None] * index[None, :] % 512)
    return halves_of(np.concatenate([np.cos(angle), np.sin(angle)], axis=0))


def dft128_tables():
    index = np.arange(128)
    angle = 2.0 * np.pi / 128 * (index[:, None] * index[None, :] % 128)
    return halves_of(np.concatenate([np.cos(angle), np.sin(angle)], axis=1) / IMG)


def row_twist():
    angle = 2.0 * np.pi / IMG * (np.arange(32)[:, None] * np.arange(128)[None, :] % IMG)
    return np.stack([np.cos(angle), np.sin(angle)], axis=1).astype(np.float32)


def col_twist():
    low, row = np.arange(8)[None, :, None], np.arange(16)[None, None, :]
    angle = 2.0 * np.pi / IMG * (low * (16 * np.arange(NV)[:, None, None] + row))
    return np.stack([np.cos(angle), np.sin(angle)], axis=1).reshape(NV, 2, 128).astype(np.float32)


def repeat_table():
    return np.tile(np.eye(32), (1, 8)).astype(bf16)


def wavelet_tables():
    up = np.zeros((512, 256))
    down = np.zeros((384, 256))
    rows_up = np.zeros((2, 16, 32))
    rows_down = np.zeros((16, 24))
    for tap in range(8):
        for side, taps in ((0, low_taps), (1, high_taps)):
            for k in range(128):
                down[2 * k + tap, 128 * side + k] = taps[tap]
            for k in range(-128, 128):
                if 0 <= 2 * k + tap < 256:
                    up[256 * side + 128 + k, 2 * k + tap] = taps[tap]
            for k in range(8):
                rows_down[8 * side + k, 2 * k + tap] = taps[tap]
            for k in range(-3, 8):
                if 0 <= 2 * k + tap < 16:
                    for part in range(2):
                        spot = 8 * side + k if k >= 0 else 16 + 3 * (part + 2 * side) + k + 3
                        rows_up[part, 2 * k + tap, spot] = taps[tap]
    sides = np.zeros((48, 32))
    sides[0:32] = rows_up.reshape(32, 32)
    sides[32:48, 0:24] = rows_down
    return tuple(part for table in (up, down, sides) for part in halves_of(table))


def lane_order():
    place = np.zeros((128, 128), np.float32)
    for t in range(128):
        place[(t % 8) * 16 + t // 8, t] = 1.0
    return place.astype(bf16)


def times(pair, cosine, sine):
    re, im = pair
    if abs(sine) < 1e-12:
        if cosine > 0:
            return pair
        return (-re, None if im is None else -im)
    if abs(cosine) < 1e-12:
        if im is None:
            return (None, re if sine > 0 else -re)
        return (-im, re) if sine > 0 else (im, -re)
    cosine, sine = np.float32(cosine), np.float32(sine)
    if im is None:
        return (re * cosine, re * sine)
    return (re * cosine - im * sine, re * sine + im * cosine)


def plus(a, b):
    if a is None:
        return b
    return a if b is None else a + b


def minus(a, b):
    if b is None:
        return a
    return -b if a is None else a - b


def small_dft(values, sign):
    count = len(values)
    if count == 1:
        return values
    even = small_dft(values[0::2], sign)
    odd = small_dft(values[1::2], sign)
    out = [None] * count
    for k in range(count // 2):
        angle = sign * 2.0 * math.pi * k / count
        turned = times(odd[k], math.cos(angle), math.sin(angle))
        out[k] = (plus(even[k][0], turned[0]), plus(even[k][1], turned[1]))
        out[k + count // 2] = (minus(even[k][0], turned[0]), minus(even[k][1], turned[1]))
    return out


def swap_groups(arrays):
    arrays = list(arrays)
    lane = lax.broadcasted_iota(jnp.int32, arrays[0].shape, arrays[0].ndim - 1)
    axis = arrays[0].ndim - 1
    for bit in range(3):
        shift = 16 << bit
        upper = (lane // shift) % 2 == 1
        for j in range(8):
            other = j | (1 << bit)
            if other == j:
                continue
            low, high = arrays[j], arrays[other]
            arrays[j] = jnp.where(upper, pltpu.roll(high, shift, axis), low)
            arrays[other] = jnp.where(upper, high, pltpu.roll(low, 128 - shift, axis))
    return arrays


def dot(a, b):
    return jnp.dot(a, b, preferred_element_type=f32)


def dot_nt(a, b):
    return lax.dot_general(a, b, (((1,), (1,)), ((), ())), preferred_element_type=f32)


def halves(value):
    high = value.astype(bf16)
    return high, (value - high.astype(f32)).astype(bf16)


def by_table(value, high, low):
    value_high, value_low = halves(value)
    return dot(value_high, high) + dot(value_low, high) + dot(value_high, low)


def table_by(high, low, value):
    value_high, value_low = halves(value)
    return dot(high, value_high) + dot(high, value_low) + dot(low, value_high)


def greet(vis_me, band_me, neighbours):
    barrier = pltpu.get_barrier_semaphore()

    def vis_signal(d, carry):
        pl.semaphore_signal(
            barrier, inc=1, device_id={"vis": vis_me ^ d}, device_id_type=MESH_ID
        )
        return carry

    def band_signal(d, carry):
        pl.semaphore_signal(
            barrier, inc=1, device_id={"band": band_me ^ d}, device_id_type=MESH_ID
        )
        return carry

    for neighbour in neighbours:
        pl.semaphore_signal(barrier, inc=1, device_id=neighbour, device_id_type=MESH_ID)
    lax.fori_loop(1, NV, vis_signal, 0)
    lax.fori_loop(1, NB, band_signal, 0)
    return barrier


def launch(sent, landed, sems, axis, count, me, same=False):
    def body(d, carry):
        peer = me ^ d
        pltpu.make_async_remote_copy(
            src_ref=sent if same else sent.at[peer],
            dst_ref=landed.at[me],
            send_sem=sems.at[0],
            recv_sem=sems.at[1],
            device_id={axis: peer},
            device_id_type=MESH_ID,
        ).start()
        return carry

    lax.fori_loop(1, count, body, 0)
    landed[me] = sent[...] if same else sent[me]


def to_neighbour(sent, landed, sems, neighbour):
    copy = pltpu.make_async_remote_copy(
        src_ref=sent,
        dst_ref=landed,
        send_sem=sems.at[0],
        recv_sem=sems.at[1],
        device_id=neighbour,
        device_id_type=MESH_ID,
    )
    copy.start()
    return copy


def arrived(landed, sems, count):
    part = landed.at[pl.ds(0, count - 1)]
    pltpu.make_async_copy(part, part, sems.at[1]).wait()


def drained(landed, sems, count):
    part = landed.at[pl.ds(0, count - 1)]
    pltpu.make_async_copy(part, part, sems.at[0]).wait()


def step_kernel(*refs):
    names = INPUTS + OUTPUTS + list(SCRATCH)
    r = dict(zip(names, refs))
    vis_me, band_me = lax.axis_index("vis"), lax.axis_index("band")
    me = band_me * NV + vis_me
    following = (me + 1) % (NB * NV)
    preceding = (me + NB * NV - 1) % (NB * NV)
    following = {"band": following // NV, "vis": following % NV}
    preceding = {"band": preceding // NV, "vis": preceding % NV}
    copies = {}
    for place, name in enumerate(STAGED):
        copies[name] = pltpu.make_async_copy(r[name], r["here_" + name], r["sem_in"].at[place])
        copies[name].start()

    def staged(name):
        if name in copies:
            copies.pop(name).wait()
        return r["here_" + name]

    barrier = greet(vis_me, band_me, (following, preceding))

    to_row = (
        lax.broadcasted_iota(jnp.int32, (256, 32), 0) // 8
        == lax.broadcasted_iota(jnp.int32, (256, 32), 1)
    ).astype(f32).astype(bf16)
    column = r["rows"][...]
    facts = jnp.concatenate(
        [column % 32 * 16 + column // 32 - 256, r["counts"][...], jnp.zeros((3, 32), jnp.int32)],
        axis=0,
    ).astype(f32).astype(bf16)
    facts = dot_nt(to_row, facts)
    slot_here = lax.broadcasted_iota(jnp.int32, (256, 8), 0) % 8 // 2
    fact = lax.broadcasted_iota(jnp.int32, (256, 8), 1)
    place = jnp.sum(jnp.where(fact == slot_here, facts, 0.0), axis=1, keepdims=True)
    count = jnp.sum(jnp.where(fact == 4, facts, 0.0), axis=1, keepdims=True)
    places = jnp.broadcast_to(place, (256, 128)).reshape(NV, 8, 128)
    live = jnp.broadcast_to(count, (256, 32)) > (
        lax.broadcasted_iota(jnp.int32, (256, 32), 0) % 8 // 2
    ).astype(f32)
    live = jnp.where(live, 1.0, 0.0)
    vis_state = r["vis_state"][...].reshape(256, 32)
    vis_data = r["vis_data"][...].reshape(256, 32)
    data_square = jnp.sum(live * vis_data * vis_data)

    weights = dot((live * vis_state).astype(bf16), r["repeat"][...]).reshape(NV, 8, 256)
    wide_row = lax.broadcasted_iota(jnp.int32, (NV, 8, 256), 1)
    wide_lane = lax.broadcasted_iota(jnp.int32, (NV, 8, 256), 2)
    crossed = jnp.where(
        wide_row % 2 == 0, pltpu.roll(weights, 7, 1), -pltpu.roll(weights, 1, 1)
    )
    weights = jnp.where(wide_lane // 32 % 2 == 0, weights, crossed)
    r["weights"][...] = jnp.where(wide_lane // 64 == wide_row // 2, weights, 0.0).astype(bf16)
    twist_col = r["twist_col"]
    eye = (
        lax.broadcasted_iota(jnp.int32, (128, 128), 0)
        == lax.broadcasted_iota(jnp.int32, (128, 128), 1)
    )
    for c in range(2):
        one = jnp.broadcast_to(r["twists"][vis_me, c : c + 1, :], (128, 128))
        one = jnp.sum(jnp.where(eye, one, 0.0), axis=1, keepdims=True)
        twist_col[:, c] = jnp.broadcast_to(one, (128, 128)).reshape(8, 16, 128)

    sent_a, got_a = r["sent_a"], r["got_a"]
    coef = staged("coef")
    for part in range(4):
        r["coef_rows"][3 * part : 3 * part + 3] = coef[part, 5:8, :]
    r["coef_rows"][12:16] = jnp.zeros((4, 2048), f32)
    kernels = staged("kernels")
    for q in range(NV):
        part = dot(r["weights"][q], kernels[q])
        sent_a[q] = jnp.concatenate([part, places[q]], axis=0).astype(bf16)
    pl.semaphore_wait(barrier, NV + NB)
    launch(sent_a, got_a, r["sem_a"], "vis", NV, vis_me)
    coef_copy = to_neighbour(r["coef_rows"], r["got_coef"], r["sem_coef"], following)

    sky = staged("sky")
    sides_hi, sides_lo = r["sides_hi"], r["sides_lo"]
    up_hi, up_lo = staged("up_hi"), staged("up_lo")
    coef_copy.wait_recv()
    rows_up = []
    for part in range(2):
        rows = slice(16 * part, 16 * part + 16)
        stack = jnp.concatenate([coef[part], coef[part + 2], r["got_coef"][...]], axis=0)
        rows_up.append(table_by(sides_hi[rows, :], sides_lo[rows, :], stack))
    stack = []
    for n in range(16):
        parts = []
        for field in rows_up:
            for block in ((n + 15) % 16, n):
                parts.append(field[:, 128 * block : 128 * block + 128])
        stack.append(jnp.concatenate(parts, axis=1))
    smooth = by_table(jnp.concatenate(stack, axis=0), up_hi[...], up_lo[...])
    raw = r["raw_here"]
    for n in range(16):
        cols = slice(256 * n, 256 * n + 256)
        raw[:, cols] = sky[:, cols] - smooth[16 * n : 16 * n + 16]
    arrived(got_a, r["sem_a"], NV)

    order, onehot, sent_b, got_b = r["order"], r["onehot"], r["sent_b"], r["got_b"]
    contrib = got_a[:, 0:8, :].astype(f32).reshape(256, 128).astype(bf16)
    where_to = got_a[:, 8:16, :].astype(f32).reshape(256, 128)
    lane = lax.broadcasted_iota(jnp.int32, (256, 128), 1).astype(f32)
    is_imag = lax.broadcasted_iota(jnp.int32, (256, 128), 0) % 2 == 1
    hots = [(where_to == lane + float(128 * g - 256)).astype(f32) for g in range(4)]
    for g in range(4):
        onehot[:, 128 * g : 128 * g + 128] = hots[g].astype(bf16)
    real_hots = [jnp.where(is_imag, 0.0, h).astype(bf16) for h in hots]
    imag_hots = [jnp.where(is_imag, h, 0.0).astype(bf16) for h in hots]
    turned = dot_nt(order[...], contrib).astype(bf16)
    for c, some in ((0, real_hots), (1, imag_hots)):
        for g in range(4):
            grid = dot(turned, some[g]).astype(bf16)
            for low in range(8):
                sent_b[low * 4 + g, c] = grid[16 * low : 16 * low + 16]
    launch(sent_b, got_b, r["sem_b"], "vis", NV, vis_me)
    table_hi, table_lo = staged("table_hi"), staged("table_lo")
    arrived(got_b, r["sem_b"], NV)

    sent_c, got_c = r["sent_c"], r["got_c"]
    spread = jnp.concatenate(
        [got_b[:, 0].reshape(512, 128), got_b[:, 1].reshape(512, 128)], axis=1
    )
    both = dot(table_hi[...], spread) + dot(table_lo[...], spread)
    sent_c[:, 0] = (both[:512, :128] - both[512:, 128:]).astype(bf16).reshape(NV, 16, 128)
    sent_c[:, 1] = (both[512:, :128] + both[:512, 128:]).astype(bf16).reshape(NV, 16, 128)
    launch(sent_c, got_c, r["sem_c"], "vis", NV, vis_me)
    arrived(got_c, r["sem_c"], NV)

    sent_d, got_d = r["sent_d"], r["got_d"]
    for g in range(4):
        values = []
        for low in range(8):
            re = got_c[low * 4 + g, 0].astype(f32)
            im = got_c[low * 4 + g, 1].astype(f32)
            cosine, sine = twist_col[low, 0], twist_col[low, 1]
            values.append((re * cosine - im * sine, re * sine + im * cosine))
        values = small_dft(values, 1.0)
        for b in range(NB):
            for c in range(2):
                sent_d[b, c, :, 128 * g : 128 * g + 128] = values[b][c].astype(sent_d.dtype)
    launch(sent_d, got_d, r["sem_d"], "band", NB, band_me)
    arrived(got_d, r["sem_d"], NB)

    mid, twist_row = r["mid"], r["twist_row"]
    for g in range(4):
        for c in range(2):
            parts = swap_groups(
                [got_d[b, c, :, 128 * g : 128 * g + 128].astype(f32) for b in range(NB)]
            )
            for a in range(8):
                mid[g * 8 + a, c] = parts[a]
    lanes = by_table(
        mid[...].reshape(1024, 128), r["lane_hi"][...], r["lane_lo"][...]
    ).reshape(32, 2, 16, 256)
    extrap = r["extrap"]
    for half in range(2):
        rows = slice(8 * half, 8 * half + 8)
        values = []
        for a in range(32):
            re = lanes[a, 0, rows, :128] - lanes[a, 1, rows, 128:]
            im = lanes[a, 0, rows, 128:] + lanes[a, 1, rows, :128]
            cosine, sine = twist_row[a, 0:1], twist_row[a, 1:2]
            values.append((re * cosine - im * sine, re * sine + im * cosine))
        values = small_dft(values, 1.0)
        for n in range(32):
            cols = slice(128 * n, 128 * n + 128)
            now = jnp.maximum(raw[rows, cols] - values[n][0], 0.0)
            raw[rows, cols] = now
            extrap[rows, cols] = 2.0 * now - sky[rows, cols]
    image_copy = to_neighbour(extrap.at[pl.ds(0, 8)], r["got_rows"], r["sem_rows"], preceding)
    out_image = pltpu.make_async_copy(raw, r["image"], r["sem_out"].at[0])
    out_image.start()

    sent_e, got_e = r["sent_e"], r["got_e"]
    for half in range(2):
        rows = slice(8 * half, 8 * half + 8)
        values = [(extrap[rows, 128 * n : 128 * n + 128], None) for n in range(32)]
        values = small_dft(values, -1.0)
        for a in range(32):
            re, im = values[a]
            cosine, sine = twist_row[a, 0:1], twist_row[a, 1:2]
            if im is None:
                mid[a, 0, rows] = re * cosine
                mid[a, 1, rows] = -re * sine
            else:
                mid[a, 0, rows] = re * cosine + im * sine
                mid[a, 1, rows] = im * cosine - re * sine
    lanes = by_table(
        mid[...].reshape(1024, 128), r["lane_hi"][...], r["lane_lo"][...]
    ).reshape(32, 2, 16, 256)
    for g in range(4):
        for c in range(2):
            parts = []
            for a in range(8):
                re, im = lanes[g * 8 + a, 0], lanes[g * 8 + a, 1]
                if c == 0:
                    parts.append(re[:, :128] + im[:, 128:])
                else:
                    parts.append(im[:, :128] - re[:, 128:])
            parts = swap_groups(parts)
            for b in range(NB):
                sent_e[b, c, :, 128 * g : 128 * g + 128] = parts[b].astype(sent_e.dtype)
    launch(sent_e, got_e, r["sem_e"], "band", NB, band_me)

    down_hi, down_lo = staged("down_hi"), staged("down_lo")
    image_copy.wait_recv()
    fields = jnp.concatenate([extrap[...], r["got_rows"][...]], axis=0)
    fields = table_by(sides_hi[32:48, 0:24], sides_lo[32:48, 0:24], fields)
    stack = []
    for n in range(16):
        if n < 15:
            stack.append(fields[:, 256 * n : 256 * n + 384])
        else:
            stack.append(jnp.concatenate([fields[:, 3840:4096], fields[:, 0:128]], axis=1))
    found = by_table(jnp.concatenate(stack, axis=0), down_hi[...], down_lo[...])
    coeffs = r["coeffs_here"]
    for n in range(16):
        cols = slice(128 * n, 128 * n + 128)
        block = found[16 * n : 16 * n + 16]
        coeffs[0, :, cols] = block[0:8, :128]
        coeffs[1, :, cols] = block[0:8, 128:]
        coeffs[2, :, cols] = block[8:16, :128]
        coeffs[3, :, cols] = block[8:16, 128:]
    abs_total = jnp.sum(jnp.abs(found))
    arrived(got_e, r["sem_e"], NB)

    sent_f, got_f = r["sent_f"], r["got_f"]
    for g in range(4):
        values = []
        for b in range(NB):
            values.append(
                tuple(
                    got_e[b, c, :, 128 * g : 128 * g + 128].astype(f32) for c in range(2)
                )
            )
        values = small_dft(values, -1.0)
        for low in range(8):
            re, im = values[low]
            cosine, sine = twist_col[low, 0], twist_col[low, 1]
            sent_f[low * 4 + g, 0] = (re * cosine + im * sine).astype(sent_f.dtype)
            sent_f[low * 4 + g, 1] = (im * cosine - re * sine).astype(sent_f.dtype)
    launch(sent_f, got_f, r["sem_f"], "vis", NV, vis_me)
    arrived(got_f, r["sem_f"], NV)

    sent_g, got_g = r["sent_g"], r["got_g"]
    spread = jnp.concatenate(
        [got_f[:, 0].reshape(512, 128), got_f[:, 1].reshape(512, 128)], axis=1
    )
    if spread.dtype == f32:
        both = table_by(table_hi[...], table_lo[...], spread)
    else:
        both = dot(table_hi[...], spread) + dot(table_lo[...], spread)
    sent_g[:, 0] = (both[:512, :128] + both[512:, 128:]).astype(bf16).reshape(NV, 16, 128)
    sent_g[:, 1] = (both[:512, 128:] - both[512:, :128]).astype(bf16).reshape(NV, 16, 128)
    launch(sent_g, got_g, r["sem_g"], "vis", NV, vis_me)
    arrived(got_g, r["sem_g"], NV)

    sent_h, got_h = r["sent_h"], r["got_h"]
    picked = []
    for c in range(2):
        total = 0.0
        for g in range(4):
            piece = jnp.concatenate([got_g[low * 4 + g, c] for low in range(8)], axis=0)
            total = total + dot_nt(onehot[:, 128 * g : 128 * g + 128], piece)
        picked.append(total)
    tiles = jnp.where(is_imag, picked[1], picked[0]).astype(bf16)
    tiles = dot(tiles, order[...])
    sent_h[...] = tiles.reshape(NV, 8, 128).astype(bf16)
    launch(sent_h, got_h, r["sem_h"], "vis", NV, vis_me)
    arrived(got_h, r["sem_h"], NV)

    products = jnp.stack([dot_nt(got_h[q], kernels[q]) for q in range(NV)])
    products = jnp.where(wide_lane // 64 == wide_row // 2, products, 0.0)
    products = products[:, :, 0:128] + products[:, :, 128:256]
    products = products + pltpu.roll(products, 64, 2)
    other = pltpu.roll(products, 96, 2)
    row = lax.broadcasted_iota(jnp.int32, (NV, 8, 128), 1)
    products = products + jnp.where(
        row % 2 == 0, -pltpu.roll(other, 7, 1), pltpu.roll(other, 1, 1)
    )
    predicted = products.reshape(256, 128)[:, 0:32]
    residual = live * (vis_state + predicted - vis_data)
    resid_square = jnp.sum(residual * residual)

    sent_t, got_t, sent_u, got_u = r["sent_t"], r["got_t"], r["sent_u"], r["got_u"]
    spot = lax.broadcasted_iota(jnp.int32, (1, 128), 1)
    sent_t[...] = jnp.where(
        spot == 0, abs_total, jnp.where(spot == 1, resid_square, data_square)
    )
    launch(sent_t, got_t, r["sem_t"], "vis", NV, vis_me, same=True)
    arrived(got_t, r["sem_t"], NV)
    sent_u[...] = jnp.sum(got_t[...], axis=0)
    launch(sent_u, got_u, r["sem_u"], "band", NB, band_me, same=True)
    arrived(got_u, r["sem_u"], NB)
    totals = jnp.sum(got_u[...], axis=0)
    abs_total, resid_square, data_square = (
        jnp.sum(jnp.where(spot == n, totals, 0.0), axis=1, keepdims=True) for n in range(3)
    )
    threshold = 0.5 * abs_total / (IMG * IMG)
    for part in range(4):
        limit = jnp.broadcast_to(threshold, (8, 2048))
        coeffs[part] = jnp.maximum(jnp.minimum(coef[part] + coeffs[part], limit), -limit)
    out_coeffs = pltpu.make_async_copy(coeffs, r["coeffs"], r["sem_out"].at[1])
    out_coeffs.start()
    radius = 0.5 * jnp.sqrt(data_square + 1e-06)
    size = jnp.sqrt(resid_square + 1e-06)
    factor = jnp.broadcast_to(1.0 - jnp.minimum(1.0, radius / size), (256, 32))
    r["vis_new"][...] = (residual * factor).reshape(NV, 4, 2, 32)

    for copy in (coef_copy, image_copy):
        copy.wait_send()
    out_image.wait()
    out_coeffs.wait()
    for name, landed, count in (
        ("a", got_a, NV), ("b", got_b, NV), ("c", got_c, NV), ("d", got_d, NB),
        ("e", got_e, NB), ("f", got_f, NV), ("g", got_g, NV), ("h", got_h, NV),
        ("t", got_t, NV), ("u", got_u, NB),
    ):
        drained(landed, r["sem_" + name], count)


STAGED = ["kernels", "coef", "sky", "up_hi", "up_lo", "table_hi", "table_lo", "down_hi", "down_lo"]
INPUTS = STAGED + [
    "vis_state", "vis_data", "rows", "counts", "repeat", "lane_hi", "lane_lo",
    "twist_row", "twists", "order", "sides_hi", "sides_lo",
]
OUTPUTS = ["image", "coeffs", "vis_new"]
VIS_TILE = (NV, 2, 16, 128)
BAND_TILE = (NB, 2, 16, 512)
SCRATCH = dict(
    here_kernels=((NV, 256, 128), bf16),
    here_coef=((4, 8, 2048), f32),
    here_sky=((16, IMG), f32),
    here_up_hi=((512, 256), bf16),
    here_up_lo=((512, 256), bf16),
    here_table_hi=((1024, 512), bf16),
    here_table_lo=((1024, 512), bf16),
    here_down_hi=((384, 256), bf16),
    here_down_lo=((384, 256), bf16),
    sent_a=((NV, 16, 128), bf16), got_a=((NV, 16, 128), bf16),
    sent_b=(VIS_TILE, bf16), got_b=(VIS_TILE, bf16),
    sent_c=(VIS_TILE, bf16), got_c=(VIS_TILE, bf16),
    sent_d=(BAND_TILE, bf16), got_d=(BAND_TILE, bf16),
    sent_e=(BAND_TILE, f32), got_e=(BAND_TILE, f32),
    sent_f=(VIS_TILE, f32), got_f=(VIS_TILE, f32),
    sent_g=(VIS_TILE, bf16), got_g=(VIS_TILE, bf16),
    sent_h=((NV, 8, 128), bf16), got_h=((NV, 8, 128), bf16),
    sent_t=((1, 128), f32), got_t=((NV, 1, 128), f32),
    sent_u=((1, 128), f32), got_u=((NB, 1, 128), f32),
    weights=((NV, 8, 256), bf16), twist_col=((8, 2, 16, 128), f32), coef_rows=((16, 2048), f32),
    got_coef=((16, 2048), f32), got_rows=((8, IMG), f32),
    raw_here=((16, IMG), f32), extrap=((16, IMG), f32), coeffs_here=((4, 8, 2048), f32),
    onehot=((256, 512), bf16), mid=((32, 2, 16, 128), f32),
    **{"sem_" + n: 2 for n in list("abcdefghtu") + ["coef", "rows", "out"]},
    sem_in=len(STAGED),
)


def step(inputs):
    anywhere = pl.BlockSpec(memory_space=pl.ANY)
    vmem = pl.BlockSpec(memory_space=pltpu.VMEM)
    scratch = []
    for what in SCRATCH.values():
        if isinstance(what, int):
            scratch.append(pltpu.SemaphoreType.DMA((what,)))
        else:
            scratch.append(pltpu.VMEM(*what))
    return pl.pallas_call(
        step_kernel,
        out_shape=(
            jax.ShapeDtypeStruct((16, IMG), f32),
            jax.ShapeDtypeStruct((4, 8, 2048), f32),
            jax.ShapeDtypeStruct((NV, 4, 2, 32), f32),
        ),
        in_specs=[anywhere if name in STAGED else vmem for name in INPUTS],
        out_specs=(anywhere, anywhere, vmem),
        scratch_shapes=scratch,
        compiler_params=pltpu.CompilerParams(
            collective_id=0, has_side_effects=True, vmem_limit_bytes=56 * 2**20
        ),
    )(*[inputs[name] for name in INPUTS])


def local(sky_image, coef_dual, vis_dual, visibilities, kernel_blocks, tile_rows, tile_counts):
    names = (
        "table_hi", "table_lo", "lane_hi", "lane_lo",
        "up_hi", "up_lo", "down_hi", "down_lo", "sides_hi", "sides_lo",
    )
    inputs = dict(zip(names, dft512_tables() + dft128_tables() + wavelet_tables()))
    inputs.update(
        twist_row=row_twist(), twists=col_twist(), order=lane_order(), repeat=repeat_table()
    )
    inputs = {name: jnp.asarray(table) for name, table in inputs.items()}
    inputs.update(
        kernels=kernel_blocks.reshape(NV, 256, 128),
        coef=coef_dual,
        sky=sky_image,
        vis_state=vis_dual.reshape(NV, 4, 2, 32),
        vis_data=visibilities.reshape(NV, 4, 2, 32),
        rows=tile_rows.reshape(NV, 4).T,
        counts=tile_counts.reshape(1, NV),
    )
    image, coeffs, vis_new = step(inputs)
    return (image, coeffs, vis_new.reshape(1, 1, NV, 4, 2, 32))


def solution(mesh):
    return jax.shard_map(
        local,
        mesh=mesh,
        in_specs=(
            P(("band", "vis"), None),
            P(None, ("band", "vis"), None),
            P("band", "vis", None, None, None, None),
            P("band", "vis", None, None, None, None),
            P("band", "vis", None, None, None, None, None),
            P("band", "vis", None, None),
            P("band", "vis", None),
        ),
        out_specs=(
            P(("band", "vis"), None),
            P(None, ("band", "vis"), None),
            P("band", "vis", None, None, None, None),
        ),
        check_vma=False,
    )
```

```python
import functools
import math

import jax
import jax.numpy as jnp
import numpy as np
from jax import lax
from jax.experimental import pallas as pl
from jax.experimental.pallas import tpu as pltpu
from jax.sharding import PartitionSpec as P

IMG = 4096
NB = 8
NV = 32
MESH_ID = pl.DeviceIdType.MESH
f32 = jnp.float32
bf16 = jnp.bfloat16

low_taps = (
    -0.010597401784997278,
    0.032883011666982945,
    0.030841381835986965,
    -0.18703481171888114,
    -0.02798376941698385,
    0.6308807679295904,
    0.7148465705525415,
    0.23037781330885523,
)
high_taps = tuple(((-1.0) ** offset * low_taps[7 - offset] for offset in range(8)))


def halves_of(table):
    high = table.astype(bf16)
    low = (table - high.astype(np.float64)).astype(bf16)
    return high, low


def dft512_tables():
    index = np.arange(512).reshape(32, 2, 8).transpose(1, 0, 2).reshape(512)
    angle = 2.0 * np.pi / 512 * (index[:, None] * index[None, :] % 512)
    return halves_of(np.concatenate([np.cos(angle), np.sin(angle)], axis=0))


def dft128_tables():
    index = np.arange(128)
    angle = 2.0 * np.pi / 128 * (index[:, None] * index[None, :] % 128)
    return halves_of(np.concatenate([np.cos(angle), np.sin(angle)], axis=1) / IMG)


def row_twist():
    angle = 2.0 * np.pi / IMG * (np.arange(32)[:, None] * np.arange(128)[None, :] % IMG)
    return np.stack([np.cos(angle), np.sin(angle)], axis=1).astype(np.float32)


def col_twist():
    low, row = np.arange(8)[None, :, None], np.arange(16)[None, None, :]
    angle = 2.0 * np.pi / IMG * (low * (16 * np.arange(NV)[:, None, None] + row))
    return np.stack([np.cos(angle), np.sin(angle)], axis=1).reshape(NV, 2, 128).astype(np.float32)


def repeat_table():
    return np.tile(np.eye(32), (1, 8)).astype(bf16)


def wavelet_tables():
    up = np.zeros((512, 256))
    down = np.zeros((384, 256))
    rows_up = np.zeros((2, 16, 32))
    rows_down = np.zeros((16, 24))
    for tap in range(8):
        for side, taps in ((0, low_taps), (1, high_taps)):
            for k in range(128):
                down[2 * k + tap, 128 * side + k] = taps[tap]
            for k in range(-128, 128):
                if 0 <= 2 * k + tap < 256:
                    up[256 * side + 128 + k, 2 * k + tap] = taps[tap]
            for k in range(8):
                rows_down[8 * side + k, 2 * k + tap] = taps[tap]
            for k in range(-3, 8):
                if 0 <= 2 * k + tap < 16:
                    for part in range(2):
                        spot = 8 * side + k if k >= 0 else 16 + 3 * (part + 2 * side) + k + 3
                        rows_up[part, 2 * k + tap, spot] = taps[tap]
    sides = np.zeros((48, 32))
    sides[0:32] = rows_up.reshape(32, 32)
    sides[32:48, 0:24] = rows_down
    return tuple(part for table in (up, down, sides) for part in halves_of(table))


def lane_order():
    place = np.zeros((128, 128), np.float32)
    for t in range(128):
        place[t // 64 * 64 + (t % 8) * 8 + t // 8 % 8, t] = 1.0
    return place.astype(bf16)


def times(pair, cosine, sine):
    re, im = pair
    if abs(sine) < 1e-12:
        if cosine > 0:
            return pair
        return (-re, None if im is None else -im)
    if abs(cosine) < 1e-12:
        if im is None:
            return (None, re if sine > 0 else -re)
        return (-im, re) if sine > 0 else (im, -re)
    cosine, sine = np.float32(cosine), np.float32(sine)
    if im is None:
        return (re * cosine, re * sine)
    return (re * cosine - im * sine, re * sine + im * cosine)


def plus(a, b):
    if a is None:
        return b
    return a if b is None else a + b


def minus(a, b):
    if b is None:
        return a
    return -b if a is None else a - b


def small_dft(values, sign):
    count = len(values)
    if count == 1:
        return values
    even = small_dft(values[0::2], sign)
    odd = small_dft(values[1::2], sign)
    out = [None] * count
    for k in range(count // 2):
        angle = sign * 2.0 * math.pi * k / count
        turned = times(odd[k], math.cos(angle), math.sin(angle))
        out[k] = (plus(even[k][0], turned[0]), plus(even[k][1], turned[1]))
        out[k + count // 2] = (minus(even[k][0], turned[0]), minus(even[k][1], turned[1]))
    return out


def swap_groups(arrays):
    arrays = list(arrays)
    lane = lax.broadcasted_iota(jnp.int32, arrays[0].shape, arrays[0].ndim - 1)
    axis = arrays[0].ndim - 1
    for bit in range(3):
        shift = 16 << bit
        upper = (lane // shift) % 2 == 1
        for j in range(8):
            other = j | (1 << bit)
            if other == j:
                continue
            low, high = arrays[j], arrays[other]
            arrays[j] = jnp.where(upper, pltpu.roll(high, shift, axis), low)
            arrays[other] = jnp.where(upper, high, pltpu.roll(low, 128 - shift, axis))
    return arrays


def dot(a, b):
    return jnp.dot(a, b, preferred_element_type=f32)


def dot_nt(a, b):
    return lax.dot_general(a, b, (((1,), (1,)), ((), ())), preferred_element_type=f32)


def halves(value):
    high = value.astype(bf16)
    return high, (value - high.astype(f32)).astype(bf16)


def by_table(value, high, low):
    value_high, value_low = halves(value)
    return dot(value_high, high) + dot(value_low, high) + dot(value_high, low)


def table_by(high, low, value):
    value_high, value_low = halves(value)
    return dot(high, value_high) + dot(high, value_low) + dot(low, value_high)


def greet(vis_me, band_me, neighbours):
    barrier = pltpu.get_barrier_semaphore()

    def vis_signal(d, carry):
        pl.semaphore_signal(
            barrier, inc=1, device_id={"vis": vis_me ^ d}, device_id_type=MESH_ID
        )
        return carry

    def band_signal(d, carry):
        pl.semaphore_signal(
            barrier, inc=1, device_id={"band": band_me ^ d}, device_id_type=MESH_ID
        )
        return carry

    for neighbour in neighbours:
        pl.semaphore_signal(barrier, inc=1, device_id=neighbour, device_id_type=MESH_ID)
    lax.fori_loop(1, NV, vis_signal, 0)
    lax.fori_loop(1, NB, band_signal, 0)
    return barrier


def launch(r, name, part, axis, count, me, same=False):
    sent, landed, sems = r["sent_" + name], r["got_" + name].at[part], r["sem_" + name]
    if not same:
        sent = sent.at[part]

    def body(d, carry):
        peer = me ^ d
        pltpu.make_async_remote_copy(
            src_ref=sent if same else sent.at[peer],
            dst_ref=landed.at[me],
            send_sem=sems.at[2 * part],
            recv_sem=sems.at[2 * part + 1],
            device_id={axis: peer},
            device_id_type=MESH_ID,
        ).start()
        return carry

    lax.fori_loop(1, count, body, 0)
    landed[me] = sent[...] if same else sent[me]


def to_neighbour(sent, landed, sems, neighbour):
    copy = pltpu.make_async_remote_copy(
        src_ref=sent,
        dst_ref=landed,
        send_sem=sems.at[0],
        recv_sem=sems.at[1],
        device_id=neighbour,
        device_id_type=MESH_ID,
    )
    copy.start()
    return copy


def finish(r, name, part, count, side):
    landed = r["got_" + name].at[part]
    landed = landed.at[pl.ds(0, count - 1)]
    pltpu.make_async_copy(landed, landed, r["sem_" + name].at[2 * part + side]).wait()


def arrived(r, name, part, count):
    finish(r, name, part, count, 1)
    return r["got_" + name].at[part]


def step_kernel(*refs):
    names = INPUTS + OUTPUTS + list(SCRATCH)
    r = dict(zip(names, refs))
    vis_me, band_me = lax.axis_index("vis"), lax.axis_index("band")
    me = band_me * NV + vis_me
    following = (me + 1) % (NB * NV)
    preceding = (me + NB * NV - 1) % (NB * NV)
    following = {"band": following // NV, "vis": following % NV}
    preceding = {"band": preceding // NV, "vis": preceding % NV}
    copies = {}
    for place, name in enumerate(STAGED):
        copies[name] = pltpu.make_async_copy(r[name], r["here_" + name], r["sem_in"].at[place])
        copies[name].start()

    def staged(name):
        if name in copies:
            copies.pop(name).wait()
        return r["here_" + name]

    barrier = greet(vis_me, band_me, (following, preceding))

    to_row = (
        lax.broadcasted_iota(jnp.int32, (256, 32), 0) // 8
        == lax.broadcasted_iota(jnp.int32, (256, 32), 1)
    ).astype(f32).astype(bf16)
    column = r["rows"][...]
    facts = jnp.concatenate(
        [column % 32 * 16 + column // 32 - 256, r["counts"][...], jnp.zeros((3, 32), jnp.int32)],
        axis=0,
    ).astype(f32).astype(bf16)
    facts = dot_nt(to_row, facts)
    slot_here = lax.broadcasted_iota(jnp.int32, (256, 8), 0) % 8 // 2
    fact = lax.broadcasted_iota(jnp.int32, (256, 8), 1)
    place = jnp.sum(jnp.where(fact == slot_here, facts, 0.0), axis=1, keepdims=True)
    count = jnp.sum(jnp.where(fact == 4, facts, 0.0), axis=1, keepdims=True)
    places = jnp.broadcast_to(place, (256, 128)).reshape(NV, 8, 128)
    live = jnp.broadcast_to(count, (256, 32)) > (
        lax.broadcasted_iota(jnp.int32, (256, 32), 0) % 8 // 2
    ).astype(f32)
    live = jnp.where(live, 1.0, 0.0)
    vis_state = r["vis_state"][...].reshape(256, 32)
    vis_data = r["vis_data"][...].reshape(256, 32)
    data_square = jnp.sum(live * vis_data * vis_data)

    weights = dot((live * vis_state).astype(bf16), r["repeat"][...]).reshape(NV, 8, 256)
    wide_row = lax.broadcasted_iota(jnp.int32, (NV, 8, 256), 1)
    wide_lane = lax.broadcasted_iota(jnp.int32, (NV, 8, 256), 2)
    crossed = jnp.where(
        wide_row % 2 == 0, pltpu.roll(weights, 7, 1), -pltpu.roll(weights, 1, 1)
    )
    weights = jnp.where(wide_lane // 32 % 2 == 0, weights, crossed)
    r["weights"][...] = jnp.where(wide_lane // 64 == wide_row // 2, weights, 0.0).astype(bf16)
    twist_col = r["twist_col"]
    eye = (
        lax.broadcasted_iota(jnp.int32, (128, 128), 0)
        == lax.broadcasted_iota(jnp.int32, (128, 128), 1)
    )
    for c in range(2):
        one = jnp.broadcast_to(r["twists"][vis_me, c : c + 1, :], (128, 128))
        one = jnp.sum(jnp.where(eye, one, 0.0), axis=1, keepdims=True)
        twist_col[:, c] = jnp.broadcast_to(one, (128, 128)).reshape(8, 16, 128)

    sent_a = r["sent_a"].at[0]
    coef = staged("coef")
    for part in range(4):
        r["coef_rows"][3 * part : 3 * part + 3] = coef[part, 5:8, :]
    r["coef_rows"][12:16] = jnp.zeros((4, 2048), f32)
    kernels = staged("kernels")
    for q in range(NV):
        part = dot(r["weights"][q], kernels[q])
        sent_a[q] = jnp.concatenate([part, places[q]], axis=0).astype(bf16)
    pl.semaphore_wait(barrier, NV + NB)
    launch(r, "a", 0, "vis", NV, vis_me)
    coef_copy = to_neighbour(r["coef_rows"], r["got_coef"], r["sem_coef"], following)

    sky = staged("sky")
    sides_hi, sides_lo = r["sides_hi"], r["sides_lo"]
    up_hi, up_lo = staged("up_hi"), staged("up_lo")
    coef_copy.wait_recv()
    rows_up = []
    for part in range(2):
        rows = slice(16 * part, 16 * part + 16)
        stack = jnp.concatenate([coef[part], coef[part + 2], r["got_coef"][...]], axis=0)
        rows_up.append(table_by(sides_hi[rows, :], sides_lo[rows, :], stack))
    stack = []
    for n in range(16):
        parts = []
        for field in rows_up:
            for block in ((n + 15) % 16, n):
                parts.append(field[:, 128 * block : 128 * block + 128])
        stack.append(jnp.concatenate(parts, axis=1))
    smooth = by_table(jnp.concatenate(stack, axis=0), up_hi[...], up_lo[...])
    raw = r["raw_here"]
    for n in range(16):
        cols = slice(256 * n, 256 * n + 256)
        raw[:, cols] = sky[:, cols] - smooth[16 * n : 16 * n + 16]
    got_a = arrived(r, "a", 0, NV)

    order, onehot = r["order"], r["onehot"]
    contrib = got_a[:, 0:8, :].astype(f32).reshape(256, 128).astype(bf16)
    where_to = got_a[:, 8:16, :].astype(f32).reshape(256, 128)
    lane = lax.broadcasted_iota(jnp.int32, (256, 128), 1).astype(f32)
    is_imag = lax.broadcasted_iota(jnp.int32, (256, 128), 0) % 2 == 1
    hots = [(where_to == lane + float(128 * g - 256)).astype(f32) for g in range(4)]
    for g in range(4):
        onehot[:, 128 * g : 128 * g + 128] = hots[g].astype(bf16)
    real_hots = [jnp.where(is_imag, 0.0, h).astype(bf16) for h in hots]
    imag_hots = [jnp.where(is_imag, h, 0.0).astype(bf16) for h in hots]
    hots = jnp.concatenate(real_hots + imag_hots, axis=1)
    turned = dot_nt(order[...], contrib).astype(bf16)
    for part in range(2):
        grid = dot(turned[64 * part : 64 * part + 64], hots)
        for c in range(2):
            for g in range(4):
                cols = slice(512 * c + 128 * g, 512 * c + 128 * g + 128)
                for low in range(8):
                    r["sent_b"][part, low * 4 + g, c] = grid[
                        8 * low : 8 * low + 8, cols
                    ].astype(bf16)
        launch(r, "b", part, "vis", NV, vis_me)

    table_hi, table_lo = staged("table_hi"), staged("table_lo")

    def spread_of(landed):
        return jnp.concatenate(
            [landed[:, 0].reshape(256, 128), landed[:, 1].reshape(256, 128)], axis=1
        )

    first = spread_of(arrived(r, "b", 0, NV))
    ahead = dot(table_hi[:, 0:256], first) + dot(table_lo[:, 0:256], first)
    second = spread_of(arrived(r, "b", 1, NV))
    for part in range(2):
        both = []
        for side in range(2):
            rows = slice(512 * side + 256 * part, 512 * side + 256 * part + 256)
            both.append(
                ahead[rows] + dot(table_hi[rows, 256:512], second)
                + dot(table_lo[rows, 256:512], second)
            )
        re = both[0][:, :128] - both[1][:, 128:]
        im = both[1][:, :128] + both[0][:, 128:]
        r["sent_c"][part, :, 0] = re.reshape(NV, 8, 128).astype(bf16)
        r["sent_c"][part, :, 1] = im.reshape(NV, 8, 128).astype(bf16)
        launch(r, "c", part, "vis", NV, vis_me)

    sent_d = r["sent_d"]
    for part in range(2):
        got_c = arrived(r, "c", part, NV)
        rows = slice(8 * part, 8 * part + 8)
        for g in range(4):
            values = []
            for low in range(8):
                re = got_c[low * 4 + g, 0].astype(f32)
                im = got_c[low * 4 + g, 1].astype(f32)
                cosine, sine = twist_col[low, 0, rows], twist_col[low, 1, rows]
                values.append((re * cosine - im * sine, re * sine + im * cosine))
            values = small_dft(values, 1.0)
            for b in range(NB):
                for c in range(2):
                    sent_d[part, b, c, :, 128 * g : 128 * g + 128] = values[b][c].astype(
                        sent_d.dtype
                    )
        launch(r, "d", part, "band", NB, band_me)

    mid, twist_row, extrap, sent_e = r["mid"], r["twist_row"], r["extrap"], r["sent_e"]

    def lane_product(part):
        return by_table(
            mid[part].reshape(512, 128), r["lane_hi"][...], r["lane_lo"][...]
        ).reshape(32, 2, 8, 256)

    for part in range(2):
        rows = slice(8 * part, 8 * part + 8)
        got_d = arrived(r, "d", part, NB)
        for g in range(4):
            for c in range(2):
                parts = swap_groups(
                    [got_d[b, c, :, 128 * g : 128 * g + 128].astype(f32) for b in range(NB)]
                )
                for a in range(8):
                    mid[part, g * 8 + a, c] = parts[a]
        lanes = lane_product(part)
        values = []
        for a in range(32):
            re = lanes[a, 0, :, :128] - lanes[a, 1, :, 128:]
            im = lanes[a, 0, :, 128:] + lanes[a, 1, :, :128]
            cosine, sine = twist_row[a, 0:1], twist_row[a, 1:2]
            values.append((re * cosine - im * sine, re * sine + im * cosine))
        values = small_dft(values, 1.0)
        for n in range(32):
            cols = slice(128 * n, 128 * n + 128)
            now = jnp.maximum(raw[rows, cols] - values[n][0], 0.0)
            raw[rows, cols] = now
            extrap[part, :, cols] = 2.0 * now - sky[rows, cols]
        if part == 0:
            image_copy = to_neighbour(extrap.at[0], r["got_rows"], r["sem_rows"], preceding)
        values = [(extrap[part, :, 128 * n : 128 * n + 128], None) for n in range(32)]
        values = small_dft(values, -1.0)
        for a in range(32):
            re, im = values[a]
            cosine, sine = twist_row[a, 0:1], twist_row[a, 1:2]
            if im is None:
                mid[part, a, 0] = re * cosine
                mid[part, a, 1] = -re * sine
            else:
                mid[part, a, 0] = re * cosine + im * sine
                mid[part, a, 1] = im * cosine - re * sine
        lanes = lane_product(part)
        for g in range(4):
            for c in range(2):
                parts = []
                for a in range(8):
                    re, im = lanes[g * 8 + a, 0], lanes[g * 8 + a, 1]
                    if c == 0:
                        parts.append(re[:, :128] + im[:, 128:])
                    else:
                        parts.append(im[:, :128] - re[:, 128:])
                parts = swap_groups(parts)
                for b in range(NB):
                    sent_e[part, b, c, :, 128 * g : 128 * g + 128] = parts[b]
        launch(r, "e", part, "band", NB, band_me)
    out_image = pltpu.make_async_copy(raw, r["image"], r["sem_out"].at[0])
    out_image.start()

    sent_f = r["sent_f"]
    for part in range(2):
        got_e = arrived(r, "e", part, NB)
        rows = slice(8 * part, 8 * part + 8)
        for g in range(4):
            values = []
            for b in range(NB):
                values.append(
                    tuple(got_e[b, c, :, 128 * g : 128 * g + 128] for c in range(2))
                )
            values = small_dft(values, -1.0)
            for low in range(8):
                re, im = values[low]
                cosine, sine = twist_col[low, 0, rows], twist_col[low, 1, rows]
                sent_f[part, low * 4 + g, 0] = (re * cosine + im * sine).astype(sent_f.dtype)
                sent_f[part, low * 4 + g, 1] = (im * cosine - re * sine).astype(sent_f.dtype)
        launch(r, "f", part, "vis", NV, vis_me)

    down_hi, down_lo = staged("down_hi"), staged("down_lo")
    image_copy.wait_recv()
    fields = jnp.concatenate([extrap[0], extrap[1], r["got_rows"][...]], axis=0)
    fields = table_by(sides_hi[32:48, 0:24], sides_lo[32:48, 0:24], fields)
    stack = []
    for n in range(16):
        if n < 15:
            stack.append(fields[:, 256 * n : 256 * n + 384])
        else:
            stack.append(jnp.concatenate([fields[:, 3840:4096], fields[:, 0:128]], axis=1))
    found = by_table(jnp.concatenate(stack, axis=0), down_hi[...], down_lo[...])
    coeffs = r["coeffs_here"]
    for n in range(16):
        cols = slice(128 * n, 128 * n + 128)
        block = found[16 * n : 16 * n + 16]
        coeffs[0, :, cols] = block[0:8, :128]
        coeffs[1, :, cols] = block[0:8, 128:]
        coeffs[2, :, cols] = block[8:16, :128]
        coeffs[3, :, cols] = block[8:16, 128:]
    abs_total = jnp.sum(jnp.abs(found))

    def through(rows, cols, spread):
        if spread.dtype == f32:
            return table_by(table_hi[rows, cols], table_lo[rows, cols], spread)
        return dot(table_hi[rows, cols], spread) + dot(table_lo[rows, cols], spread)

    first = spread_of(arrived(r, "f", 0, NV))
    ahead = through(slice(0, 1024), slice(0, 256), first)
    second = spread_of(arrived(r, "f", 1, NV))
    for part in range(2):
        both = []
        for side in range(2):
            rows = slice(512 * side + 256 * part, 512 * side + 256 * part + 256)
            both.append(ahead[rows] + through(rows, slice(256, 512), second))
        re = both[0][:, :128] + both[1][:, 128:]
        im = both[0][:, 128:] - both[1][:, :128]
        r["sent_g"][part, :, 0] = re.reshape(NV, 8, 128).astype(bf16)
        r["sent_g"][part, :, 1] = im.reshape(NV, 8, 128).astype(bf16)
        launch(r, "g", part, "vis", NV, vis_me)

    picked = [[], []]
    for part in range(2):
        got_g = arrived(r, "g", part, NV)
        for c in range(2):
            total = 0.0
            for g in range(4):
                piece = jnp.concatenate(
                    [got_g[low * 4 + g, c].astype(f32) for low in range(8)], axis=0
                ).astype(bf16)
                total = total + dot_nt(onehot[:, 128 * g : 128 * g + 128], piece)
            picked[c].append(total)
    picked = [jnp.concatenate(p, axis=1) for p in picked]
    tiles = jnp.where(is_imag, picked[1], picked[0]).astype(bf16)
    tiles = dot(tiles, order[...])
    r["sent_h"][0] = tiles.reshape(NV, 8, 128).astype(bf16)
    launch(r, "h", 0, "vis", NV, vis_me)
    got_h = arrived(r, "h", 0, NV)

    products = jnp.stack([dot_nt(got_h[q], kernels[q]) for q in range(NV)])
    products = jnp.where(wide_lane // 64 == wide_row // 2, products, 0.0)
    products = products[:, :, 0:128] + products[:, :, 128:256]
    products = products + pltpu.roll(products, 64, 2)
    other = pltpu.roll(products, 96, 2)
    row = lax.broadcasted_iota(jnp.int32, (NV, 8, 128), 1)
    products = products + jnp.where(
        row % 2 == 0, -pltpu.roll(other, 7, 1), pltpu.roll(other, 1, 1)
    )
    predicted = products.reshape(256, 128)[:, 0:32]
    residual = live * (vis_state + predicted - vis_data)
    resid_square = jnp.sum(residual * residual)

    sent_t, sent_u = r["sent_t"], r["sent_u"]
    spot = lax.broadcasted_iota(jnp.int32, (1, 128), 1)
    sent_t[...] = jnp.where(
        spot == 0, abs_total, jnp.where(spot == 1, resid_square, data_square)
    )
    launch(r, "t", 0, "vis", NV, vis_me, same=True)
    sent_u[...] = jnp.sum(arrived(r, "t", 0, NV)[...], axis=0)
    launch(r, "u", 0, "band", NB, band_me, same=True)
    totals = jnp.sum(arrived(r, "u", 0, NB)[...], axis=0)
    abs_total, resid_square, data_square = (
        jnp.sum(jnp.where(spot == n, totals, 0.0), axis=1, keepdims=True) for n in range(3)
    )
    threshold = 0.5 * abs_total / (IMG * IMG)
    for part in range(4):
        limit = jnp.broadcast_to(threshold, (8, 2048))
        coeffs[part] = jnp.maximum(jnp.minimum(coef[part] + coeffs[part], limit), -limit)
    out_coeffs = pltpu.make_async_copy(coeffs, r["coeffs"], r["sem_out"].at[1])
    out_coeffs.start()
    radius = 0.5 * jnp.sqrt(data_square + 1e-06)
    size = jnp.sqrt(resid_square + 1e-06)
    factor = jnp.broadcast_to(1.0 - jnp.minimum(1.0, radius / size), (256, 32))
    r["vis_new"][...] = (residual * factor).reshape(NV, 4, 2, 32)

    for copy in (coef_copy, image_copy):
        copy.wait_send()
    out_image.wait()
    out_coeffs.wait()
    for name in "abcdefghtu":
        for part in range(2 if name in "bcdefg" else 1):
            finish(r, name, part, NB if name in "deu" else NV, 0)


STAGED = ["kernels", "coef", "sky", "up_hi", "up_lo", "table_hi", "table_lo", "down_hi", "down_lo"]
INPUTS = STAGED + [
    "vis_state", "vis_data", "rows", "counts", "repeat", "lane_hi", "lane_lo",
    "twist_row", "twists", "order", "sides_hi", "sides_lo",
]
OUTPUTS = ["image", "coeffs", "vis_new"]
VIS_TILE = (2, NV, 2, 8, 128)
BAND_TILE = (2, NB, 2, 8, 512)
SCRATCH = dict(
    here_kernels=((NV, 256, 128), bf16),
    here_coef=((4, 8, 2048), f32),
    here_sky=((16, IMG), f32),
    here_up_hi=((512, 256), bf16),
    here_up_lo=((512, 256), bf16),
    here_table_hi=((1024, 512), bf16),
    here_table_lo=((1024, 512), bf16),
    here_down_hi=((384, 256), bf16),
    here_down_lo=((384, 256), bf16),
    sent_a=((1, NV, 16, 128), bf16), got_a=((1, NV, 16, 128), bf16),
    sent_b=(VIS_TILE, bf16), got_b=(VIS_TILE, bf16),
    sent_c=(VIS_TILE, bf16), got_c=(VIS_TILE, bf16),
    sent_d=(BAND_TILE, bf16), got_d=(BAND_TILE, bf16),
    sent_e=(BAND_TILE, f32), got_e=(BAND_TILE, f32),
    sent_f=(VIS_TILE, f32), got_f=(VIS_TILE, f32),
    sent_g=(VIS_TILE, bf16), got_g=(VIS_TILE, bf16),
    sent_h=((1, NV, 8, 128), bf16), got_h=((1, NV, 8, 128), bf16),
    sent_t=((1, 128), f32), got_t=((1, NV, 1, 128), f32),
    sent_u=((1, 128), f32), got_u=((1, NB, 1, 128), f32),
    weights=((NV, 8, 256), bf16), twist_col=((8, 2, 16, 128), f32), coef_rows=((16, 2048), f32),
    got_coef=((16, 2048), f32), got_rows=((8, IMG), f32),
    raw_here=((16, IMG), f32), extrap=((2, 8, IMG), f32), coeffs_here=((4, 8, 2048), f32),
    onehot=((256, 512), bf16), mid=((2, 32, 2, 8, 128), f32),
    **{"sem_" + n: 4 for n in list("abcdefghtu") + ["coef", "rows", "out"]},
    sem_in=len(STAGED),
)


def step(inputs):
    anywhere = pl.BlockSpec(memory_space=pl.ANY)
    vmem = pl.BlockSpec(memory_space=pltpu.VMEM)
    scratch = []
    for what in SCRATCH.values():
        if isinstance(what, int):
            scratch.append(pltpu.SemaphoreType.DMA((what,)))
        else:
            scratch.append(pltpu.VMEM(*what))
    return pl.pallas_call(
        step_kernel,
        out_shape=(
            jax.ShapeDtypeStruct((16, IMG), f32),
            jax.ShapeDtypeStruct((4, 8, 2048), f32),
            jax.ShapeDtypeStruct((NV, 4, 2, 32), f32),
        ),
        in_specs=[anywhere if name in STAGED else vmem for name in INPUTS],
        out_specs=(anywhere, anywhere, vmem),
        scratch_shapes=scratch,
        compiler_params=pltpu.CompilerParams(
            collective_id=0, has_side_effects=True, vmem_limit_bytes=56 * 2**20
        ),
    )(*[inputs[name] for name in INPUTS])


def local(sky_image, coef_dual, vis_dual, visibilities, kernel_blocks, tile_rows, tile_counts):
    names = (
        "table_hi", "table_lo", "lane_hi", "lane_lo",
        "up_hi", "up_lo", "down_hi", "down_lo", "sides_hi", "sides_lo",
    )
    inputs = dict(zip(names, dft512_tables() + dft128_tables() + wavelet_tables()))
    inputs.update(
        twist_row=row_twist(), twists=col_twist(), order=lane_order(), repeat=repeat_table()
    )
    inputs = {name: jnp.asarray(table) for name, table in inputs.items()}
    inputs.update(
        kernels=kernel_blocks.reshape(NV, 256, 128),
        coef=coef_dual,
        sky=sky_image,
        vis_state=vis_dual.reshape(NV, 4, 2, 32),
        vis_data=visibilities.reshape(NV, 4, 2, 32),
        rows=tile_rows.reshape(NV, 4).T,
        counts=tile_counts.reshape(1, NV),
    )
    image, coeffs, vis_new = step(inputs)
    return (image, coeffs, vis_new.reshape(1, 1, NV, 4, 2, 32))


def solution(mesh):
    return jax.shard_map(
        local,
        mesh=mesh,
        in_specs=(
            P(("band", "vis"), None),
            P(None, ("band", "vis"), None),
            P("band", "vis", None, None, None, None),
            P("band", "vis", None, None, None, None),
            P("band", "vis", None, None, None, None, None),
            P("band", "vis", None, None),
            P("band", "vis", None),
        ),
        out_specs=(
            P(("band", "vis"), None),
            P(None, ("band", "vis"), None),
            P("band", "vis", None, None, None, None),
        ),
        check_vma=False,
    )
```

```python
import functools
import math

import jax
import jax.numpy as jnp
import numpy as np
from jax import lax
from jax.experimental import pallas as pl
from jax.experimental.pallas import tpu as pltpu
from jax.sharding import PartitionSpec as P

IMG = 4096
NB = 8
NV = 32
MESH_ID = pl.DeviceIdType.MESH
f32 = jnp.float32
bf16 = jnp.bfloat16

low_taps = (
    -0.010597401784997278,
    0.032883011666982945,
    0.030841381835986965,
    -0.18703481171888114,
    -0.02798376941698385,
    0.6308807679295904,
    0.7148465705525415,
    0.23037781330885523,
)
high_taps = tuple(((-1.0) ** offset * low_taps[7 - offset] for offset in range(8)))


def halves_of(table):
    high = table.astype(bf16)
    low = (table - high.astype(np.float64)).astype(bf16)
    return high, low


def dft512_tables():
    index = np.arange(512).reshape(32, 2, 8).transpose(1, 0, 2).reshape(512)
    angle = 2.0 * np.pi / 512 * (index[:, None] * index[None, :] % 512)
    return halves_of(np.concatenate([np.cos(angle), np.sin(angle)], axis=0))


def dft128_tables():
    index = np.arange(128)
    angle = 2.0 * np.pi / 128 * (index[:, None] * index[None, :] % 128)
    return halves_of(np.concatenate([np.cos(angle), np.sin(angle)], axis=1) / IMG)


def row_twist():
    angle = 2.0 * np.pi / IMG * (np.arange(32)[:, None] * np.arange(128)[None, :] % IMG)
    return np.stack([np.cos(angle), np.sin(angle)], axis=1).astype(np.float32)


def col_twist():
    low, row = np.arange(8)[None, :, None], np.arange(16)[None, None, :]
    angle = 2.0 * np.pi / IMG * (low * (16 * np.arange(NV)[:, None, None] + row))
    return np.stack([np.cos(angle), np.sin(angle)], axis=1).reshape(NV, 2, 128).astype(np.float32)


def repeat_table():
    return np.tile(np.eye(32), (1, 8)).astype(bf16)


def wavelet_tables():
    up = np.zeros((512, 256))
    down = np.zeros((384, 256))
    rows_up = np.zeros((2, 16, 32))
    rows_down = np.zeros((16, 24))
    for tap in range(8):
        for side, taps in ((0, low_taps), (1, high_taps)):
            for k in range(128):
                down[2 * k + tap, 128 * side + k] = taps[tap]
            for k in range(-128, 128):
                if 0 <= 2 * k + tap < 256:
                    up[256 * side + 128 + k, 2 * k + tap] = taps[tap]
            for k in range(8):
                rows_down[8 * side + k, 2 * k + tap] = taps[tap]
            for k in range(-3, 8):
                if 0 <= 2 * k + tap < 16:
                    for part in range(2):
                        spot = 8 * side + k if k >= 0 else 16 + 3 * (part + 2 * side) + k + 3
                        rows_up[part, 2 * k + tap, spot] = taps[tap]
    sides = np.zeros((48, 32))
    sides[0:32] = rows_up.reshape(32, 32)
    sides[32:48, 0:24] = rows_down
    return tuple(part for table in (up, down, sides) for part in halves_of(table))


def lane_order():
    place = np.zeros((128, 128), np.float32)
    for t in range(128):
        place[t // 64 * 64 + (t % 8) * 8 + t // 8 % 8, t] = 1.0
    return place.astype(bf16)


def times(pair, cosine, sine):
    re, im = pair
    if abs(sine) < 1e-12:
        if cosine > 0:
            return pair
        return (-re, None if im is None else -im)
    if abs(cosine) < 1e-12:
        if im is None:
            return (None, re if sine > 0 else -re)
        return (-im, re) if sine > 0 else (im, -re)
    cosine, sine = np.float32(cosine), np.float32(sine)
    if im is None:
        return (re * cosine, re * sine)
    return (re * cosine - im * sine, re * sine + im * cosine)


def plus(a, b):
    if a is None:
        return b
    return a if b is None else a + b


def minus(a, b):
    if b is None:
        return a
    return -b if a is None else a - b


def small_dft(values, sign):
    count = len(values)
    if count == 1:
        return values
    even = small_dft(values[0::2], sign)
    odd = small_dft(values[1::2], sign)
    out = [None] * count
    for k in range(count // 2):
        angle = sign * 2.0 * math.pi * k / count
        turned = times(odd[k], math.cos(angle), math.sin(angle))
        out[k] = (plus(even[k][0], turned[0]), plus(even[k][1], turned[1]))
        out[k + count // 2] = (minus(even[k][0], turned[0]), minus(even[k][1], turned[1]))
    return out


def swap_groups(arrays):
    arrays = list(arrays)
    lane = lax.broadcasted_iota(jnp.int32, arrays[0].shape, arrays[0].ndim - 1)
    axis = arrays[0].ndim - 1
    for bit in range(3):
        shift = 16 << bit
        upper = (lane // shift) % 2 == 1
        for j in range(8):
            other = j | (1 << bit)
            if other == j:
                continue
            low, high = arrays[j], arrays[other]
            arrays[j] = jnp.where(upper, pltpu.roll(high, shift, axis), low)
            arrays[other] = jnp.where(upper, high, pltpu.roll(low, 128 - shift, axis))
    return arrays


def dot(a, b):
    return jnp.dot(a, b, preferred_element_type=f32)


def dot_nt(a, b):
    return lax.dot_general(a, b, (((1,), (1,)), ((), ())), preferred_element_type=f32)


def halves(value):
    high = value.astype(bf16)
    return high, (value - high.astype(f32)).astype(bf16)


def by_table(value, high, low):
    value_high, value_low = halves(value)
    return dot(value_high, high) + dot(value_low, high) + dot(value_high, low)


def table_by(high, low, value):
    value_high, value_low = halves(value)
    return dot(high, value_high) + dot(high, value_low) + dot(low, value_high)


def greet(vis_me, band_me, neighbours):
    barrier = pltpu.get_barrier_semaphore()

    def vis_signal(d, carry):
        pl.semaphore_signal(
            barrier, inc=1, device_id={"vis": vis_me ^ d}, device_id_type=MESH_ID
        )
        return carry

    def band_signal(d, carry):
        pl.semaphore_signal(
            barrier, inc=1, device_id={"band": band_me ^ d}, device_id_type=MESH_ID
        )
        return carry

    for neighbour in neighbours:
        pl.semaphore_signal(barrier, inc=1, device_id=neighbour, device_id_type=MESH_ID)
    lax.fori_loop(1, NV, vis_signal, 0)
    lax.fori_loop(1, NB, band_signal, 0)
    return barrier


def launch(r, name, part, axis, count, me, same=False):
    sent, landed, sems = r["sent_" + name], r["got_" + name].at[part], r["sem_" + name]
    if not same:
        sent = sent.at[part]

    def body(d, carry):
        peer = me ^ d
        pltpu.make_async_remote_copy(
            src_ref=sent if same else sent.at[peer],
            dst_ref=landed.at[me],
            send_sem=sems.at[2 * part],
            recv_sem=sems.at[2 * part + 1],
            device_id={axis: peer},
            device_id_type=MESH_ID,
        ).start()
        return carry

    lax.fori_loop(1, count, body, 0)
    landed[me] = sent[...] if same else sent[me]


def to_neighbour(sent, landed, sems, neighbour):
    copy = pltpu.make_async_remote_copy(
        src_ref=sent,
        dst_ref=landed,
        send_sem=sems.at[0],
        recv_sem=sems.at[1],
        device_id=neighbour,
        device_id_type=MESH_ID,
    )
    copy.start()
    return copy


def finish(r, name, part, count, side):
    landed = r["got_" + name].at[part]
    landed = landed.at[pl.ds(0, count - 1)]
    pltpu.make_async_copy(landed, landed, r["sem_" + name].at[2 * part + side]).wait()


def arrived(r, name, part, count):
    finish(r, name, part, count, 1)
    return r["got_" + name].at[part]


def step_kernel(*refs):
    names = INPUTS + OUTPUTS + list(SCRATCH)
    r = dict(zip(names, refs))
    vis_me, band_me = lax.axis_index("vis"), lax.axis_index("band")
    me = band_me * NV + vis_me
    following = (me + 1) % (NB * NV)
    preceding = (me + NB * NV - 1) % (NB * NV)
    following = {"band": following // NV, "vis": following % NV}
    preceding = {"band": preceding // NV, "vis": preceding % NV}
    copies = {}
    for place, name in enumerate(STAGED):
        copies[name] = pltpu.make_async_copy(r[name], r["here_" + name], r["sem_in"].at[place])
        copies[name].start()

    def staged(name):
        if name in copies:
            copies.pop(name).wait()
        return r["here_" + name]

    barrier = greet(vis_me, band_me, (following, preceding))

    to_row = (
        lax.broadcasted_iota(jnp.int32, (256, 32), 0) // 8
        == lax.broadcasted_iota(jnp.int32, (256, 32), 1)
    ).astype(f32).astype(bf16)
    column = r["rows"][...]
    facts = jnp.concatenate(
        [column % 32 * 16 + column // 32 - 256, r["counts"][...], jnp.zeros((3, 32), jnp.int32)],
        axis=0,
    ).astype(f32).astype(bf16)
    facts = dot_nt(to_row, facts)
    slot_here = lax.broadcasted_iota(jnp.int32, (256, 8), 0) % 8 // 2
    fact = lax.broadcasted_iota(jnp.int32, (256, 8), 1)
    place = jnp.sum(jnp.where(fact == slot_here, facts, 0.0), axis=1, keepdims=True)
    count = jnp.sum(jnp.where(fact == 4, facts, 0.0), axis=1, keepdims=True)
    places = jnp.broadcast_to(place, (256, 128)).reshape(NV, 8, 128)
    live = jnp.broadcast_to(count, (256, 32)) > (
        lax.broadcasted_iota(jnp.int32, (256, 32), 0) % 8 // 2
    ).astype(f32)
    live = jnp.where(live, 1.0, 0.0)
    vis_state = r["vis_state"][...].reshape(256, 32)
    vis_data = r["vis_data"][...].reshape(256, 32)
    data_square = jnp.sum(live * vis_data * vis_data)

    weights = dot((live * vis_state).astype(bf16), r["repeat"][...]).reshape(NV, 8, 256)
    wide_row = lax.broadcasted_iota(jnp.int32, (NV, 8, 256), 1)
    wide_lane = lax.broadcasted_iota(jnp.int32, (NV, 8, 256), 2)
    crossed = jnp.where(
        wide_row % 2 == 0, pltpu.roll(weights, 7, 1), -pltpu.roll(weights, 1, 1)
    )
    weights = jnp.where(wide_lane // 32 % 2 == 0, weights, crossed)
    r["weights"][...] = jnp.where(wide_lane // 64 == wide_row // 2, weights, 0.0).astype(bf16)
    twist_col = r["twist_col"]
    eye = (
        lax.broadcasted_iota(jnp.int32, (128, 128), 0)
        == lax.broadcasted_iota(jnp.int32, (128, 128), 1)
    )
    for c in range(2):
        one = jnp.broadcast_to(r["twists"][vis_me, c : c + 1, :], (128, 128))
        one = jnp.sum(jnp.where(eye, one, 0.0), axis=1, keepdims=True)
        twist_col[:, c] = jnp.broadcast_to(one, (128, 128)).reshape(8, 16, 128)

    sent_a = r["sent_a"].at[0]
    coef = staged("coef")
    for part in range(4):
        r["coef_rows"][3 * part : 3 * part + 3] = coef[part, 5:8, :]
    r["coef_rows"][12:16] = jnp.zeros((4, 2048), f32)
    kernels = staged("kernels")
    for q in range(NV):
        part = dot(r["weights"][q], kernels[q])
        sent_a[q] = jnp.concatenate([part, places[q]], axis=0).astype(bf16)
    pl.semaphore_wait(barrier, NV + NB)
    launch(r, "a", 0, "vis", NV, vis_me)
    coef_copy = to_neighbour(r["coef_rows"], r["got_coef"], r["sem_coef"], following)

    sky = staged("sky")
    sides_hi, sides_lo = r["sides_hi"], r["sides_lo"]
    up_hi, up_lo = staged("up_hi"), staged("up_lo")
    coef_copy.wait_recv()
    rows_up = []
    for part in range(2):
        rows = slice(16 * part, 16 * part + 16)
        stack = jnp.concatenate([coef[part], coef[part + 2], r["got_coef"][...]], axis=0)
        rows_up.append(table_by(sides_hi[rows, :], sides_lo[rows, :], stack))
    stack = []
    for n in range(16):
        parts = []
        for field in rows_up:
            for block in ((n + 15) % 16, n):
                parts.append(field[:, 128 * block : 128 * block + 128])
        stack.append(jnp.concatenate(parts, axis=1))
    smooth = by_table(jnp.concatenate(stack, axis=0), up_hi[...], up_lo[...])
    raw = r["raw_here"]
    for n in range(16):
        cols = slice(256 * n, 256 * n + 256)
        raw[:, cols] = sky[:, cols] - smooth[16 * n : 16 * n + 16]
    got_a = arrived(r, "a", 0, NV)

    order, onehot = r["order"], r["onehot"]
    contrib = got_a[:, 0:8, :].astype(f32).reshape(256, 128).astype(bf16)
    where_to = got_a[:, 8:16, :].astype(f32).reshape(256, 128)
    lane = lax.broadcasted_iota(jnp.int32, (256, 128), 1).astype(f32)
    is_imag = lax.broadcasted_iota(jnp.int32, (256, 128), 0) % 2 == 1
    hots = [(where_to == lane + float(128 * g - 256)).astype(f32) for g in range(4)]
    for g in range(4):
        onehot[:, 128 * g : 128 * g + 128] = hots[g].astype(bf16)
    real_hots = [jnp.where(is_imag, 0.0, h).astype(bf16) for h in hots]
    imag_hots = [jnp.where(is_imag, h, 0.0).astype(bf16) for h in hots]
    hots = jnp.concatenate(real_hots + imag_hots, axis=1)
    turned = dot_nt(order[...], contrib).astype(bf16)
    for part in range(2):
        grid = dot(turned[64 * part : 64 * part + 64], hots)
        for c in range(2):
            for g in range(4):
                cols = slice(512 * c + 128 * g, 512 * c + 128 * g + 128)
                for low in range(8):
                    r["sent_b"][part, low * 4 + g, c] = grid[
                        8 * low : 8 * low + 8, cols
                    ].astype(bf16)
        launch(r, "b", part, "vis", NV, vis_me)

    table_hi, table_lo = staged("table_hi"), staged("table_lo")

    def spread_of(landed):
        return jnp.concatenate(
            [landed[:, 0].reshape(256, 128), landed[:, 1].reshape(256, 128)], axis=1
        )

    first = spread_of(arrived(r, "b", 0, NV))
    ahead = dot(table_hi[:, 0:256], first) + dot(table_lo[:, 0:256], first)
    second = spread_of(arrived(r, "b", 1, NV))
    for part in range(2):
        both = []
        for side in range(2):
            rows = slice(512 * side + 256 * part, 512 * side + 256 * part + 256)
            both.append(
                ahead[rows] + dot(table_hi[rows, 256:512], second)
                + dot(table_lo[rows, 256:512], second)
            )
        re = both[0][:, :128] - both[1][:, 128:]
        im = both[1][:, :128] + both[0][:, 128:]
        r["sent_c"][part, :, 0] = re.reshape(NV, 8, 128).astype(bf16)
        r["sent_c"][part, :, 1] = im.reshape(NV, 8, 128).astype(bf16)
        launch(r, "c", part, "vis", NV, vis_me)

    sent_d = r["sent_d"]
    for part in range(2):
        got_c = arrived(r, "c", part, NV)
        rows = slice(8 * part, 8 * part + 8)
        for g in range(4):
            values = []
            for low in range(8):
                re = got_c[low * 4 + g, 0].astype(f32)
                im = got_c[low * 4 + g, 1].astype(f32)
                cosine, sine = twist_col[low, 0, rows], twist_col[low, 1, rows]
                values.append((re * cosine - im * sine, re * sine + im * cosine))
            values = small_dft(values, 1.0)
            for b in range(NB):
                for c in range(2):
                    sent_d[part, b, c, :, 128 * g : 128 * g + 128] = values[b][c].astype(
                        sent_d.dtype
                    )
        launch(r, "d", part, "band", NB, band_me)

    mid, twist_row, extrap, sent_e = r["mid"], r["twist_row"], r["extrap"], r["sent_e"]

    def lane_product(part):
        return by_table(
            mid[part].reshape(512, 128), r["lane_hi"][...], r["lane_lo"][...]
        ).reshape(32, 2, 8, 256)

    for part in range(2):
        rows = slice(8 * part, 8 * part + 8)
        got_d = arrived(r, "d", part, NB)
        for g in range(4):
            for c in range(2):
                parts = swap_groups(
                    [got_d[b, c, :, 128 * g : 128 * g + 128].astype(f32) for b in range(NB)]
                )
                for a in range(8):
                    mid[part, g * 8 + a, c] = parts[a]
        lanes = lane_product(part)
        values = []
        for a in range(32):
            re = lanes[a, 0, :, :128] - lanes[a, 1, :, 128:]
            im = lanes[a, 0, :, 128:] + lanes[a, 1, :, :128]
            cosine, sine = twist_row[a, 0:1], twist_row[a, 1:2]
            values.append((re * cosine - im * sine, re * sine + im * cosine))
        values = small_dft(values, 1.0)
        for n in range(32):
            cols = slice(128 * n, 128 * n + 128)
            now = jnp.maximum(raw[rows, cols] - values[n][0], 0.0)
            raw[rows, cols] = now
            extrap[part, :, cols] = 2.0 * now - sky[rows, cols]
        if part == 0:
            image_copy = to_neighbour(extrap.at[0], r["got_rows"], r["sem_rows"], preceding)
        values = [(extrap[part, :, 128 * n : 128 * n + 128], None) for n in range(32)]
        values = small_dft(values, -1.0)
        for a in range(32):
            re, im = values[a]
            cosine, sine = twist_row[a, 0:1], twist_row[a, 1:2]
            if im is None:
                mid[part, a, 0] = re * cosine
                mid[part, a, 1] = -re * sine
            else:
                mid[part, a, 0] = re * cosine + im * sine
                mid[part, a, 1] = im * cosine - re * sine
        lanes = lane_product(part)
        for g in range(4):
            for c in range(2):
                parts = []
                for a in range(8):
                    re, im = lanes[g * 8 + a, 0], lanes[g * 8 + a, 1]
                    if c == 0:
                        parts.append(re[:, :128] + im[:, 128:])
                    else:
                        parts.append(im[:, :128] - re[:, 128:])
                parts = swap_groups(parts)
                for b in range(NB):
                    sent_e[part, b, c, :, 128 * g : 128 * g + 128] = parts[b]
        launch(r, "e", part, "band", NB, band_me)
    out_image = pltpu.make_async_copy(raw, r["image"], r["sem_out"].at[0])
    out_image.start()

    sent_f = r["sent_f"]
    for part in range(2):
        got_e = arrived(r, "e", part, NB)
        rows = slice(8 * part, 8 * part + 8)
        for g in range(4):
            values = []
            for b in range(NB):
                values.append(
                    tuple(got_e[b, c, :, 128 * g : 128 * g + 128] for c in range(2))
                )
            values = small_dft(values, -1.0)
            for low in range(8):
                re, im = values[low]
                cosine, sine = twist_col[low, 0, rows], twist_col[low, 1, rows]
                sent_f[part, low * 4 + g, 0] = (re * cosine + im * sine).astype(sent_f.dtype)
                sent_f[part, low * 4 + g, 1] = (im * cosine - re * sine).astype(sent_f.dtype)
        launch(r, "f", part, "vis", NV, vis_me)

    down_hi, down_lo = staged("down_hi"), staged("down_lo")
    image_copy.wait_recv()
    fields = jnp.concatenate([extrap[0], extrap[1], r["got_rows"][...]], axis=0)
    fields = table_by(sides_hi[32:48, 0:24], sides_lo[32:48, 0:24], fields)
    stack = []
    for n in range(16):
        if n < 15:
            stack.append(fields[:, 256 * n : 256 * n + 384])
        else:
            stack.append(jnp.concatenate([fields[:, 3840:4096], fields[:, 0:128]], axis=1))
    found = by_table(jnp.concatenate(stack, axis=0), down_hi[...], down_lo[...])
    coeffs = r["coeffs_here"]
    for n in range(16):
        cols = slice(128 * n, 128 * n + 128)
        block = found[16 * n : 16 * n + 16]
        coeffs[0, :, cols] = coef[0, :, cols] + block[0:8, :128]
        coeffs[1, :, cols] = coef[1, :, cols] + block[0:8, 128:]
        coeffs[2, :, cols] = coef[2, :, cols] + block[8:16, :128]
        coeffs[3, :, cols] = coef[3, :, cols] + block[8:16, 128:]
    abs_total = jnp.sum(jnp.abs(found))
    out_coeffs = pltpu.make_async_copy(coeffs, r["coeffs"], r["sem_out"].at[1])
    out_coeffs.start()

    def through(rows, cols, spread):
        if spread.dtype == f32:
            return table_by(table_hi[rows, cols], table_lo[rows, cols], spread)
        return dot(table_hi[rows, cols], spread) + dot(table_lo[rows, cols], spread)

    first = spread_of(arrived(r, "f", 0, NV))
    ahead = through(slice(0, 1024), slice(0, 256), first)
    second = spread_of(arrived(r, "f", 1, NV))
    for part in range(2):
        both = []
        for side in range(2):
            rows = slice(512 * side + 256 * part, 512 * side + 256 * part + 256)
            both.append(ahead[rows] + through(rows, slice(256, 512), second))
        re = both[0][:, :128] + both[1][:, 128:]
        im = both[0][:, 128:] - both[1][:, :128]
        r["sent_g"][part, :, 0] = re.reshape(NV, 8, 128).astype(bf16)
        r["sent_g"][part, :, 1] = im.reshape(NV, 8, 128).astype(bf16)
        launch(r, "g", part, "vis", NV, vis_me)

    picked = [[], []]
    for part in range(2):
        got_g = arrived(r, "g", part, NV)
        for c in range(2):
            total = 0.0
            for g in range(4):
                piece = jnp.concatenate(
                    [got_g[low * 4 + g, c].astype(f32) for low in range(8)], axis=0
                ).astype(bf16)
                total = total + dot_nt(onehot[:, 128 * g : 128 * g + 128], piece)
            picked[c].append(total)
    picked = [jnp.concatenate(p, axis=1) for p in picked]
    tiles = jnp.where(is_imag, picked[1], picked[0]).astype(bf16)
    tiles = dot(tiles, order[...])
    r["sent_h"][0] = tiles.reshape(NV, 8, 128).astype(bf16)
    launch(r, "h", 0, "vis", NV, vis_me)
    got_h = arrived(r, "h", 0, NV)

    products = jnp.stack([dot_nt(got_h[q], kernels[q]) for q in range(NV)])
    products = jnp.where(wide_lane // 64 == wide_row // 2, products, 0.0)
    products = products[:, :, 0:128] + products[:, :, 128:256]
    products = products + pltpu.roll(products, 64, 2)
    other = pltpu.roll(products, 96, 2)
    row = lax.broadcasted_iota(jnp.int32, (NV, 8, 128), 1)
    products = products + jnp.where(
        row % 2 == 0, -pltpu.roll(other, 7, 1), pltpu.roll(other, 1, 1)
    )
    predicted = products.reshape(256, 128)[:, 0:32]
    residual = live * (vis_state + predicted - vis_data)
    resid_square = jnp.sum(residual * residual)
    r["residual"][...] = residual.reshape(NV, 4, 2, 32)

    sent_t, sent_u = r["sent_t"], r["sent_u"]
    spot = lax.broadcasted_iota(jnp.int32, (1, 128), 1)
    sent_t[...] = jnp.where(
        spot == 0, abs_total, jnp.where(spot == 1, resid_square, data_square)
    )
    launch(r, "t", 0, "vis", NV, vis_me, same=True)
    sent_u[...] = jnp.sum(arrived(r, "t", 0, NV)[...], axis=0)
    launch(r, "u", 0, "band", NB, band_me, same=True)
    totals = jnp.sum(arrived(r, "u", 0, NB)[...], axis=0)
    r["totals"][...] = totals

    for copy in (coef_copy, image_copy):
        copy.wait_send()
    out_image.wait()
    out_coeffs.wait()
    for name in "abcdefghtu":
        for part in range(2 if name in "bcdefg" else 1):
            finish(r, name, part, NB if name in "deu" else NV, 0)


STAGED = ["kernels", "coef", "sky", "up_hi", "up_lo", "table_hi", "table_lo", "down_hi", "down_lo"]
INPUTS = STAGED + [
    "vis_state", "vis_data", "rows", "counts", "repeat", "lane_hi", "lane_lo",
    "twist_row", "twists", "order", "sides_hi", "sides_lo",
]
OUTPUTS = ["image", "coeffs", "residual", "totals"]
VIS_TILE = (2, NV, 2, 8, 128)
BAND_TILE = (2, NB, 2, 8, 512)
SCRATCH = dict(
    here_kernels=((NV, 256, 128), bf16),
    here_coef=((4, 8, 2048), f32),
    here_sky=((16, IMG), f32),
    here_up_hi=((512, 256), bf16),
    here_up_lo=((512, 256), bf16),
    here_table_hi=((1024, 512), bf16),
    here_table_lo=((1024, 512), bf16),
    here_down_hi=((384, 256), bf16),
    here_down_lo=((384, 256), bf16),
    sent_a=((1, NV, 16, 128), bf16), got_a=((1, NV, 16, 128), bf16),
    sent_b=(VIS_TILE, bf16), got_b=(VIS_TILE, bf16),
    sent_c=(VIS_TILE, bf16), got_c=(VIS_TILE, bf16),
    sent_d=(BAND_TILE, bf16), got_d=(BAND_TILE, bf16),
    sent_e=(BAND_TILE, f32), got_e=(BAND_TILE, f32),
    sent_f=(VIS_TILE, f32), got_f=(VIS_TILE, f32),
    sent_g=(VIS_TILE, bf16), got_g=(VIS_TILE, bf16),
    sent_h=((1, NV, 8, 128), bf16), got_h=((1, NV, 8, 128), bf16),
    sent_t=((1, 128), f32), got_t=((1, NV, 1, 128), f32),
    sent_u=((1, 128), f32), got_u=((1, NB, 1, 128), f32),
    weights=((NV, 8, 256), bf16), twist_col=((8, 2, 16, 128), f32), coef_rows=((16, 2048), f32),
    got_coef=((16, 2048), f32), got_rows=((8, IMG), f32),
    raw_here=((16, IMG), f32), extrap=((2, 8, IMG), f32), coeffs_here=((4, 8, 2048), f32),
    onehot=((256, 512), bf16), mid=((2, 32, 2, 8, 128), f32),
    **{"sem_" + n: 4 for n in list("abcdefghtu") + ["coef", "rows", "out"]},
    sem_in=len(STAGED),
)


def step(inputs):
    anywhere = pl.BlockSpec(memory_space=pl.ANY)
    vmem = pl.BlockSpec(memory_space=pltpu.VMEM)
    scratch = []
    for what in SCRATCH.values():
        if isinstance(what, int):
            scratch.append(pltpu.SemaphoreType.DMA((what,)))
        else:
            scratch.append(pltpu.VMEM(*what))
    return pl.pallas_call(
        step_kernel,
        out_shape=(
            jax.ShapeDtypeStruct((16, IMG), f32),
            jax.ShapeDtypeStruct((4, 8, 2048), f32),
            jax.ShapeDtypeStruct((NV, 4, 2, 32), f32),
            jax.ShapeDtypeStruct((1, 128), f32),
        ),
        in_specs=[anywhere if name in STAGED else vmem for name in INPUTS],
        out_specs=(anywhere, anywhere, vmem, vmem),
        scratch_shapes=scratch,
        compiler_params=pltpu.CompilerParams(
            collective_id=0, has_side_effects=True, vmem_limit_bytes=56 * 2**20
        ),
    )(*[inputs[name] for name in INPUTS])


def closing_kernel(*refs):
    given, out, here, sems = refs[0:4], refs[4:7], refs[7:11], refs[11]
    copies = [pltpu.make_async_copy(given[n], here[n], sems.at[n]) for n in range(4)]
    for copy in copies:
        copy.start()

    def hand_out(n):
        copies[n] = pltpu.make_async_copy(here[n], out[n], sems.at[n])
        copies[n].start()

    spot = lax.broadcasted_iota(jnp.int32, (1, 128), 1)
    copies.pop().wait()
    copies[0].wait()
    hand_out(0)
    abs_total, resid_square, data_square = (
        jnp.sum(jnp.where(spot == n, here[3][...], 0.0), axis=1, keepdims=True)
        for n in range(3)
    )
    limit = jnp.broadcast_to(0.5 * abs_total / (IMG * IMG), (8, 2048))
    copies[1].wait()
    for part in range(4):
        here[1][part] = jnp.maximum(jnp.minimum(here[1][part], limit), -limit)
    hand_out(1)
    radius = 0.5 * jnp.sqrt(data_square + 1e-06)
    size = jnp.sqrt(resid_square + 1e-06)
    factor = 1.0 - jnp.minimum(1.0, radius / size)
    copies[2].wait()
    here[2][...] = here[2][...] * jnp.broadcast_to(factor.reshape(1, 1, 1, 1), (NV, 4, 2, 32))
    hand_out(2)
    for copy in copies:
        copy.wait()


def closing(results):
    anywhere = pl.BlockSpec(memory_space=pl.ANY)
    return pl.pallas_call(
        closing_kernel,
        out_shape=tuple(jax.ShapeDtypeStruct(x.shape, x.dtype) for x in results[:3]),
        in_specs=[anywhere] * 4,
        out_specs=(anywhere,) * 3,
        scratch_shapes=[pltpu.VMEM(x.shape, x.dtype) for x in results]
        + [pltpu.SemaphoreType.DMA((4,))],
    )(*results)


def local(sky_image, coef_dual, vis_dual, visibilities, kernel_blocks, tile_rows, tile_counts):
    names = (
        "table_hi", "table_lo", "lane_hi", "lane_lo",
        "up_hi", "up_lo", "down_hi", "down_lo", "sides_hi", "sides_lo",
    )
    inputs = dict(zip(names, dft512_tables() + dft128_tables() + wavelet_tables()))
    inputs.update(
        twist_row=row_twist(), twists=col_twist(), order=lane_order(), repeat=repeat_table()
    )
    inputs = {name: jnp.asarray(table) for name, table in inputs.items()}
    inputs.update(
        kernels=kernel_blocks.reshape(NV, 256, 128),
        coef=coef_dual,
        sky=sky_image,
        vis_state=vis_dual.reshape(NV, 4, 2, 32),
        vis_data=visibilities.reshape(NV, 4, 2, 32),
        rows=tile_rows.reshape(NV, 4).T,
        counts=tile_counts.reshape(1, NV),
    )
    image, coeffs, vis_new = closing(step(inputs))
    return (image, coeffs, vis_new.reshape(1, 1, NV, 4, 2, 32))


def solution(mesh):
    return jax.shard_map(
        local,
        mesh=mesh,
        in_specs=(
            P(("band", "vis"), None),
            P(None, ("band", "vis"), None),
            P("band", "vis", None, None, None, None),
            P("band", "vis", None, None, None, None),
            P("band", "vis", None, None, None, None, None),
            P("band", "vis", None, None),
            P("band", "vis", None),
        ),
        out_specs=(
            P(("band", "vis"), None),
            P(None, ("band", "vis"), None),
            P("band", "vis", None, None, None, None),
        ),
        check_vma=False,
    )
```

```python
import functools
import math

import jax
import jax.numpy as jnp
import numpy as np
from jax import lax
from jax.experimental import pallas as pl
from jax.experimental.pallas import tpu as pltpu
from jax.sharding import PartitionSpec as P

IMG = 4096
NB = 8
NV = 32
MESH_ID = pl.DeviceIdType.MESH
f32 = jnp.float32
bf16 = jnp.bfloat16

low_taps = (
    -0.010597401784997278,
    0.032883011666982945,
    0.030841381835986965,
    -0.18703481171888114,
    -0.02798376941698385,
    0.6308807679295904,
    0.7148465705525415,
    0.23037781330885523,
)
high_taps = tuple(((-1.0) ** offset * low_taps[7 - offset] for offset in range(8)))


def halves_of(table):
    high = table.astype(bf16)
    low = (table - high.astype(np.float64)).astype(bf16)
    return high, low


def dft512_tables():
    index = np.arange(512).reshape(32, 2, 8).transpose(1, 0, 2).reshape(512)
    angle = 2.0 * np.pi / 512 * (index[:, None] * index[None, :] % 512)
    return halves_of(np.concatenate([np.cos(angle), np.sin(angle)], axis=0))


def dft128_tables():
    index = np.arange(128)
    angle = 2.0 * np.pi / 128 * (index[:, None] * index[None, :] % 128)
    return halves_of(np.concatenate([np.cos(angle), np.sin(angle)], axis=1) / IMG)


def row_twist():
    angle = 2.0 * np.pi / IMG * (np.arange(32)[:, None] * np.arange(128)[None, :] % IMG)
    return np.stack([np.cos(angle), np.sin(angle)], axis=1).astype(np.float32)


def col_twist():
    low, row = np.arange(8)[None, :, None], np.arange(16)[None, None, :]
    angle = 2.0 * np.pi / IMG * (low * (16 * np.arange(NV)[:, None, None] + row))
    return np.stack([np.cos(angle), np.sin(angle)], axis=1).reshape(NV, 2, 128).astype(np.float32)


def repeat_table():
    return np.tile(np.eye(32), (1, 8)).astype(bf16)


def wavelet_tables():
    up = np.zeros((512, 256))
    down = np.zeros((384, 256))
    rows_up = np.zeros((2, 16, 32))
    rows_down = np.zeros((16, 24))
    for tap in range(8):
        for side, taps in ((0, low_taps), (1, high_taps)):
            for k in range(128):
                down[2 * k + tap, 128 * side + k] = taps[tap]
            for k in range(-128, 128):
                if 0 <= 2 * k + tap < 256:
                    up[256 * side + 128 + k, 2 * k + tap] = taps[tap]
            for k in range(8):
                rows_down[8 * side + k, 2 * k + tap] = taps[tap]
            for k in range(-3, 8):
                if 0 <= 2 * k + tap < 16:
                    for part in range(2):
                        spot = 8 * side + k if k >= 0 else 16 + 3 * (part + 2 * side) + k + 3
                        rows_up[part, 2 * k + tap, spot] = taps[tap]
    sides = np.zeros((48, 32))
    sides[0:32] = rows_up.reshape(32, 32)
    sides[32:48, 0:24] = rows_down
    return tuple(part for table in (up, down, sides) for part in halves_of(table))


def lane_order():
    place = np.zeros((128, 128), np.float32)
    for t in range(128):
        place[t // 64 * 64 + (t % 8) * 8 + t // 8 % 8, t] = 1.0
    return place.astype(bf16)


def times(pair, cosine, sine):
    re, im = pair
    if abs(sine) < 1e-12:
        if cosine > 0:
            return pair
        return (-re, None if im is None else -im)
    if abs(cosine) < 1e-12:
        if im is None:
            return (None, re if sine > 0 else -re)
        return (-im, re) if sine > 0 else (im, -re)
    cosine, sine = np.float32(cosine), np.float32(sine)
    if im is None:
        return (re * cosine, re * sine)
    return (re * cosine - im * sine, re * sine + im * cosine)


def plus(a, b):
    if a is None:
        return b
    return a if b is None else a + b


def minus(a, b):
    if b is None:
        return a
    return -b if a is None else a - b


def small_dft(values, sign):
    count = len(values)
    if count == 1:
        return values
    even = small_dft(values[0::2], sign)
    odd = small_dft(values[1::2], sign)
    out = [None] * count
    for k in range(count // 2):
        angle = sign * 2.0 * math.pi * k / count
        turned = times(odd[k], math.cos(angle), math.sin(angle))
        out[k] = (plus(even[k][0], turned[0]), plus(even[k][1], turned[1]))
        out[k + count // 2] = (minus(even[k][0], turned[0]), minus(even[k][1], turned[1]))
    return out


def swap_groups(arrays):
    arrays = list(arrays)
    lane = lax.broadcasted_iota(jnp.int32, arrays[0].shape, arrays[0].ndim - 1)
    axis = arrays[0].ndim - 1
    for bit in range(3):
        shift = 16 << bit
        upper = (lane // shift) % 2 == 1
        for j in range(8):
            other = j | (1 << bit)
            if other == j:
                continue
            low, high = arrays[j], arrays[other]
            arrays[j] = jnp.where(upper, pltpu.roll(high, shift, axis), low)
            arrays[other] = jnp.where(upper, high, pltpu.roll(low, 128 - shift, axis))
    return arrays


def dot(a, b):
    return jnp.dot(a, b, preferred_element_type=f32)


def dot_nt(a, b):
    return lax.dot_general(a, b, (((1,), (1,)), ((), ())), preferred_element_type=f32)


def halves(value):
    high = value.astype(bf16)
    return high, (value - high.astype(f32)).astype(bf16)


def by_table(value, high, low):
    value_high, value_low = halves(value)
    return dot(value_high, high) + dot(value_low, high) + dot(value_high, low)


def table_by(high, low, value):
    value_high, value_low = halves(value)
    return dot(high, value_high) + dot(high, value_low) + dot(low, value_high)


def greet(vis_me, band_me, neighbours):
    barrier = pltpu.get_barrier_semaphore()

    def vis_signal(d, carry):
        pl.semaphore_signal(
            barrier, inc=1, device_id={"vis": vis_me ^ d}, device_id_type=MESH_ID
        )
        return carry

    def band_signal(d, carry):
        pl.semaphore_signal(
            barrier, inc=1, device_id={"band": band_me ^ d}, device_id_type=MESH_ID
        )
        return carry

    for neighbour in neighbours:
        pl.semaphore_signal(barrier, inc=1, device_id=neighbour, device_id_type=MESH_ID)
    lax.fori_loop(1, NV, vis_signal, 0)
    lax.fori_loop(1, NB, band_signal, 0)
    return barrier


def far_first(n, count):
    if count == NV:
        z, y = n // 8, n // 2 % 4
        return n % 2 + 2 * (z ^ z // 2) + 8 * (y ^ y // 2)
    x = n % 4
    return (x ^ x // 2) + n // 4 * 4


def launch(r, name, part, axis, count, me, same=False):
    sent, landed, sems = r["sent_" + name], r["got_" + name].at[part], r["sem_" + name]
    if not same:
        sent = sent.at[part]

    def body(step, carry):
        peer = me ^ far_first(count - step, count)
        pltpu.make_async_remote_copy(
            src_ref=sent if same else sent.at[peer],
            dst_ref=landed.at[me],
            send_sem=sems.at[2 * part],
            recv_sem=sems.at[2 * part + 1],
            device_id={axis: peer},
            device_id_type=MESH_ID,
        ).start()
        return carry

    lax.fori_loop(1, count, body, 0)
    landed[me] = sent[...] if same else sent[me]


def to_neighbour(sent, landed, sems, neighbour):
    copy = pltpu.make_async_remote_copy(
        src_ref=sent,
        dst_ref=landed,
        send_sem=sems.at[0],
        recv_sem=sems.at[1],
        device_id=neighbour,
        device_id_type=MESH_ID,
    )
    copy.start()
    return copy


def finish(r, name, part, count, side):
    landed = r["got_" + name].at[part]
    landed = landed.at[pl.ds(0, count - 1)]
    pltpu.make_async_copy(landed, landed, r["sem_" + name].at[2 * part + side]).wait()


def arrived(r, name, part, count):
    finish(r, name, part, count, 1)
    return r["got_" + name].at[part]


def step_kernel(*refs):
    names = INPUTS + OUTPUTS + list(SCRATCH)
    r = dict(zip(names, refs))
    vis_me, band_me = lax.axis_index("vis"), lax.axis_index("band")
    me = band_me * NV + vis_me
    following = (me + 1) % (NB * NV)
    preceding = (me + NB * NV - 1) % (NB * NV)
    following = {"band": following // NV, "vis": following % NV}
    preceding = {"band": preceding // NV, "vis": preceding % NV}
    copies = {}
    for place, name in enumerate(STAGED):
        copies[name] = pltpu.make_async_copy(r[name], r["here_" + name], r["sem_in"].at[place])
        copies[name].start()

    def staged(name):
        if name in copies:
            copies.pop(name).wait()
        return r["here_" + name]

    barrier = greet(vis_me, band_me, (following, preceding))

    to_row = (
        lax.broadcasted_iota(jnp.int32, (256, 32), 0) // 8
        == lax.broadcasted_iota(jnp.int32, (256, 32), 1)
    ).astype(f32).astype(bf16)
    column = r["rows"][...]
    facts = jnp.concatenate(
        [
            (column % 32 * 16 + column // 32 - 256).astype(f32),
            r["counts"][...].astype(f32),
            jnp.zeros((123, 32), f32),
        ],
        axis=0,
    ).astype(bf16)
    eye = (
        lax.broadcasted_iota(jnp.int32, (32, 32), 0)
        == lax.broadcasted_iota(jnp.int32, (32, 32), 1)
    ).astype(f32).astype(bf16)
    facts = dot_nt(eye, facts)
    r["sent_i"][0] = facts.reshape(NV, 1, 128)
    row_slot = lax.broadcasted_iota(jnp.int32, (256, 128), 0) % 8 // 2
    fact = lax.broadcasted_iota(jnp.int32, (256, 128), 1)

    def per_row(table, choice):
        wide = dot(to_row, table.astype(bf16))
        return jnp.sum(jnp.where(fact == choice, wide, 0.0), axis=1, keepdims=True)

    count = per_row(facts, 4)
    live = jnp.broadcast_to(count, (256, 32)) > (
        lax.broadcasted_iota(jnp.int32, (256, 32), 0) % 8 // 2
    ).astype(f32)
    live = jnp.where(live, 1.0, 0.0)
    vis_state = r["vis_state"][...].reshape(256, 32)
    vis_data = r["vis_data"][...].reshape(256, 32)
    data_square = jnp.sum(live * vis_data * vis_data)

    weights = dot((live * vis_state).astype(bf16), r["repeat"][...]).reshape(NV, 8, 256)
    wide_row = lax.broadcasted_iota(jnp.int32, (NV, 8, 256), 1)
    wide_lane = lax.broadcasted_iota(jnp.int32, (NV, 8, 256), 2)
    crossed = jnp.where(
        wide_row % 2 == 0, pltpu.roll(weights, 7, 1), -pltpu.roll(weights, 1, 1)
    )
    weights = jnp.where(wide_lane // 32 % 2 == 0, weights, crossed)
    r["weights"][...] = jnp.where(wide_lane // 64 == wide_row // 2, weights, 0.0).astype(bf16)
    twist_col = r["twist_col"]
    eye = (
        lax.broadcasted_iota(jnp.int32, (128, 128), 0)
        == lax.broadcasted_iota(jnp.int32, (128, 128), 1)
    )
    for c in range(2):
        one = jnp.broadcast_to(r["twists"][vis_me, c : c + 1, :], (128, 128))
        one = jnp.sum(jnp.where(eye, one, 0.0), axis=1, keepdims=True)
        twist_col[:, c] = jnp.broadcast_to(one, (128, 128)).reshape(8, 16, 128)

    kernels = staged("kernels")
    for q in range(NV):
        r["sent_a"][0, q] = dot(r["weights"][q], kernels[q]).astype(bf16)
    coef = staged("coef")
    for part in range(4):
        r["coef_rows"][3 * part : 3 * part + 3] = coef[part, 5:8, :]
    r["coef_rows"][12:16] = jnp.zeros((4, 2048), f32)
    pl.semaphore_wait(barrier, NV + NB)
    launch(r, "i", 0, "vis", NV, vis_me)
    launch(r, "a", 0, "vis", NV, vis_me)

    order, onehot = r["order"], r["onehot"]
    where_to = per_row(arrived(r, "i", 0, NV)[...].reshape(NV, 128), row_slot)
    where_to = jnp.broadcast_to(where_to, (256, 128))
    lane = lax.broadcasted_iota(jnp.int32, (256, 128), 1).astype(f32)
    is_imag = lax.broadcasted_iota(jnp.int32, (256, 128), 0) % 2 == 1
    hots = [(where_to == lane + float(128 * g - 256)).astype(f32) for g in range(4)]
    for g in range(4):
        onehot[:, 128 * g : 128 * g + 128] = hots[g].astype(bf16)
    real_hots = [jnp.where(is_imag, 0.0, h).astype(bf16) for h in hots]
    imag_hots = [jnp.where(is_imag, h, 0.0).astype(bf16) for h in hots]
    hots = jnp.concatenate(real_hots + imag_hots, axis=1)
    contrib = arrived(r, "a", 0, NV)[...].astype(f32).reshape(256, 128).astype(bf16)
    turned = dot_nt(order[...], contrib).astype(bf16)
    for part in range(2):
        grid = dot(turned[64 * part : 64 * part + 64], hots)
        for c in range(2):
            for g in range(4):
                cols = slice(512 * c + 128 * g, 512 * c + 128 * g + 128)
                for low in range(8):
                    r["sent_b"][part, low * 4 + g, c] = grid[
                        8 * low : 8 * low + 8, cols
                    ].astype(bf16)
        launch(r, "b", part, "vis", NV, vis_me)

    table_hi, table_lo = staged("table_hi"), staged("table_lo")

    def spread_of(landed):
        return jnp.concatenate(
            [landed[:, 0].reshape(256, 128), landed[:, 1].reshape(256, 128)], axis=1
        )

    first = spread_of(arrived(r, "b", 0, NV))
    ahead = dot(table_hi[:, 0:256], first) + dot(table_lo[:, 0:256], first)
    second = spread_of(arrived(r, "b", 1, NV))
    for part in range(2):
        both = []
        for side in range(2):
            rows = slice(512 * side + 256 * part, 512 * side + 256 * part + 256)
            both.append(
                ahead[rows] + dot(table_hi[rows, 256:512], second)
                + dot(table_lo[rows, 256:512], second)
            )
        re = both[0][:, :128] - both[1][:, 128:]
        im = both[1][:, :128] + both[0][:, 128:]
        r["sent_c"][part, :, 0] = re.reshape(NV, 8, 128).astype(bf16)
        r["sent_c"][part, :, 1] = im.reshape(NV, 8, 128).astype(bf16)
        launch(r, "c", part, "vis", NV, vis_me)
    coef_copy = to_neighbour(r["coef_rows"], r["got_coef"], r["sem_coef"], following)

    sent_d = r["sent_d"]
    for part in range(2):
        got_c = arrived(r, "c", part, NV)
        rows = slice(8 * part, 8 * part + 8)
        for g in range(4):
            values = []
            for low in range(8):
                re = got_c[low * 4 + g, 0].astype(f32)
                im = got_c[low * 4 + g, 1].astype(f32)
                cosine, sine = twist_col[low, 0, rows], twist_col[low, 1, rows]
                values.append((re * cosine - im * sine, re * sine + im * cosine))
            values = small_dft(values, 1.0)
            for b in range(NB):
                for c in range(2):
                    sent_d[part, b, c, :, 128 * g : 128 * g + 128] = values[b][c].astype(
                        sent_d.dtype
                    )
        launch(r, "d", part, "band", NB, band_me)

    sky = staged("sky")
    sides_hi, sides_lo = r["sides_hi"], r["sides_lo"]
    up_hi, up_lo = staged("up_hi"), staged("up_lo")
    coef_copy.wait_recv()
    rows_up = []
    for part in range(2):
        rows = slice(16 * part, 16 * part + 16)
        stack = jnp.concatenate([coef[part], coef[part + 2], r["got_coef"][...]], axis=0)
        rows_up.append(table_by(sides_hi[rows, :], sides_lo[rows, :], stack))
    stack = []
    for n in range(16):
        parts = []
        for field in rows_up:
            for block in ((n + 15) % 16, n):
                parts.append(field[:, 128 * block : 128 * block + 128])
        stack.append(jnp.concatenate(parts, axis=1))
    smooth = by_table(jnp.concatenate(stack, axis=0), up_hi[...], up_lo[...])
    raw = r["raw_here"]
    for n in range(16):
        cols = slice(256 * n, 256 * n + 256)
        raw[:, cols] = sky[:, cols] - smooth[16 * n : 16 * n + 16]

    mid, twist_row, extrap, sent_e = r["mid"], r["twist_row"], r["extrap"], r["sent_e"]

    def lane_product(part):
        return by_table(
            mid[part].reshape(512, 128), r["lane_hi"][...], r["lane_lo"][...]
        ).reshape(32, 2, 8, 256)

    for part in range(2):
        rows = slice(8 * part, 8 * part + 8)
        got_d = arrived(r, "d", part, NB)
        for g in range(4):
            for c in range(2):
                parts = swap_groups(
                    [got_d[b, c, :, 128 * g : 128 * g + 128].astype(f32) for b in range(NB)]
                )
                for a in range(8):
                    mid[part, g * 8 + a, c] = parts[a]
        lanes = lane_product(part)
        values = []
        for a in range(32):
            re = lanes[a, 0, :, :128] - lanes[a, 1, :, 128:]
            im = lanes[a, 0, :, 128:] + lanes[a, 1, :, :128]
            cosine, sine = twist_row[a, 0:1], twist_row[a, 1:2]
            values.append((re * cosine - im * sine, re * sine + im * cosine))
        values = small_dft(values, 1.0)
        for n in range(32):
            cols = slice(128 * n, 128 * n + 128)
            now = jnp.maximum(raw[rows, cols] - values[n][0], 0.0)
            raw[rows, cols] = now
            extrap[part, :, cols] = 2.0 * now - sky[rows, cols]
        if part == 0:
            image_copy = to_neighbour(extrap.at[0], r["got_rows"], r["sem_rows"], preceding)
        values = [(extrap[part, :, 128 * n : 128 * n + 128], None) for n in range(32)]
        values = small_dft(values, -1.0)
        for a in range(32):
            re, im = values[a]
            cosine, sine = twist_row[a, 0:1], twist_row[a, 1:2]
            if im is None:
                mid[part, a, 0] = re * cosine
                mid[part, a, 1] = -re * sine
            else:
                mid[part, a, 0] = re * cosine + im * sine
                mid[part, a, 1] = im * cosine - re * sine
        lanes = lane_product(part)
        for g in range(4):
            for c in range(2):
                parts = []
                for a in range(8):
                    re, im = lanes[g * 8 + a, 0], lanes[g * 8 + a, 1]
                    if c == 0:
                        parts.append(re[:, :128] + im[:, 128:])
                    else:
                        parts.append(im[:, :128] - re[:, 128:])
                parts = swap_groups(parts)
                for b in range(NB):
                    sent_e[part, b, c, :, 128 * g : 128 * g + 128] = parts[b]
        launch(r, "e", part, "band", NB, band_me)
    out_image = pltpu.make_async_copy(raw, r["image"], r["sem_out"].at[0])
    out_image.start()

    sent_f = r["sent_f"]
    for part in range(2):
        got_e = arrived(r, "e", part, NB)
        rows = slice(8 * part, 8 * part + 8)
        for g in range(4):
            values = []
            for b in range(NB):
                values.append(
                    tuple(got_e[b, c, :, 128 * g : 128 * g + 128] for c in range(2))
                )
            values = small_dft(values, -1.0)
            for low in range(8):
                re, im = values[low]
                cosine, sine = twist_col[low, 0, rows], twist_col[low, 1, rows]
                sent_f[part, low * 4 + g, 0] = (re * cosine + im * sine).astype(sent_f.dtype)
                sent_f[part, low * 4 + g, 1] = (im * cosine - re * sine).astype(sent_f.dtype)
        launch(r, "f", part, "vis", NV, vis_me)

    down_hi, down_lo = staged("down_hi"), staged("down_lo")
    image_copy.wait_recv()
    fields = jnp.concatenate([extrap[0], extrap[1], r["got_rows"][...]], axis=0)
    fields = table_by(sides_hi[32:48, 0:24], sides_lo[32:48, 0:24], fields)
    stack = []
    for n in range(16):
        if n < 15:
            stack.append(fields[:, 256 * n : 256 * n + 384])
        else:
            stack.append(jnp.concatenate([fields[:, 3840:4096], fields[:, 0:128]], axis=1))
    found = by_table(jnp.concatenate(stack, axis=0), down_hi[...], down_lo[...])
    coeffs = r["coeffs_here"]
    for n in range(16):
        cols = slice(128 * n, 128 * n + 128)
        block = found[16 * n : 16 * n + 16]
        coeffs[0, :, cols] = coef[0, :, cols] + block[0:8, :128]
        coeffs[1, :, cols] = coef[1, :, cols] + block[0:8, 128:]
        coeffs[2, :, cols] = coef[2, :, cols] + block[8:16, :128]
        coeffs[3, :, cols] = coef[3, :, cols] + block[8:16, 128:]
    abs_total = jnp.sum(jnp.abs(found))
    out_coeffs = pltpu.make_async_copy(coeffs, r["coeffs"], r["sem_out"].at[1])
    out_coeffs.start()

    def through(rows, cols, spread):
        if spread.dtype == f32:
            return table_by(table_hi[rows, cols], table_lo[rows, cols], spread)
        return dot(table_hi[rows, cols], spread) + dot(table_lo[rows, cols], spread)

    first = spread_of(arrived(r, "f", 0, NV))
    ahead = through(slice(0, 1024), slice(0, 256), first)
    second = spread_of(arrived(r, "f", 1, NV))
    for part in range(2):
        both = []
        for side in range(2):
            rows = slice(512 * side + 256 * part, 512 * side + 256 * part + 256)
            both.append(ahead[rows] + through(rows, slice(256, 512), second))
        re = both[0][:, :128] + both[1][:, 128:]
        im = both[0][:, 128:] - both[1][:, :128]
        r["sent_g"][part, :, 0] = re.reshape(NV, 8, 128).astype(bf16)
        r["sent_g"][part, :, 1] = im.reshape(NV, 8, 128).astype(bf16)
        launch(r, "g", part, "vis", NV, vis_me)

    picked = [[], []]
    for part in range(2):
        got_g = arrived(r, "g", part, NV)
        for c in range(2):
            total = 0.0
            for g in range(4):
                piece = jnp.concatenate(
                    [got_g[low * 4 + g, c].astype(f32) for low in range(8)], axis=0
                ).astype(bf16)
                total = total + dot_nt(onehot[:, 128 * g : 128 * g + 128], piece)
            picked[c].append(total)
    picked = [jnp.concatenate(p, axis=1) for p in picked]
    tiles = jnp.where(is_imag, picked[1], picked[0]).astype(bf16)
    tiles = dot(tiles, order[...])
    r["sent_h"][0] = tiles.reshape(NV, 8, 128).astype(bf16)
    launch(r, "h", 0, "vis", NV, vis_me)
    got_h = arrived(r, "h", 0, NV)

    products = jnp.stack([dot_nt(got_h[q], kernels[q]) for q in range(NV)])
    products = jnp.where(wide_lane // 64 == wide_row // 2, products, 0.0)
    products = products[:, :, 0:128] + products[:, :, 128:256]
    products = products + pltpu.roll(products, 64, 2)
    other = pltpu.roll(products, 96, 2)
    row = lax.broadcasted_iota(jnp.int32, (NV, 8, 128), 1)
    products = products + jnp.where(
        row % 2 == 0, -pltpu.roll(other, 7, 1), pltpu.roll(other, 1, 1)
    )
    predicted = products.reshape(256, 128)[:, 0:32]
    residual = live * (vis_state + predicted - vis_data)
    resid_square = jnp.sum(residual * residual)
    r["residual"][...] = residual.reshape(NV, 4, 2, 32)

    sent_t, sent_u = r["sent_t"], r["sent_u"]
    spot = lax.broadcasted_iota(jnp.int32, (1, 128), 1)
    sent_t[...] = jnp.where(
        spot == 0, abs_total, jnp.where(spot == 1, resid_square, data_square)
    )
    launch(r, "t", 0, "vis", NV, vis_me, same=True)
    sent_u[...] = jnp.sum(arrived(r, "t", 0, NV)[...], axis=0)
    launch(r, "u", 0, "band", NB, band_me, same=True)
    totals = jnp.sum(arrived(r, "u", 0, NB)[...], axis=0)
    r["totals"][...] = totals

    for copy in (coef_copy, image_copy):
        copy.wait_send()
    out_image.wait()
    out_coeffs.wait()
    for name in "abcdefghitu":
        for part in range(2 if name in "bcdefg" else 1):
            finish(r, name, part, NB if name in "deu" else NV, 0)


STAGED = ["kernels", "coef", "sky", "up_hi", "up_lo", "table_hi", "table_lo", "down_hi", "down_lo"]
INPUTS = STAGED + [
    "vis_state", "vis_data", "rows", "counts", "repeat", "lane_hi", "lane_lo",
    "twist_row", "twists", "order", "sides_hi", "sides_lo",
]
OUTPUTS = ["image", "coeffs", "residual", "totals"]
VIS_TILE = (2, NV, 2, 8, 128)
BAND_TILE = (2, NB, 2, 8, 512)
SCRATCH = dict(
    here_kernels=((NV, 256, 128), bf16),
    here_coef=((4, 8, 2048), f32),
    here_sky=((16, IMG), f32),
    here_up_hi=((512, 256), bf16),
    here_up_lo=((512, 256), bf16),
    here_table_hi=((1024, 512), bf16),
    here_table_lo=((1024, 512), bf16),
    here_down_hi=((384, 256), bf16),
    here_down_lo=((384, 256), bf16),
    sent_a=((1, NV, 8, 128), bf16), got_a=((1, NV, 8, 128), bf16),
    sent_i=((1, NV, 1, 128), f32), got_i=((1, NV, 1, 128), f32),
    sent_b=(VIS_TILE, bf16), got_b=(VIS_TILE, bf16),
    sent_c=(VIS_TILE, bf16), got_c=(VIS_TILE, bf16),
    sent_d=(BAND_TILE, bf16), got_d=(BAND_TILE, bf16),
    sent_e=(BAND_TILE, f32), got_e=(BAND_TILE, f32),
    sent_f=(VIS_TILE, f32), got_f=(VIS_TILE, f32),
    sent_g=(VIS_TILE, bf16), got_g=(VIS_TILE, bf16),
    sent_h=((1, NV, 8, 128), bf16), got_h=((1, NV, 8, 128), bf16),
    sent_t=((1, 128), f32), got_t=((1, NV, 1, 128), f32),
    sent_u=((1, 128), f32), got_u=((1, NB, 1, 128), f32),
    weights=((NV, 8, 256), bf16), twist_col=((8, 2, 16, 128), f32), coef_rows=((16, 2048), f32),
    got_coef=((16, 2048), f32), got_rows=((8, IMG), f32),
    raw_here=((16, IMG), f32), extrap=((2, 8, IMG), f32), coeffs_here=((4, 8, 2048), f32),
    onehot=((256, 512), bf16), mid=((2, 32, 2, 8, 128), f32),
    **{"sem_" + n: 4 for n in list("abcdefghitu") + ["coef", "rows", "out"]},
    sem_in=len(STAGED),
)


def step(inputs):
    anywhere = pl.BlockSpec(memory_space=pl.ANY)
    vmem = pl.BlockSpec(memory_space=pltpu.VMEM)
    scratch = []
    for what in SCRATCH.values():
        if isinstance(what, int):
            scratch.append(pltpu.SemaphoreType.DMA((what,)))
        else:
            scratch.append(pltpu.VMEM(*what))
    return pl.pallas_call(
        step_kernel,
        out_shape=(
            jax.ShapeDtypeStruct((16, IMG), f32),
            jax.ShapeDtypeStruct((4, 8, 2048), f32),
            jax.ShapeDtypeStruct((NV, 4, 2, 32), f32),
            jax.ShapeDtypeStruct((1, 128), f32),
        ),
        in_specs=[anywhere if name in STAGED else vmem for name in INPUTS],
        out_specs=(anywhere, anywhere, vmem, vmem),
        scratch_shapes=scratch,
        compiler_params=pltpu.CompilerParams(
            collective_id=0, has_side_effects=True, vmem_limit_bytes=56 * 2**20
        ),
    )(*[inputs[name] for name in INPUTS])


def closing_kernel(*refs):
    given, out, here, sems = refs[0:4], refs[4:7], refs[7:11], refs[11]
    copies = [pltpu.make_async_copy(given[n], here[n], sems.at[n]) for n in range(4)]
    for copy in copies:
        copy.start()

    def hand_out(n):
        copies[n] = pltpu.make_async_copy(here[n], out[n], sems.at[n])
        copies[n].start()

    spot = lax.broadcasted_iota(jnp.int32, (1, 128), 1)
    copies.pop().wait()
    copies[0].wait()
    hand_out(0)
    abs_total, resid_square, data_square = (
        jnp.sum(jnp.where(spot == n, here[3][...], 0.0), axis=1, keepdims=True)
        for n in range(3)
    )
    limit = jnp.broadcast_to(0.5 * abs_total / (IMG * IMG), (8, 2048))
    copies[1].wait()
    for part in range(4):
        here[1][part] = jnp.maximum(jnp.minimum(here[1][part], limit), -limit)
    hand_out(1)
    radius = 0.5 * jnp.sqrt(data_square + 1e-06)
    size = jnp.sqrt(resid_square + 1e-06)
    factor = 1.0 - jnp.minimum(1.0, radius / size)
    copies[2].wait()
    here[2][...] = here[2][...] * jnp.broadcast_to(factor.reshape(1, 1, 1, 1), (NV, 4, 2, 32))
    hand_out(2)
    for copy in copies:
        copy.wait()


def closing(results):
    anywhere = pl.BlockSpec(memory_space=pl.ANY)
    return pl.pallas_call(
        closing_kernel,
        out_shape=tuple(jax.ShapeDtypeStruct(x.shape, x.dtype) for x in results[:3]),
        in_specs=[anywhere] * 4,
        out_specs=(anywhere,) * 3,
        scratch_shapes=[pltpu.VMEM(x.shape, x.dtype) for x in results]
        + [pltpu.SemaphoreType.DMA((4,))],
    )(*results)


def local(sky_image, coef_dual, vis_dual, visibilities, kernel_blocks, tile_rows, tile_counts):
    names = (
        "table_hi", "table_lo", "lane_hi", "lane_lo",
        "up_hi", "up_lo", "down_hi", "down_lo", "sides_hi", "sides_lo",
    )
    inputs = dict(zip(names, dft512_tables() + dft128_tables() + wavelet_tables()))
    inputs.update(
        twist_row=row_twist(), twists=col_twist(), order=lane_order(), repeat=repeat_table()
    )
    inputs = {name: jnp.asarray(table) for name, table in inputs.items()}
    inputs.update(
        kernels=kernel_blocks.reshape(NV, 256, 128),
        coef=coef_dual,
        sky=sky_image,
        vis_state=vis_dual.reshape(NV, 4, 2, 32),
        vis_data=visibilities.reshape(NV, 4, 2, 32),
        rows=tile_rows.reshape(NV, 4).T,
        counts=tile_counts.reshape(1, NV),
    )
    image, coeffs, vis_new = closing(step(inputs))
    return (image, coeffs, vis_new.reshape(1, 1, NV, 4, 2, 32))


def solution(mesh):
    return jax.shard_map(
        local,
        mesh=mesh,
        in_specs=(
            P(("band", "vis"), None),
            P(None, ("band", "vis"), None),
            P("band", "vis", None, None, None, None),
            P("band", "vis", None, None, None, None),
            P("band", "vis", None, None, None, None, None),
            P("band", "vis", None, None),
            P("band", "vis", None),
        ),
        out_specs=(
            P(("band", "vis"), None),
            P(None, ("band", "vis"), None),
            P("band", "vis", None, None, None, None),
        ),
        check_vma=False,
    )
```

```python
import functools
import math

import jax
import jax.numpy as jnp
import numpy as np
from jax import lax
from jax.experimental import pallas as pl
from jax.experimental.pallas import tpu as pltpu
from jax.sharding import PartitionSpec as P

IMG = 4096
NB = 8
NV = 32
MESH_ID = pl.DeviceIdType.MESH
f32 = jnp.float32
bf16 = jnp.bfloat16

low_taps = (
    -0.010597401784997278,
    0.032883011666982945,
    0.030841381835986965,
    -0.18703481171888114,
    -0.02798376941698385,
    0.6308807679295904,
    0.7148465705525415,
    0.23037781330885523,
)
high_taps = tuple(((-1.0) ** offset * low_taps[7 - offset] for offset in range(8)))


def halves_of(table):
    high = table.astype(bf16)
    low = (table - high.astype(np.float64)).astype(bf16)
    return high, low


def dft512_tables():
    index = np.arange(512).reshape(32, 2, 8).transpose(1, 0, 2).reshape(512)
    angle = 2.0 * np.pi / 512 * (index[:, None] * index[None, :] % 512)
    return halves_of(np.concatenate([np.cos(angle), np.sin(angle)], axis=0))


def dft128_tables():
    index = np.arange(128)
    angle = 2.0 * np.pi / 128 * (index[:, None] * index[None, :] % 128)
    return halves_of(np.concatenate([np.cos(angle), np.sin(angle)], axis=1) / IMG)


def row_twist():
    angle = 2.0 * np.pi / IMG * (np.arange(32)[:, None] * np.arange(128)[None, :] % IMG)
    return np.stack([np.cos(angle), np.sin(angle)], axis=1).astype(np.float32)


def col_twist():
    low, row = np.arange(8)[None, :, None], np.arange(16)[None, None, :]
    angle = 2.0 * np.pi / IMG * (low * (16 * np.arange(NV)[:, None, None] + row))
    return np.stack([np.cos(angle), np.sin(angle)], axis=1).reshape(NV, 2, 128).astype(np.float32)


def repeat_table():
    return np.tile(np.eye(32), (1, 8)).astype(bf16)


def wavelet_tables():
    up = np.zeros((512, 256))
    down = np.zeros((384, 256))
    rows_up = np.zeros((2, 16, 32))
    rows_down = np.zeros((16, 24))
    for tap in range(8):
        for side, taps in ((0, low_taps), (1, high_taps)):
            for k in range(128):
                down[2 * k + tap, 128 * side + k] = taps[tap]
            for k in range(-128, 128):
                if 0 <= 2 * k + tap < 256:
                    up[256 * side + 128 + k, 2 * k + tap] = taps[tap]
            for k in range(8):
                rows_down[8 * side + k, 2 * k + tap] = taps[tap]
            for k in range(-3, 8):
                if 0 <= 2 * k + tap < 16:
                    for part in range(2):
                        spot = 8 * side + k if k >= 0 else 16 + 3 * (part + 2 * side) + k + 3
                        rows_up[part, 2 * k + tap, spot] = taps[tap]
    sides = np.zeros((48, 32))
    sides[0:32] = rows_up.reshape(32, 32)
    sides[32:48, 0:24] = rows_down
    return tuple(part for table in (up, down, sides) for part in halves_of(table))


def lane_order():
    place = np.zeros((128, 128), np.float32)
    for t in range(128):
        place[t // 64 * 64 + (t % 8) * 8 + t // 8 % 8, t] = 1.0
    return place.astype(bf16)


def times(pair, cosine, sine):
    re, im = pair
    if abs(sine) < 1e-12:
        if cosine > 0:
            return pair
        return (-re, None if im is None else -im)
    if abs(cosine) < 1e-12:
        if im is None:
            return (None, re if sine > 0 else -re)
        return (-im, re) if sine > 0 else (im, -re)
    cosine, sine = np.float32(cosine), np.float32(sine)
    if im is None:
        return (re * cosine, re * sine)
    return (re * cosine - im * sine, re * sine + im * cosine)


def plus(a, b):
    if a is None:
        return b
    return a if b is None else a + b


def minus(a, b):
    if b is None:
        return a
    return -b if a is None else a - b


def small_dft(values, sign):
    count = len(values)
    if count == 1:
        return values
    even = small_dft(values[0::2], sign)
    odd = small_dft(values[1::2], sign)
    out = [None] * count
    for k in range(count // 2):
        angle = sign * 2.0 * math.pi * k / count
        turned = times(odd[k], math.cos(angle), math.sin(angle))
        out[k] = (plus(even[k][0], turned[0]), plus(even[k][1], turned[1]))
        out[k + count // 2] = (minus(even[k][0], turned[0]), minus(even[k][1], turned[1]))
    return out


def swap_groups(arrays):
    arrays = list(arrays)
    lane = lax.broadcasted_iota(jnp.int32, arrays[0].shape, arrays[0].ndim - 1)
    axis = arrays[0].ndim - 1
    for bit in range(3):
        shift = 16 << bit
        upper = (lane // shift) % 2 == 1
        for j in range(8):
            other = j | (1 << bit)
            if other == j:
                continue
            low, high = arrays[j], arrays[other]
            arrays[j] = jnp.where(upper, pltpu.roll(high, shift, axis), low)
            arrays[other] = jnp.where(upper, high, pltpu.roll(low, 128 - shift, axis))
    return arrays


def dot(a, b):
    return jnp.dot(a, b, preferred_element_type=f32)


def dot_nt(a, b):
    return lax.dot_general(a, b, (((1,), (1,)), ((), ())), preferred_element_type=f32)


def halves(value):
    high = value.astype(bf16)
    return high, (value - high.astype(f32)).astype(bf16)


def by_table(value, high, low):
    value_high, value_low = halves(value)
    return dot(value_high, high) + dot(value_low, high) + dot(value_high, low)


def table_by(high, low, value):
    value_high, value_low = halves(value)
    return dot(high, value_high) + dot(high, value_low) + dot(low, value_high)


def dropped(value):
    return value - value.astype(bf16).astype(f32)


def greet(vis_me, band_me, neighbours):
    barrier = pltpu.get_barrier_semaphore()

    def vis_signal(d, carry):
        pl.semaphore_signal(
            barrier, inc=1, device_id={"vis": vis_me ^ d}, device_id_type=MESH_ID
        )
        return carry

    def band_signal(d, carry):
        pl.semaphore_signal(
            barrier, inc=1, device_id={"band": band_me ^ d}, device_id_type=MESH_ID
        )
        return carry

    for neighbour in neighbours:
        pl.semaphore_signal(barrier, inc=1, device_id=neighbour, device_id_type=MESH_ID)
    lax.fori_loop(1, NV, vis_signal, 0)
    lax.fori_loop(1, NB, band_signal, 0)
    return barrier


def far_first(n, count):
    if count == NV:
        z, y = n // 8, n // 2 % 4
        return n % 2 + 2 * (z ^ z // 2) + 8 * (y ^ y // 2)
    x = n % 4
    return (x ^ x // 2) + n // 4 * 4


def launch(r, name, part, axis, count, me, same=False):
    sent, landed, sems = r["sent_" + name], r["got_" + name].at[part], r["sem_" + name]
    if not same:
        sent = sent.at[part]

    def body(step, carry):
        peer = me ^ far_first(count - step, count)
        pltpu.make_async_remote_copy(
            src_ref=sent if same else sent.at[peer],
            dst_ref=landed.at[me],
            send_sem=sems.at[2 * part],
            recv_sem=sems.at[2 * part + 1],
            device_id={axis: peer},
            device_id_type=MESH_ID,
        ).start()
        return carry

    lax.fori_loop(1, count, body, 0)
    landed[me] = sent[...] if same else sent[me]


def rest_copy(r, part, low, me):
    return pltpu.make_async_remote_copy(
        src_ref=r["sent_l"].at[part, low],
        dst_ref=r["got_l"].at[part, me],
        send_sem=r["sem_l"].at[2 * part],
        recv_sem=r["sem_l"].at[2 * part + 1],
        device_id={"vis": 4 * low},
        device_id_type=MESH_ID,
    )


def launch_rest(r, part, me):
    for low in range(8):

        @pl.when(me != 4 * low)
        def _():
            rest_copy(r, part, low, me).start()

        @pl.when(me == 4 * low)
        def _():
            r["got_l"][part, me] = r["sent_l"][part, low]


def rest_arrived(r, part, me):
    @pl.when(me % 4 == 0)
    def _():
        finish(r, "l", part, NV, 1)


def rest_drained(r, part, me):
    finish(r, "l", part, 8, 0)

    @pl.when(me % 4 != 0)
    def _():
        finish(r, "l", part, 2, 0)


def to_neighbour(sent, landed, sems, neighbour):
    copy = pltpu.make_async_remote_copy(
        src_ref=sent,
        dst_ref=landed,
        send_sem=sems.at[0],
        recv_sem=sems.at[1],
        device_id=neighbour,
        device_id_type=MESH_ID,
    )
    copy.start()
    return copy


def finish(r, name, part, count, side):
    landed = r["got_" + name].at[part]
    landed = landed.at[pl.ds(0, count - 1)]
    pltpu.make_async_copy(landed, landed, r["sem_" + name].at[2 * part + side]).wait()


def arrived(r, name, part, count):
    finish(r, name, part, count, 1)
    return r["got_" + name].at[part]


def step_kernel(*refs):
    names = INPUTS + OUTPUTS + list(SCRATCH)
    r = dict(zip(names, refs))
    vis_me, band_me = lax.axis_index("vis"), lax.axis_index("band")
    me = band_me * NV + vis_me
    following = (me + 1) % (NB * NV)
    preceding = (me + NB * NV - 1) % (NB * NV)
    following = {"band": following // NV, "vis": following % NV}
    preceding = {"band": preceding // NV, "vis": preceding % NV}
    copies = {}
    for place, name in enumerate(STAGED):
        copies[name] = pltpu.make_async_copy(r[name], r["here_" + name], r["sem_in"].at[place])
        copies[name].start()

    def staged(name):
        if name in copies:
            copies.pop(name).wait()
        return r["here_" + name]

    barrier = greet(vis_me, band_me, (following, preceding))

    to_row = (
        lax.broadcasted_iota(jnp.int32, (256, 32), 0) // 8
        == lax.broadcasted_iota(jnp.int32, (256, 32), 1)
    ).astype(f32).astype(bf16)
    column = r["rows"][...]
    facts = jnp.concatenate(
        [
            (column % 32 * 16 + column // 32 - 256).astype(f32),
            r["counts"][...].astype(f32),
            jnp.zeros((123, 32), f32),
        ],
        axis=0,
    ).astype(bf16)
    eye = (
        lax.broadcasted_iota(jnp.int32, (32, 32), 0)
        == lax.broadcasted_iota(jnp.int32, (32, 32), 1)
    ).astype(f32).astype(bf16)
    facts = dot_nt(eye, facts)
    r["sent_i"][0] = facts.reshape(NV, 1, 128)
    row_slot = lax.broadcasted_iota(jnp.int32, (256, 128), 0) % 8 // 2
    fact = lax.broadcasted_iota(jnp.int32, (256, 128), 1)

    def per_row(table, choice):
        wide = dot(to_row, table.astype(bf16))
        return jnp.sum(jnp.where(fact == choice, wide, 0.0), axis=1, keepdims=True)

    count = per_row(facts, 4)
    live = jnp.broadcast_to(count, (256, 32)) > (
        lax.broadcasted_iota(jnp.int32, (256, 32), 0) % 8 // 2
    ).astype(f32)
    live = jnp.where(live, 1.0, 0.0)
    vis_state = r["vis_state"][...].reshape(256, 32)
    vis_data = r["vis_data"][...].reshape(256, 32)
    data_square = jnp.sum(live * vis_data * vis_data)

    weights = dot((live * vis_state).astype(bf16), r["repeat"][...]).reshape(NV, 8, 256)
    wide_row = lax.broadcasted_iota(jnp.int32, (NV, 8, 256), 1)
    wide_lane = lax.broadcasted_iota(jnp.int32, (NV, 8, 256), 2)
    crossed = jnp.where(
        wide_row % 2 == 0, pltpu.roll(weights, 7, 1), -pltpu.roll(weights, 1, 1)
    )
    weights = jnp.where(wide_lane // 32 % 2 == 0, weights, crossed)
    r["weights"][...] = jnp.where(wide_lane // 64 == wide_row // 2, weights, 0.0).astype(bf16)
    twist_col = r["twist_col"]
    eye = (
        lax.broadcasted_iota(jnp.int32, (128, 128), 0)
        == lax.broadcasted_iota(jnp.int32, (128, 128), 1)
    )
    for c in range(2):
        one = jnp.broadcast_to(r["twists"][vis_me, c : c + 1, :], (128, 128))
        one = jnp.sum(jnp.where(eye, one, 0.0), axis=1, keepdims=True)
        twist_col[:, c] = jnp.broadcast_to(one, (128, 128)).reshape(8, 16, 128)

    kernels = staged("kernels")
    for q in range(NV):
        r["sent_a"][0, q] = dot(r["weights"][q], kernels[q]).astype(bf16)
    coef = staged("coef")
    for part in range(4):
        r["coef_rows"][3 * part : 3 * part + 3] = coef[part, 5:8, :]
    r["coef_rows"][12:16] = jnp.zeros((4, 2048), f32)
    r["got_l"][...] = jnp.zeros((2, NV, 8, 128), bf16)
    pl.semaphore_wait(barrier, NV + NB)
    launch(r, "i", 0, "vis", NV, vis_me)
    launch(r, "a", 0, "vis", NV, vis_me)

    order, onehot = r["order"], r["onehot"]
    where_to = per_row(arrived(r, "i", 0, NV)[...].reshape(NV, 128), row_slot)
    where_to = jnp.broadcast_to(where_to, (256, 128))
    lane = lax.broadcasted_iota(jnp.int32, (256, 128), 1).astype(f32)
    is_imag = lax.broadcasted_iota(jnp.int32, (256, 128), 0) % 2 == 1
    hots = [(where_to == lane + float(128 * g - 256)).astype(f32) for g in range(4)]
    for g in range(4):
        onehot[:, 128 * g : 128 * g + 128] = hots[g].astype(bf16)
    real_hots = [jnp.where(is_imag, 0.0, h).astype(bf16) for h in hots]
    imag_hots = [jnp.where(is_imag, h, 0.0).astype(bf16) for h in hots]
    hots = jnp.concatenate(real_hots + imag_hots, axis=1)
    contrib = arrived(r, "a", 0, NV)[...].astype(f32).reshape(256, 128).astype(bf16)
    turned = dot_nt(order[...], contrib).astype(bf16)
    for part in range(2):
        grid = dot(turned[64 * part : 64 * part + 64], hots)
        for c in range(2):
            for g in range(4):
                cols = slice(512 * c + 128 * g, 512 * c + 128 * g + 128)
                for low in range(8):
                    r["sent_b"][part, low * 4 + g, c] = grid[
                        8 * low : 8 * low + 8, cols
                    ].astype(bf16)
        launch(r, "b", part, "vis", NV, vis_me)

    table_hi, table_lo = staged("table_hi"), staged("table_lo")

    def spread_of(landed):
        return jnp.concatenate(
            [landed[:, 0].reshape(256, 128), landed[:, 1].reshape(256, 128)], axis=1
        )

    first = spread_of(arrived(r, "b", 0, NV))
    ahead = dot(table_hi[:, 0:256], first) + dot(table_lo[:, 0:256], first)
    second = spread_of(arrived(r, "b", 1, NV))
    for part in range(2):
        both = []
        for side in range(2):
            rows = slice(512 * side + 256 * part, 512 * side + 256 * part + 256)
            both.append(
                ahead[rows] + dot(table_hi[rows, 256:512], second)
                + dot(table_lo[rows, 256:512], second)
            )
        re = both[0][:, :128] - both[1][:, 128:]
        im = both[1][:, :128] + both[0][:, 128:]
        r["sent_c"][part, :, 0] = re.reshape(NV, 8, 128).astype(bf16)
        r["sent_c"][part, :, 1] = im.reshape(NV, 8, 128).astype(bf16)
        launch(r, "c", part, "vis", NV, vis_me)
    coef_copy = to_neighbour(r["coef_rows"], r["got_coef"], r["sem_coef"], following)

    sent_d = r["sent_d"]
    for part in range(2):
        got_c = arrived(r, "c", part, NV)
        rows = slice(8 * part, 8 * part + 8)
        for g in range(4):
            values = []
            for low in range(8):
                re = got_c[low * 4 + g, 0].astype(f32)
                im = got_c[low * 4 + g, 1].astype(f32)
                cosine, sine = twist_col[low, 0, rows], twist_col[low, 1, rows]
                values.append((re * cosine - im * sine, re * sine + im * cosine))
            values = small_dft(values, 1.0)
            for b in range(NB):
                for c in range(2):
                    sent_d[part, b, c, :, 128 * g : 128 * g + 128] = values[b][c].astype(
                        sent_d.dtype
                    )
        launch(r, "d", part, "band", NB, band_me)

    sky = staged("sky")
    sides_hi, sides_lo = r["sides_hi"], r["sides_lo"]
    up_hi, up_lo = staged("up_hi"), staged("up_lo")
    coef_copy.wait_recv()
    rows_up = []
    for part in range(2):
        rows = slice(16 * part, 16 * part + 16)
        stack = jnp.concatenate([coef[part], coef[part + 2], r["got_coef"][...]], axis=0)
        rows_up.append(table_by(sides_hi[rows, :], sides_lo[rows, :], stack))
    stack = []
    for n in range(16):
        parts = []
        for field in rows_up:
            for block in ((n + 15) % 16, n):
                parts.append(field[:, 128 * block : 128 * block + 128])
        stack.append(jnp.concatenate(parts, axis=1))
    smooth = by_table(jnp.concatenate(stack, axis=0), up_hi[...], up_lo[...])
    raw = r["raw_here"]
    for n in range(16):
        cols = slice(256 * n, 256 * n + 256)
        raw[:, cols] = sky[:, cols] - smooth[16 * n : 16 * n + 16]

    mid, twist_row, extrap, sent_e = r["mid"], r["twist_row"], r["extrap"], r["sent_e"]

    first_lane = lax.broadcasted_iota(jnp.int32, (8, 128), 1) == 0
    second_lane = lax.broadcasted_iota(jnp.int32, (8, 128), 1) == 1

    def lane_product(part):
        return by_table(
            mid[part].reshape(512, 128), r["lane_hi"][...], r["lane_lo"][...]
        ).reshape(32, 2, 8, 256)

    for part in range(2):
        rows = slice(8 * part, 8 * part + 8)
        got_d = arrived(r, "d", part, NB)
        for g in range(4):
            for c in range(2):
                parts = swap_groups(
                    [got_d[b, c, :, 128 * g : 128 * g + 128].astype(f32) for b in range(NB)]
                )
                for a in range(8):
                    mid[part, g * 8 + a, c] = parts[a]
        lanes = lane_product(part)
        values = []
        for a in range(32):
            re = lanes[a, 0, :, :128] - lanes[a, 1, :, 128:]
            im = lanes[a, 0, :, 128:] + lanes[a, 1, :, :128]
            cosine, sine = twist_row[a, 0:1], twist_row[a, 1:2]
            values.append((re * cosine - im * sine, re * sine + im * cosine))
        values = small_dft(values, 1.0)
        for n in range(32):
            cols = slice(128 * n, 128 * n + 128)
            now = jnp.maximum(raw[rows, cols] - values[n][0], 0.0)
            raw[rows, cols] = now
            extrap[part, :, cols] = 2.0 * now - sky[rows, cols]
        if part == 0:
            image_copy = to_neighbour(extrap.at[0], r["got_rows"], r["sem_rows"], preceding)
        values = [(extrap[part, :, 128 * n : 128 * n + 128], None) for n in range(32)]
        values = small_dft(values, -1.0)
        for a in range(32):
            re, im = values[a]
            cosine, sine = twist_row[a, 0:1], twist_row[a, 1:2]
            if im is None:
                mid[part, a, 0] = re * cosine
                mid[part, a, 1] = -re * sine
            else:
                mid[part, a, 0] = re * cosine + im * sine
                mid[part, a, 1] = im * cosine - re * sine
        lanes = lane_product(part)
        for g in range(4):
            cols = slice(128 * g, 128 * g + 128)
            reals, imags = [], []
            for a in range(8):
                re, im = lanes[g * 8 + a, 0], lanes[g * 8 + a, 1]
                reals.append(re[:, :128] + im[:, 128:])
                imags.append(im[:, :128] - re[:, 128:])
            reals, imags = swap_groups(reals), swap_groups(imags)
            if g == 0:
                imags[0] = jnp.where(first_lane, dropped(reals[0]), imags[0])
            for b in range(NB):
                sent_e[part, b, 0, :, cols] = reals[b].astype(bf16)
                sent_e[part, b, 1, :, cols] = imags[b].astype(bf16)
        launch(r, "e", part, "band", NB, band_me)
    out_image = pltpu.make_async_copy(raw, r["image"], r["sem_out"].at[0])
    out_image.start()

    sent_f = r["sent_f"]
    column_zero = jnp.where(first_lane, jnp.where(band_me == 0, 1.0, 0.0), 0.0)
    for part in range(2):
        got_e = arrived(r, "e", part, NB)
        rows = slice(8 * part, 8 * part + 8)
        for g in range(4):
            values = []
            for b in range(NB):
                re, im = (
                    got_e[b, c, :, 128 * g : 128 * g + 128].astype(f32) for c in range(2)
                )
                if g == 0:
                    re, im = re + im * column_zero, im * (1.0 - column_zero)
                values.append((re, im))
            values = small_dft(values, -1.0)
            for low in range(8):
                re, im = values[low]
                cosine, sine = twist_col[low, 0, rows], twist_col[low, 1, rows]
                re, im = re * cosine + im * sine, im * cosine - re * sine
                sent_f[part, low * 4 + g, 0] = re.astype(bf16)
                sent_f[part, low * 4 + g, 1] = im.astype(bf16)
                if g == 0:
                    rest = jnp.where(first_lane, dropped(re), 0.0)
                    rest = jnp.where(second_lane, pltpu.roll(dropped(im), 1, 1), rest)
                    r["sent_l"][part, low] = rest.astype(bf16)
        launch(r, "f", part, "vis", NV, vis_me)
        launch_rest(r, part, vis_me)

    down_hi, down_lo = staged("down_hi"), staged("down_lo")
    image_copy.wait_recv()
    fields = jnp.concatenate([extrap[0], extrap[1], r["got_rows"][...]], axis=0)
    fields = table_by(sides_hi[32:48, 0:24], sides_lo[32:48, 0:24], fields)
    stack = []
    for n in range(16):
        if n < 15:
            stack.append(fields[:, 256 * n : 256 * n + 384])
        else:
            stack.append(jnp.concatenate([fields[:, 3840:4096], fields[:, 0:128]], axis=1))
    found = by_table(jnp.concatenate(stack, axis=0), down_hi[...], down_lo[...])
    coeffs = r["coeffs_here"]
    for n in range(16):
        cols = slice(128 * n, 128 * n + 128)
        block = found[16 * n : 16 * n + 16]
        coeffs[0, :, cols] = coef[0, :, cols] + block[0:8, :128]
        coeffs[1, :, cols] = coef[1, :, cols] + block[0:8, 128:]
        coeffs[2, :, cols] = coef[2, :, cols] + block[8:16, :128]
        coeffs[3, :, cols] = coef[3, :, cols] + block[8:16, 128:]
    abs_total = jnp.sum(jnp.abs(found))
    out_coeffs = pltpu.make_async_copy(coeffs, r["coeffs"], r["sem_out"].at[1])
    out_coeffs.start()

    def through(rows, cols, spread, rest):
        wide = dot(table_hi[rows, cols], spread) + dot(table_lo[rows, cols], spread)
        rest = dot(table_hi[rows, cols], rest)
        one = lax.broadcasted_iota(jnp.int32, rest.shape, 1) == 0
        return wide + jnp.concatenate(
            [jnp.where(one, rest, 0.0), jnp.where(one, pltpu.roll(rest, 127, 1), 0.0)], axis=1
        )

    def rest_of(part):
        rest_arrived(r, part, vis_me)
        return r["got_l"][part].astype(f32).reshape(256, 128).astype(bf16)

    first = spread_of(arrived(r, "f", 0, NV))
    ahead = through(slice(0, 1024), slice(0, 256), first, rest_of(0))
    second = spread_of(arrived(r, "f", 1, NV))
    rest = rest_of(1)
    for part in range(2):
        both = []
        for side in range(2):
            rows = slice(512 * side + 256 * part, 512 * side + 256 * part + 256)
            both.append(ahead[rows] + through(rows, slice(256, 512), second, rest))
        re = both[0][:, :128] + both[1][:, 128:]
        im = both[0][:, 128:] - both[1][:, :128]
        r["sent_g"][part, :, 0] = re.reshape(NV, 8, 128).astype(bf16)
        r["sent_g"][part, :, 1] = im.reshape(NV, 8, 128).astype(bf16)
        launch(r, "g", part, "vis", NV, vis_me)

    picked = [[], []]
    for part in range(2):
        got_g = arrived(r, "g", part, NV)
        for c in range(2):
            total = 0.0
            for g in range(4):
                piece = jnp.concatenate(
                    [got_g[low * 4 + g, c].astype(f32) for low in range(8)], axis=0
                ).astype(bf16)
                total = total + dot_nt(onehot[:, 128 * g : 128 * g + 128], piece)
            picked[c].append(total)
    picked = [jnp.concatenate(p, axis=1) for p in picked]
    tiles = jnp.where(is_imag, picked[1], picked[0]).astype(bf16)
    tiles = dot(tiles, order[...])
    r["sent_h"][0] = tiles.reshape(NV, 8, 128).astype(bf16)
    launch(r, "h", 0, "vis", NV, vis_me)
    got_h = arrived(r, "h", 0, NV)

    products = jnp.stack([dot_nt(got_h[q], kernels[q]) for q in range(NV)])
    products = jnp.where(wide_lane // 64 == wide_row // 2, products, 0.0)
    products = products[:, :, 0:128] + products[:, :, 128:256]
    products = products + pltpu.roll(products, 64, 2)
    other = pltpu.roll(products, 96, 2)
    row = lax.broadcasted_iota(jnp.int32, (NV, 8, 128), 1)
    products = products + jnp.where(
        row % 2 == 0, -pltpu.roll(other, 7, 1), pltpu.roll(other, 1, 1)
    )
    predicted = products.reshape(256, 128)[:, 0:32]
    residual = live * (vis_state + predicted - vis_data)
    resid_square = jnp.sum(residual * residual)
    r["residual"][...] = residual.reshape(NV, 4, 2, 32)

    sent_t, sent_u = r["sent_t"], r["sent_u"]
    spot = lax.broadcasted_iota(jnp.int32, (1, 128), 1)
    sent_t[...] = jnp.where(
        spot == 0, abs_total, jnp.where(spot == 1, resid_square, data_square)
    )
    launch(r, "t", 0, "vis", NV, vis_me, same=True)
    sent_u[...] = jnp.sum(arrived(r, "t", 0, NV)[...], axis=0)
    launch(r, "u", 0, "band", NB, band_me, same=True)
    totals = jnp.sum(arrived(r, "u", 0, NB)[...], axis=0)
    r["totals"][...] = totals

    for copy in (coef_copy, image_copy):
        copy.wait_send()
    out_image.wait()
    out_coeffs.wait()
    for name in "abcdefghitu":
        for part in range(2 if name in "bcdefg" else 1):
            finish(r, name, part, NB if name in "deu" else NV, 0)
    for part in range(2):
        rest_drained(r, part, vis_me)


STAGED = ["kernels", "coef", "sky", "up_hi", "up_lo", "table_hi", "table_lo", "down_hi", "down_lo"]
INPUTS = STAGED + [
    "vis_state", "vis_data", "rows", "counts", "repeat", "lane_hi", "lane_lo",
    "twist_row", "twists", "order", "sides_hi", "sides_lo",
]
OUTPUTS = ["image", "coeffs", "residual", "totals"]
VIS_TILE = (2, NV, 2, 8, 128)
BAND_TILE = (2, NB, 2, 8, 512)
SCRATCH = dict(
    here_kernels=((NV, 256, 128), bf16),
    here_coef=((4, 8, 2048), f32),
    here_sky=((16, IMG), f32),
    here_up_hi=((512, 256), bf16),
    here_up_lo=((512, 256), bf16),
    here_table_hi=((1024, 512), bf16),
    here_table_lo=((1024, 512), bf16),
    here_down_hi=((384, 256), bf16),
    here_down_lo=((384, 256), bf16),
    sent_a=((1, NV, 8, 128), bf16), got_a=((1, NV, 8, 128), bf16),
    sent_i=((1, NV, 1, 128), f32), got_i=((1, NV, 1, 128), f32),
    sent_b=(VIS_TILE, bf16), got_b=(VIS_TILE, bf16),
    sent_c=(VIS_TILE, bf16), got_c=(VIS_TILE, bf16),
    sent_d=(BAND_TILE, bf16), got_d=(BAND_TILE, bf16),
    sent_e=(BAND_TILE, bf16), got_e=(BAND_TILE, bf16),
    sent_f=(VIS_TILE, bf16), got_f=(VIS_TILE, bf16),
    sent_l=((2, 8, 8, 128), bf16), got_l=((2, NV, 8, 128), bf16),
    sent_g=(VIS_TILE, bf16), got_g=(VIS_TILE, bf16),
    sent_h=((1, NV, 8, 128), bf16), got_h=((1, NV, 8, 128), bf16),
    sent_t=((1, 128), f32), got_t=((1, NV, 1, 128), f32),
    sent_u=((1, 128), f32), got_u=((1, NB, 1, 128), f32),
    weights=((NV, 8, 256), bf16), twist_col=((8, 2, 16, 128), f32), coef_rows=((16, 2048), f32),
    got_coef=((16, 2048), f32), got_rows=((8, IMG), f32),
    raw_here=((16, IMG), f32), extrap=((2, 8, IMG), f32), coeffs_here=((4, 8, 2048), f32),
    onehot=((256, 512), bf16), mid=((2, 32, 2, 8, 128), f32),
    **{"sem_" + n: 4 for n in list("abcdefghiltu") + ["coef", "rows", "out"]},
    sem_in=len(STAGED),
)


def step(inputs):
    anywhere = pl.BlockSpec(memory_space=pl.ANY)
    vmem = pl.BlockSpec(memory_space=pltpu.VMEM)
    scratch = []
    for what in SCRATCH.values():
        if isinstance(what, int):
            scratch.append(pltpu.SemaphoreType.DMA((what,)))
        else:
            scratch.append(pltpu.VMEM(*what))
    return pl.pallas_call(
        step_kernel,
        out_shape=(
            jax.ShapeDtypeStruct((16, IMG), f32),
            jax.ShapeDtypeStruct((4, 8, 2048), f32),
            jax.ShapeDtypeStruct((NV, 4, 2, 32), f32),
            jax.ShapeDtypeStruct((1, 128), f32),
        ),
        in_specs=[anywhere if name in STAGED else vmem for name in INPUTS],
        out_specs=(anywhere, anywhere, vmem, vmem),
        scratch_shapes=scratch,
        compiler_params=pltpu.CompilerParams(
            collective_id=0, has_side_effects=True, vmem_limit_bytes=56 * 2**20
        ),
    )(*[inputs[name] for name in INPUTS])


def closing_kernel(*refs):
    given, out, here, sems = refs[0:4], refs[4:7], refs[7:11], refs[11]
    copies = [pltpu.make_async_copy(given[n], here[n], sems.at[n]) for n in range(4)]
    for copy in copies:
        copy.start()

    def hand_out(n):
        copies[n] = pltpu.make_async_copy(here[n], out[n], sems.at[n])
        copies[n].start()

    spot = lax.broadcasted_iota(jnp.int32, (1, 128), 1)
    copies.pop().wait()
    copies[0].wait()
    hand_out(0)
    abs_total, resid_square, data_square = (
        jnp.sum(jnp.where(spot == n, here[3][...], 0.0), axis=1, keepdims=True)
        for n in range(3)
    )
    limit = jnp.broadcast_to(0.5 * abs_total / (IMG * IMG), (8, 2048))
    copies[1].wait()
    for part in range(4):
        here[1][part] = jnp.maximum(jnp.minimum(here[1][part], limit), -limit)
    hand_out(1)
    radius = 0.5 * jnp.sqrt(data_square + 1e-06)
    size = jnp.sqrt(resid_square + 1e-06)
    factor = 1.0 - jnp.minimum(1.0, radius / size)
    copies[2].wait()
    here[2][...] = here[2][...] * jnp.broadcast_to(factor.reshape(1, 1, 1, 1), (NV, 4, 2, 32))
    hand_out(2)
    for copy in copies:
        copy.wait()


def closing(results):
    anywhere = pl.BlockSpec(memory_space=pl.ANY)
    return pl.pallas_call(
        closing_kernel,
        out_shape=tuple(jax.ShapeDtypeStruct(x.shape, x.dtype) for x in results[:3]),
        in_specs=[anywhere] * 4,
        out_specs=(anywhere,) * 3,
        scratch_shapes=[pltpu.VMEM(x.shape, x.dtype) for x in results]
        + [pltpu.SemaphoreType.DMA((4,))],
    )(*results)


def local(sky_image, coef_dual, vis_dual, visibilities, kernel_blocks, tile_rows, tile_counts):
    names = (
        "table_hi", "table_lo", "lane_hi", "lane_lo",
        "up_hi", "up_lo", "down_hi", "down_lo", "sides_hi", "sides_lo",
    )
    inputs = dict(zip(names, dft512_tables() + dft128_tables() + wavelet_tables()))
    inputs.update(
        twist_row=row_twist(), twists=col_twist(), order=lane_order(), repeat=repeat_table()
    )
    inputs = {name: jnp.asarray(table) for name, table in inputs.items()}
    inputs.update(
        kernels=kernel_blocks.reshape(NV, 256, 128),
        coef=coef_dual,
        sky=sky_image,
        vis_state=vis_dual.reshape(NV, 4, 2, 32),
        vis_data=visibilities.reshape(NV, 4, 2, 32),
        rows=tile_rows.reshape(NV, 4).T,
        counts=tile_counts.reshape(1, NV),
    )
    image, coeffs, vis_new = closing(step(inputs))
    return (image, coeffs, vis_new.reshape(1, 1, NV, 4, 2, 32))


def solution(mesh):
    return jax.shard_map(
        local,
        mesh=mesh,
        in_specs=(
            P(("band", "vis"), None),
            P(None, ("band", "vis"), None),
            P("band", "vis", None, None, None, None),
            P("band", "vis", None, None, None, None),
            P("band", "vis", None, None, None, None, None),
            P("band", "vis", None, None),
            P("band", "vis", None),
        ),
        out_specs=(
            P(("band", "vis"), None),
            P(None, ("band", "vis"), None),
            P("band", "vis", None, None, None, None),
        ),
        check_vma=False,
    )
```

```python
import functools
import math

import jax
import jax.numpy as jnp
import numpy as np
from jax import lax
from jax.experimental import pallas as pl
from jax.experimental.pallas import tpu as pltpu
from jax.sharding import PartitionSpec as P

IMG = 4096
NB = 8
NV = 32
MESH_ID = pl.DeviceIdType.MESH
f32 = jnp.float32
bf16 = jnp.bfloat16

low_taps = (
    -0.010597401784997278,
    0.032883011666982945,
    0.030841381835986965,
    -0.18703481171888114,
    -0.02798376941698385,
    0.6308807679295904,
    0.7148465705525415,
    0.23037781330885523,
)
high_taps = tuple(((-1.0) ** offset * low_taps[7 - offset] for offset in range(8)))


def halves_of(table):
    high = table.astype(bf16)
    low = (table - high.astype(np.float64)).astype(bf16)
    return high, low


def dft512_tables():
    index = np.arange(512).reshape(32, 2, 8).transpose(1, 0, 2).reshape(512)
    angle = 2.0 * np.pi / 512 * (index[:, None] * index[None, :] % 512)
    return halves_of(np.concatenate([np.cos(angle), np.sin(angle)], axis=0))


def dft128_tables():
    index = np.arange(128)
    angle = 2.0 * np.pi / 128 * (index[:, None] * index[None, :] % 128)
    return halves_of(np.concatenate([np.cos(angle), np.sin(angle)], axis=1) / IMG)


def row_twist():
    angle = 2.0 * np.pi / IMG * (np.arange(32)[:, None] * np.arange(128)[None, :] % IMG)
    return np.stack([np.cos(angle), np.sin(angle)], axis=1).astype(np.float32)


def col_twist():
    low, row = np.arange(8)[None, :, None], np.arange(16)[None, None, :]
    angle = 2.0 * np.pi / IMG * (low * (16 * np.arange(NV)[:, None, None] + row))
    return np.stack([np.cos(angle), np.sin(angle)], axis=1).reshape(NV, 2, 128).astype(np.float32)


def repeat_table():
    return np.tile(np.eye(32), (1, 8)).astype(bf16)


def wavelet_tables():
    up = np.zeros((512, 256))
    down = np.zeros((384, 256))
    rows_up = np.zeros((2, 16, 32))
    rows_down = np.zeros((16, 24))
    for tap in range(8):
        for side, taps in ((0, low_taps), (1, high_taps)):
            for k in range(128):
                down[2 * k + tap, 128 * side + k] = taps[tap]
            for k in range(-128, 128):
                if 0 <= 2 * k + tap < 256:
                    up[256 * side + 128 + k, 2 * k + tap] = taps[tap]
            for k in range(8):
                rows_down[8 * side + k, 2 * k + tap] = taps[tap]
            for k in range(-3, 8):
                if 0 <= 2 * k + tap < 16:
                    for part in range(2):
                        spot = 8 * side + k if k >= 0 else 16 + 3 * (part + 2 * side) + k + 3
                        rows_up[part, 2 * k + tap, spot] = taps[tap]
    sides = np.zeros((48, 32))
    sides[0:32] = rows_up.reshape(32, 32)
    sides[32:48, 0:24] = rows_down
    return tuple(part for table in (up, down, sides) for part in halves_of(table))


def lane_order():
    place = np.zeros((128, 128), np.float32)
    for t in range(128):
        place[t // 64 * 64 + (t % 8) * 8 + t // 8 % 8, t] = 1.0
    return place.astype(bf16)


def times(pair, cosine, sine):
    re, im = pair
    if abs(sine) < 1e-12:
        if cosine > 0:
            return pair
        return (-re, None if im is None else -im)
    if abs(cosine) < 1e-12:
        if im is None:
            return (None, re if sine > 0 else -re)
        return (-im, re) if sine > 0 else (im, -re)
    cosine, sine = np.float32(cosine), np.float32(sine)
    if im is None:
        return (re * cosine, re * sine)
    return (re * cosine - im * sine, re * sine + im * cosine)


def plus(a, b):
    if a is None:
        return b
    return a if b is None else a + b


def minus(a, b):
    if b is None:
        return a
    return -b if a is None else a - b


def small_dft(values, sign):
    count = len(values)
    if count == 1:
        return values
    even = small_dft(values[0::2], sign)
    odd = small_dft(values[1::2], sign)
    out = [None] * count
    for k in range(count // 2):
        angle = sign * 2.0 * math.pi * k / count
        turned = times(odd[k], math.cos(angle), math.sin(angle))
        out[k] = (plus(even[k][0], turned[0]), plus(even[k][1], turned[1]))
        out[k + count // 2] = (minus(even[k][0], turned[0]), minus(even[k][1], turned[1]))
    return out


def swap_groups(arrays, width=16):
    arrays = list(arrays)
    axis = arrays[0].ndim - 1
    lane = lax.broadcasted_iota(jnp.int32, arrays[0].shape, axis)
    bit = 1
    while bit < len(arrays):
        shift = width * bit
        upper = (lane // shift) % 2 == 1
        for j in range(len(arrays)):
            other = j | bit
            if other == j:
                continue
            low, high = arrays[j], arrays[other]
            arrays[j] = jnp.where(upper, pltpu.roll(high, shift, axis), low)
            arrays[other] = jnp.where(upper, high, pltpu.roll(low, 128 - shift, axis))
        bit *= 2
    return arrays


def dot(a, b):
    return jnp.dot(a, b, preferred_element_type=f32)


def dot_nt(a, b):
    return lax.dot_general(a, b, (((1,), (1,)), ((), ())), preferred_element_type=f32)


def halves(value):
    high = value.astype(bf16)
    return high, (value - high.astype(f32)).astype(bf16)


def by_table(value, high, low):
    value_high, value_low = halves(value)
    return dot(value_high, high) + dot(value_low, high) + dot(value_high, low)


def table_by(high, low, value):
    value_high, value_low = halves(value)
    return dot(high, value_high) + dot(high, value_low) + dot(low, value_high)


def dropped(value):
    return value - value.astype(bf16).astype(f32)


def greet(vis_me, band_me, neighbours):
    barrier = pltpu.get_barrier_semaphore()

    def vis_signal(d, carry):
        pl.semaphore_signal(
            barrier, inc=1, device_id={"vis": vis_me ^ d}, device_id_type=MESH_ID
        )
        return carry

    def band_signal(d, carry):
        pl.semaphore_signal(
            barrier, inc=1, device_id={"band": band_me ^ d}, device_id_type=MESH_ID
        )
        return carry

    for neighbour in neighbours:
        pl.semaphore_signal(barrier, inc=1, device_id=neighbour, device_id_type=MESH_ID)
    lax.fori_loop(1, NV, vis_signal, 0)
    lax.fori_loop(1, NB, band_signal, 0)
    return barrier


def far_first(n, count):
    if count == NV:
        z, y = n // 8, n // 2 % 4
        return n % 2 + 2 * (z ^ z // 2) + 8 * (y ^ y // 2)
    x = n % 4
    return (x ^ x // 2) + n // 4 * 4


def launch(r, name, part, axis, count, me, same=False):
    sent, landed, sems = r["sent_" + name], r["got_" + name].at[part], r["sem_" + name]
    if not same:
        sent = sent.at[part]

    def body(step, carry):
        peer = me ^ far_first(count - step, count)
        pltpu.make_async_remote_copy(
            src_ref=sent if same else sent.at[peer],
            dst_ref=landed.at[me],
            send_sem=sems.at[2 * part],
            recv_sem=sems.at[2 * part + 1],
            device_id={axis: peer},
            device_id_type=MESH_ID,
        ).start()
        return carry

    lax.fori_loop(1, count, body, 0)
    landed[me] = sent[...] if same else sent[me]


def rest_copy(r, part, low, me):
    return pltpu.make_async_remote_copy(
        src_ref=r["sent_l"].at[part, low],
        dst_ref=r["got_l"].at[part, me],
        send_sem=r["sem_l"].at[2 * part],
        recv_sem=r["sem_l"].at[2 * part + 1],
        device_id={"vis": 4 * low},
        device_id_type=MESH_ID,
    )


def launch_rest(r, part, me):
    for low in range(8):

        @pl.when(me != 4 * low)
        def _():
            rest_copy(r, part, low, me).start()

        @pl.when(me == 4 * low)
        def _():
            r["got_l"][part, me] = r["sent_l"][part, low]


def rest_arrived(r, part, me):
    @pl.when(me % 4 == 0)
    def _():
        finish(r, "l", part, NV, 1)


def rest_drained(r, part, me):
    finish(r, "l", part, 8, 0)

    @pl.when(me % 4 != 0)
    def _():
        finish(r, "l", part, 2, 0)


def to_neighbour(sent, landed, sems, neighbour):
    copy = pltpu.make_async_remote_copy(
        src_ref=sent,
        dst_ref=landed,
        send_sem=sems.at[0],
        recv_sem=sems.at[1],
        device_id=neighbour,
        device_id_type=MESH_ID,
    )
    copy.start()
    return copy


def finish(r, name, part, count, side):
    landed = r["got_" + name].at[part]
    landed = landed.at[pl.ds(0, count - 1)]
    pltpu.make_async_copy(landed, landed, r["sem_" + name].at[2 * part + side]).wait()


def arrived(r, name, part, count):
    finish(r, name, part, count, 1)
    return r["got_" + name].at[part]


def step_kernel(*refs):
    names = INPUTS + OUTPUTS + list(SCRATCH)
    r = dict(zip(names, refs))
    vis_me, band_me = lax.axis_index("vis"), lax.axis_index("band")
    me = band_me * NV + vis_me
    following = (me + 1) % (NB * NV)
    preceding = (me + NB * NV - 1) % (NB * NV)
    following = {"band": following // NV, "vis": following % NV}
    preceding = {"band": preceding // NV, "vis": preceding % NV}
    copies = {}
    for place, name in enumerate(STAGED):
        copies[name] = pltpu.make_async_copy(r[name], r["here_" + name], r["sem_in"].at[place])
        copies[name].start()

    def staged(name):
        if name in copies:
            copies.pop(name).wait()
        return r["here_" + name]

    barrier = greet(vis_me, band_me, (following, preceding))

    to_row = (
        lax.broadcasted_iota(jnp.int32, (256, 32), 0) // 8
        == lax.broadcasted_iota(jnp.int32, (256, 32), 1)
    ).astype(f32).astype(bf16)
    column = r["rows"][...]
    facts = jnp.concatenate(
        [
            (column % 32 * 16 + column // 32 - 256).astype(f32),
            r["counts"][...].astype(f32),
            jnp.zeros((123, 32), f32),
        ],
        axis=0,
    ).astype(bf16)
    eye = (
        lax.broadcasted_iota(jnp.int32, (32, 32), 0)
        == lax.broadcasted_iota(jnp.int32, (32, 32), 1)
    ).astype(f32).astype(bf16)
    facts = dot_nt(eye, facts)
    place = (column % 32 * 16 + column // 32 - 256).astype(f32)
    r["sent_i"][...] = jnp.concatenate([place[n : n + 1] for n in range(4)], axis=1)
    row, col = (lax.broadcasted_iota(jnp.int32, (256, 256), n) for n in range(2))
    source = row // 8 % 8 * 32 + row % 2 * 16 + row // 64 * 4 + row % 8 // 2
    r["reorder"][...] = (col == source).astype(f32).astype(bf16)
    r["blocks"][...] = jnp.zeros((4, 128, 1024), bf16)
    row_slot = lax.broadcasted_iota(jnp.int32, (256, 128), 0) % 8 // 2
    fact = lax.broadcasted_iota(jnp.int32, (256, 128), 1)

    def per_row(table, choice):
        wide = dot(to_row, table.astype(bf16))
        return jnp.sum(jnp.where(fact == choice, wide, 0.0), axis=1, keepdims=True)

    count = per_row(facts, 4)
    live = jnp.broadcast_to(count, (256, 32)) > (
        lax.broadcasted_iota(jnp.int32, (256, 32), 0) % 8 // 2
    ).astype(f32)
    live = jnp.where(live, 1.0, 0.0)
    vis_state = r["vis_state"][...].reshape(256, 32)
    vis_data = r["vis_data"][...].reshape(256, 32)
    data_square = jnp.sum(live * vis_data * vis_data)

    weights = dot((live * vis_state).astype(bf16), r["repeat"][...]).reshape(NV, 8, 256)
    wide_row = lax.broadcasted_iota(jnp.int32, (NV, 8, 256), 1)
    wide_lane = lax.broadcasted_iota(jnp.int32, (NV, 8, 256), 2)
    crossed = jnp.where(
        wide_row % 2 == 0, pltpu.roll(weights, 7, 1), -pltpu.roll(weights, 1, 1)
    )
    weights = jnp.where(wide_lane // 32 % 2 == 0, weights, crossed)
    r["weights"][...] = jnp.where(wide_lane // 64 == wide_row // 2, weights, 0.0).astype(bf16)
    twist_col = r["twist_col"]
    eye = (
        lax.broadcasted_iota(jnp.int32, (128, 128), 0)
        == lax.broadcasted_iota(jnp.int32, (128, 128), 1)
    )
    for c in range(2):
        one = jnp.broadcast_to(r["twists"][vis_me, c : c + 1, :], (128, 128))
        one = jnp.sum(jnp.where(eye, one, 0.0), axis=1, keepdims=True)
        twist_col[:, c] = jnp.broadcast_to(one, (128, 128)).reshape(8, 16, 128)

    kernels = staged("kernels")
    for q in range(NV):
        r["sent_a"][0, q] = dot(r["weights"][q], kernels[q]).astype(bf16)
    coef = staged("coef")
    for part in range(4):
        r["coef_rows"][3 * part : 3 * part + 3] = coef[part, 5:8, :]
    r["coef_rows"][12:16] = jnp.zeros((4, 2048), f32)
    r["got_l"][...] = jnp.zeros((2, NV, 8, 128), bf16)
    pl.semaphore_wait(barrier, NV + NB)
    launch(r, "i", 0, "vis", NV, vis_me, same=True)
    launch(r, "a", 0, "vis", NV, vis_me)
    coef_copy = to_neighbour(r["coef_rows"], r["got_coef"], r["sem_coef"], following)

    order = r["order"]
    positions = arrived(r, "i", 0, NV)[...].reshape(NV, 128)
    where_to = per_row(positions, 32 * row_slot + vis_me)
    where_to = jnp.broadcast_to(where_to, (256, 128))
    lane = lax.broadcasted_iota(jnp.int32, (256, 128), 1).astype(f32)
    is_imag = lax.broadcasted_iota(jnp.int32, (256, 128), 0) % 2 == 1
    hots = [(where_to == lane + float(128 * g - 256)).astype(f32) for g in range(4)]
    real_hots = [jnp.where(is_imag, 0.0, h).astype(bf16) for h in hots]
    imag_hots = [jnp.where(is_imag, h, 0.0).astype(bf16) for h in hots]
    hots = jnp.concatenate(real_hots + imag_hots, axis=1)
    contrib = arrived(r, "a", 0, NV)[...].astype(f32).reshape(256, 128).astype(bf16)
    turned = dot_nt(order[...], contrib).astype(bf16)
    for part in range(2):
        grid = dot(turned[64 * part : 64 * part + 64], hots)
        for c in range(2):
            for g in range(4):
                cols = slice(512 * c + 128 * g, 512 * c + 128 * g + 128)
                for low in range(8):
                    r["sent_b"][part, low * 4 + g, c] = grid[
                        8 * low : 8 * low + 8, cols
                    ].astype(bf16)
        launch(r, "b", part, "vis", NV, vis_me)

    to_row = (
        lax.broadcasted_iota(jnp.int32, (128, 32), 0) // 4
        == lax.broadcasted_iota(jnp.int32, (128, 32), 1)
    ).astype(f32).astype(bf16)
    row, lane = (lax.broadcasted_iota(jnp.int32, (128, 128), n) for n in range(2))
    wide = jnp.where(lane // 32 == row % 4, dot(to_row, positions.astype(bf16)), 0.0)
    wide = wide + pltpu.roll(wide, 64, 1)
    wide = wide + pltpu.roll(wide, 32, 1)
    here = (lane + 128 * (vis_me % 4) - 256).astype(f32)
    for q in range(NV):
        hot = jnp.broadcast_to(wide[:, q : q + 1], (128, 128)) == here
        cols = slice(128 * (q % 8), 128 * (q % 8) + 128)
        r["hots"][q // 8, :, cols] = hot.astype(f32).astype(bf16)

    sky = staged("sky")
    sides_hi, sides_lo = r["sides_hi"], r["sides_lo"]
    up_hi, up_lo = staged("up_hi"), staged("up_lo")
    coef_copy.wait_recv()
    rows_up = []
    for part in range(2):
        rows = slice(16 * part, 16 * part + 16)
        stack = jnp.concatenate([coef[part], coef[part + 2], r["got_coef"][...]], axis=0)
        rows_up.append(table_by(sides_hi[rows, :], sides_lo[rows, :], stack))
    stack = []
    for n in range(16):
        parts = []
        for field in rows_up:
            for block in ((n + 15) % 16, n):
                parts.append(field[:, 128 * block : 128 * block + 128])
        stack.append(jnp.concatenate(parts, axis=1))
    smooth = by_table(jnp.concatenate(stack, axis=0), up_hi[...], up_lo[...])
    raw = r["raw_here"]
    for n in range(16):
        cols = slice(256 * n, 256 * n + 256)
        raw[:, cols] = sky[:, cols] - smooth[16 * n : 16 * n + 16]

    table_hi, table_lo = staged("table_hi"), staged("table_lo")

    def spread_of(landed):
        return jnp.concatenate(
            [landed[:, 0].reshape(256, 128), landed[:, 1].reshape(256, 128)], axis=1
        )

    first = spread_of(arrived(r, "b", 0, NV))
    ahead = dot(table_hi[:, 0:256], first) + dot(table_lo[:, 0:256], first)
    second = spread_of(arrived(r, "b", 1, NV))
    for part in range(2):
        both = []
        for side in range(2):
            rows = slice(512 * side + 256 * part, 512 * side + 256 * part + 256)
            both.append(
                ahead[rows] + dot(table_hi[rows, 256:512], second)
                + dot(table_lo[rows, 256:512], second)
            )
        re = both[0][:, :128] - both[1][:, 128:]
        im = both[1][:, :128] + both[0][:, 128:]
        r["sent_c"][part, :, 0] = re.reshape(NV, 8, 128).astype(bf16)
        r["sent_c"][part, :, 1] = im.reshape(NV, 8, 128).astype(bf16)
        launch(r, "c", part, "vis", NV, vis_me)

    sent_d = r["sent_d"]
    for part in range(2):
        got_c = arrived(r, "c", part, NV)
        rows = slice(8 * part, 8 * part + 8)
        for g in range(4):
            values = []
            for low in range(8):
                re = got_c[low * 4 + g, 0].astype(f32)
                im = got_c[low * 4 + g, 1].astype(f32)
                cosine, sine = twist_col[low, 0, rows], twist_col[low, 1, rows]
                values.append((re * cosine - im * sine, re * sine + im * cosine))
            values = small_dft(values, 1.0)
            for b in range(NB):
                for c in range(2):
                    sent_d[part, b, c, :, 128 * g : 128 * g + 128] = values[b][c].astype(
                        sent_d.dtype
                    )
        launch(r, "d", part, "band", NB, band_me)

    mid, twist_row, extrap, sent_e = r["mid"], r["twist_row"], r["extrap"], r["sent_e"]

    first_lane = lax.broadcasted_iota(jnp.int32, (8, 128), 1) == 0
    second_lane = lax.broadcasted_iota(jnp.int32, (8, 128), 1) == 1

    def lane_product(part):
        return by_table(
            mid[part].reshape(512, 128), r["lane_hi"][...], r["lane_lo"][...]
        ).reshape(32, 2, 8, 256)

    for part in range(2):
        rows = slice(8 * part, 8 * part + 8)
        got_d = arrived(r, "d", part, NB)
        for g in range(4):
            for c in range(2):
                parts = swap_groups(
                    [got_d[b, c, :, 128 * g : 128 * g + 128].astype(f32) for b in range(NB)]
                )
                for a in range(8):
                    mid[part, g * 8 + a, c] = parts[a]
        lanes = lane_product(part)
        values = []
        for a in range(32):
            re = lanes[a, 0, :, :128] - lanes[a, 1, :, 128:]
            im = lanes[a, 0, :, 128:] + lanes[a, 1, :, :128]
            cosine, sine = twist_row[a, 0:1], twist_row[a, 1:2]
            values.append((re * cosine - im * sine, re * sine + im * cosine))
        values = small_dft(values, 1.0)
        for n in range(32):
            cols = slice(128 * n, 128 * n + 128)
            now = jnp.maximum(raw[rows, cols] - values[n][0], 0.0)
            raw[rows, cols] = now
            extrap[part, :, cols] = 2.0 * now - sky[rows, cols]
        values = [(extrap[part, :, 128 * n : 128 * n + 128], None) for n in range(32)]
        values = small_dft(values, -1.0)
        for a in range(32):
            re, im = values[a]
            cosine, sine = twist_row[a, 0:1], twist_row[a, 1:2]
            if im is None:
                mid[part, a, 0] = re * cosine
                mid[part, a, 1] = -re * sine
            else:
                mid[part, a, 0] = re * cosine + im * sine
                mid[part, a, 1] = im * cosine - re * sine
        lanes = lane_product(part)
        for g in range(4):
            cols = slice(128 * g, 128 * g + 128)
            reals, imags = [], []
            for a in range(8):
                re, im = lanes[g * 8 + a, 0], lanes[g * 8 + a, 1]
                reals.append(re[:, :128] + im[:, 128:])
                imags.append(im[:, :128] - re[:, 128:])
            reals, imags = swap_groups(reals), swap_groups(imags)
            if g == 0:
                imags[0] = jnp.where(first_lane, dropped(reals[0]), imags[0])
            for b in range(NB):
                sent_e[part, b, 0, :, cols] = reals[b].astype(bf16)
                sent_e[part, b, 1, :, cols] = imags[b].astype(bf16)
        launch(r, "e", part, "band", NB, band_me)
    out_image = pltpu.make_async_copy(raw, r["image"], r["sem_out"].at[0])
    out_image.start()

    sent_f = r["sent_f"]
    column_zero = jnp.where(first_lane, jnp.where(band_me == 0, 1.0, 0.0), 0.0)
    for part in range(2):
        got_e = arrived(r, "e", part, NB)
        rows = slice(8 * part, 8 * part + 8)
        for g in range(4):
            values = []
            for b in range(NB):
                re, im = (
                    got_e[b, c, :, 128 * g : 128 * g + 128].astype(f32) for c in range(2)
                )
                if g == 0:
                    re, im = re + im * column_zero, im * (1.0 - column_zero)
                values.append((re, im))
            values = small_dft(values, -1.0)
            for low in range(8):
                re, im = values[low]
                cosine, sine = twist_col[low, 0, rows], twist_col[low, 1, rows]
                re, im = re * cosine + im * sine, im * cosine - re * sine
                sent_f[part, low * 4 + g, 0] = re.astype(bf16)
                sent_f[part, low * 4 + g, 1] = im.astype(bf16)
                if g == 0:
                    rest = jnp.where(first_lane, dropped(re), 0.0)
                    rest = jnp.where(second_lane, pltpu.roll(dropped(im), 1, 1), rest)
                    r["sent_l"][part, low] = rest.astype(bf16)
        launch(r, "f", part, "vis", NV, vis_me)
        launch_rest(r, part, vis_me)
    image_copy = to_neighbour(extrap.at[0], r["got_rows"], r["sem_rows"], preceding)

    def through(rows, cols, spread, rest):
        wide = dot(table_hi[rows, cols], spread) + dot(table_lo[rows, cols], spread)
        rest = dot(table_hi[rows, cols], rest)
        one = lax.broadcasted_iota(jnp.int32, rest.shape, 1) == 0
        return wide + jnp.concatenate(
            [jnp.where(one, rest, 0.0), jnp.where(one, pltpu.roll(rest, 127, 1), 0.0)], axis=1
        )

    def rest_of(part):
        rest_arrived(r, part, vis_me)
        return r["got_l"][part].astype(f32).reshape(256, 128).astype(bf16)

    first = spread_of(arrived(r, "f", 0, NV))
    ahead = through(slice(0, 1024), slice(0, 256), first, rest_of(0))
    second = spread_of(arrived(r, "f", 1, NV))
    rest = rest_of(1)
    for part in range(2):
        both = []
        for side in range(2):
            rows = slice(512 * side + 256 * part, 512 * side + 256 * part + 256)
            both.append(ahead[rows] + through(rows, slice(256, 512), second, rest))
        re = both[0][:, :128] + both[1][:, 128:]
        im = both[0][:, 128:] - both[1][:, :128]
        for q in range(NV):
            rows, cols = (slice(n * (q % 8), n * (q % 8) + n) for n in (16, 128))
            r["blocks"][q // 8, rows, cols] = jnp.concatenate(
                [re[8 * q : 8 * q + 8], im[8 * q : 8 * q + 8]], axis=0
            ).astype(bf16)
        picked = [
            dot_nt(r["hots"][n], r["blocks"][n]).reshape(16, 8, 128) for n in range(4)
        ]
        upper = lax.broadcasted_iota(jnp.int32, (16, 8, 128), 1) < 4
        chunks = []
        for n in (0, 2):
            one, two = picked[n], picked[n + 1]
            even = jnp.where(upper, one, pltpu.roll(two, 4, 1))
            odd = jnp.where(upper, pltpu.roll(one, 4, 1), two)
            chunks.append(jnp.stack([even, odd], axis=1).reshape(NV, 8, 128))
        r["sent_g"][part] = jnp.concatenate(chunks, axis=1).astype(bf16)
        launch(r, "g", part, "vis", NV, vis_me)

    down_hi, down_lo = staged("down_hi"), staged("down_lo")
    image_copy.wait_recv()
    fields = jnp.concatenate([extrap[0], extrap[1], r["got_rows"][...]], axis=0)
    fields = table_by(sides_hi[32:48, 0:24], sides_lo[32:48, 0:24], fields)
    stack = []
    for n in range(16):
        if n < 15:
            stack.append(fields[:, 256 * n : 256 * n + 384])
        else:
            stack.append(jnp.concatenate([fields[:, 3840:4096], fields[:, 0:128]], axis=1))
    found = by_table(jnp.concatenate(stack, axis=0), down_hi[...], down_lo[...])
    coeffs = r["coeffs_here"]
    for n in range(16):
        cols = slice(128 * n, 128 * n + 128)
        block = found[16 * n : 16 * n + 16]
        coeffs[0, :, cols] = coef[0, :, cols] + block[0:8, :128]
        coeffs[1, :, cols] = coef[1, :, cols] + block[0:8, 128:]
        coeffs[2, :, cols] = coef[2, :, cols] + block[8:16, :128]
        coeffs[3, :, cols] = coef[3, :, cols] + block[8:16, 128:]
    abs_total = jnp.sum(jnp.abs(found))
    out_coeffs = pltpu.make_async_copy(coeffs, r["coeffs"], r["sem_out"].at[1])
    out_coeffs.start()
    values = []
    for part in range(2):
        got_g = arrived(r, "g", part, NV)
        for low in range(8):
            first, second, third, fourth = (got_g[4 * low + g].astype(f32) for g in range(4))
            values.append((first + second) + (third + fourth))
    tiles = jnp.concatenate(swap_groups(values, 8), axis=0).astype(bf16)
    tiles = dot(r["reorder"][...], tiles).astype(bf16)
    tiles = dot(tiles, order[...]).reshape(NV, 8, 128).astype(bf16)
    products = jnp.stack([dot_nt(tiles[q], kernels[q]) for q in range(NV)])
    products = jnp.where(wide_lane // 64 == wide_row // 2, products, 0.0)
    products = products[:, :, 0:128] + products[:, :, 128:256]
    products = products + pltpu.roll(products, 64, 2)
    other = pltpu.roll(products, 96, 2)
    row = lax.broadcasted_iota(jnp.int32, (NV, 8, 128), 1)
    products = products + jnp.where(
        row % 2 == 0, -pltpu.roll(other, 7, 1), pltpu.roll(other, 1, 1)
    )
    predicted = products.reshape(256, 128)[:, 0:32]
    residual = live * (vis_state + predicted - vis_data)
    resid_square = jnp.sum(residual * residual)
    r["residual"][...] = residual.reshape(NV, 4, 2, 32)

    sent_t, sent_u = r["sent_t"], r["sent_u"]
    spot = lax.broadcasted_iota(jnp.int32, (1, 128), 1)
    sent_t[...] = jnp.where(
        spot == 0, abs_total, jnp.where(spot == 1, resid_square, data_square)
    )
    launch(r, "t", 0, "vis", NV, vis_me, same=True)
    sent_u[...] = jnp.sum(arrived(r, "t", 0, NV)[...], axis=0)
    launch(r, "u", 0, "band", NB, band_me, same=True)
    totals = jnp.sum(arrived(r, "u", 0, NB)[...], axis=0)
    r["totals"][...] = totals

    for copy in (coef_copy, image_copy):
        copy.wait_send()
    out_image.wait()
    out_coeffs.wait()
    for name in "abcdefgitu":
        for part in range(2 if name in "bcdefg" else 1):
            finish(r, name, part, NB if name in "deu" else NV, 0)
    for part in range(2):
        rest_drained(r, part, vis_me)


STAGED = ["kernels", "coef", "sky", "up_hi", "up_lo", "table_hi", "table_lo", "down_hi", "down_lo"]
INPUTS = STAGED + [
    "vis_state", "vis_data", "rows", "counts", "repeat", "lane_hi", "lane_lo",
    "twist_row", "twists", "order", "sides_hi", "sides_lo",
]
OUTPUTS = ["image", "coeffs", "residual", "totals"]
VIS_TILE = (2, NV, 2, 8, 128)
BAND_TILE = (2, NB, 2, 8, 512)
SCRATCH = dict(
    here_kernels=((NV, 256, 128), bf16),
    here_coef=((4, 8, 2048), f32),
    here_sky=((16, IMG), f32),
    here_up_hi=((512, 256), bf16),
    here_up_lo=((512, 256), bf16),
    here_table_hi=((1024, 512), bf16),
    here_table_lo=((1024, 512), bf16),
    here_down_hi=((384, 256), bf16),
    here_down_lo=((384, 256), bf16),
    sent_a=((1, NV, 8, 128), bf16), got_a=((1, NV, 8, 128), bf16),
    sent_i=((1, 128), f32), got_i=((1, NV, 1, 128), f32),
    sent_b=(VIS_TILE, bf16), got_b=(VIS_TILE, bf16),
    sent_c=(VIS_TILE, bf16), got_c=(VIS_TILE, bf16),
    sent_d=(BAND_TILE, bf16), got_d=(BAND_TILE, bf16),
    sent_e=(BAND_TILE, bf16), got_e=(BAND_TILE, bf16),
    sent_f=(VIS_TILE, bf16), got_f=(VIS_TILE, bf16),
    sent_l=((2, 8, 8, 128), bf16), got_l=((2, NV, 8, 128), bf16),
    sent_g=((2, NV, 16, 128), bf16), got_g=((2, NV, 16, 128), bf16),
    hots=((4, 128, 1024), bf16), blocks=((4, 128, 1024), bf16), reorder=((256, 256), bf16),
    sent_t=((1, 128), f32), got_t=((1, NV, 1, 128), f32),
    sent_u=((1, 128), f32), got_u=((1, NB, 1, 128), f32),
    weights=((NV, 8, 256), bf16), twist_col=((8, 2, 16, 128), f32), coef_rows=((16, 2048), f32),
    got_coef=((16, 2048), f32), got_rows=((8, IMG), f32),
    raw_here=((16, IMG), f32), extrap=((2, 8, IMG), f32), coeffs_here=((4, 8, 2048), f32),
    mid=((2, 32, 2, 8, 128), f32),
    **{"sem_" + n: 4 for n in list("abcdefgiltu") + ["coef", "rows", "out"]},
    sem_in=len(STAGED),
)


def step(inputs):
    anywhere = pl.BlockSpec(memory_space=pl.ANY)
    vmem = pl.BlockSpec(memory_space=pltpu.VMEM)
    scratch = []
    for what in SCRATCH.values():
        if isinstance(what, int):
            scratch.append(pltpu.SemaphoreType.DMA((what,)))
        else:
            scratch.append(pltpu.VMEM(*what))
    return pl.pallas_call(
        step_kernel,
        out_shape=(
            jax.ShapeDtypeStruct((16, IMG), f32),
            jax.ShapeDtypeStruct((4, 8, 2048), f32),
            jax.ShapeDtypeStruct((NV, 4, 2, 32), f32),
            jax.ShapeDtypeStruct((1, 128), f32),
        ),
        in_specs=[anywhere if name in STAGED else vmem for name in INPUTS],
        out_specs=(anywhere, anywhere, vmem, vmem),
        scratch_shapes=scratch,
        compiler_params=pltpu.CompilerParams(
            collective_id=0, has_side_effects=True, vmem_limit_bytes=56 * 2**20
        ),
    )(*[inputs[name] for name in INPUTS])


def closing_kernel(*refs):
    given, out, here, sems = refs[0:4], refs[4:7], refs[7:11], refs[11]
    copies = [pltpu.make_async_copy(given[n], here[n], sems.at[n]) for n in range(4)]
    for copy in copies:
        copy.start()

    def hand_out(n):
        copies[n] = pltpu.make_async_copy(here[n], out[n], sems.at[n])
        copies[n].start()

    spot = lax.broadcasted_iota(jnp.int32, (1, 128), 1)
    copies.pop().wait()
    copies[0].wait()
    hand_out(0)
    abs_total, resid_square, data_square = (
        jnp.sum(jnp.where(spot == n, here[3][...], 0.0), axis=1, keepdims=True)
        for n in range(3)
    )
    limit = jnp.broadcast_to(0.5 * abs_total / (IMG * IMG), (8, 2048))
    copies[1].wait()
    for part in range(4):
        here[1][part] = jnp.maximum(jnp.minimum(here[1][part], limit), -limit)
    hand_out(1)
    radius = 0.5 * jnp.sqrt(data_square + 1e-06)
    size = jnp.sqrt(resid_square + 1e-06)
    factor = 1.0 - jnp.minimum(1.0, radius / size)
    copies[2].wait()
    here[2][...] = here[2][...] * jnp.broadcast_to(factor.reshape(1, 1, 1, 1), (NV, 4, 2, 32))
    hand_out(2)
    for copy in copies:
        copy.wait()


def closing(results):
    anywhere = pl.BlockSpec(memory_space=pl.ANY)
    return pl.pallas_call(
        closing_kernel,
        out_shape=tuple(jax.ShapeDtypeStruct(x.shape, x.dtype) for x in results[:3]),
        in_specs=[anywhere] * 4,
        out_specs=(anywhere,) * 3,
        scratch_shapes=[pltpu.VMEM(x.shape, x.dtype) for x in results]
        + [pltpu.SemaphoreType.DMA((4,))],
    )(*results)


def local(sky_image, coef_dual, vis_dual, visibilities, kernel_blocks, tile_rows, tile_counts):
    names = (
        "table_hi", "table_lo", "lane_hi", "lane_lo",
        "up_hi", "up_lo", "down_hi", "down_lo", "sides_hi", "sides_lo",
    )
    inputs = dict(zip(names, dft512_tables() + dft128_tables() + wavelet_tables()))
    inputs.update(
        twist_row=row_twist(), twists=col_twist(), order=lane_order(), repeat=repeat_table()
    )
    inputs = {name: jnp.asarray(table) for name, table in inputs.items()}
    inputs.update(
        kernels=kernel_blocks.reshape(NV, 256, 128),
        coef=coef_dual,
        sky=sky_image,
        vis_state=vis_dual.reshape(NV, 4, 2, 32),
        vis_data=visibilities.reshape(NV, 4, 2, 32),
        rows=tile_rows.reshape(NV, 4).T,
        counts=tile_counts.reshape(1, NV),
    )
    image, coeffs, vis_new = closing(step(inputs))
    return (image, coeffs, vis_new.reshape(1, 1, NV, 4, 2, 32))


def solution(mesh):
    return jax.shard_map(
        local,
        mesh=mesh,
        in_specs=(
            P(("band", "vis"), None),
            P(None, ("band", "vis"), None),
            P("band", "vis", None, None, None, None),
            P("band", "vis", None, None, None, None),
            P("band", "vis", None, None, None, None, None),
            P("band", "vis", None, None),
            P("band", "vis", None),
        ),
        out_specs=(
            P(("band", "vis"), None),
            P(None, ("band", "vis"), None),
            P("band", "vis", None, None, None, None),
        ),
        check_vma=False,
    )
```

```python
import functools
import math

import jax
import jax.numpy as jnp
import numpy as np
from jax import lax
from jax.experimental import pallas as pl
from jax.experimental.pallas import tpu as pltpu
from jax.sharding import PartitionSpec as P

IMG = 4096
NB = 8
NV = 32
MESH_ID = pl.DeviceIdType.MESH
f32 = jnp.float32
bf16 = jnp.bfloat16

low_taps = (
    -0.010597401784997278,
    0.032883011666982945,
    0.030841381835986965,
    -0.18703481171888114,
    -0.02798376941698385,
    0.6308807679295904,
    0.7148465705525415,
    0.23037781330885523,
)
high_taps = tuple(((-1.0) ** offset * low_taps[7 - offset] for offset in range(8)))


def halves_of(table):
    high = table.astype(bf16)
    low = (table - high.astype(np.float64)).astype(bf16)
    return high, low


def dft512_tables():
    index = np.arange(512).reshape(32, 2, 8).transpose(1, 0, 2).reshape(512)
    angle = 2.0 * np.pi / 512 * (index[:, None] * index[None, :] % 512)
    return halves_of(np.concatenate([np.cos(angle), np.sin(angle)], axis=0))


def dft128_tables():
    index = np.arange(128)
    angle = 2.0 * np.pi / 128 * (index[:, None] * index[None, :] % 128)
    return halves_of(np.concatenate([np.cos(angle), np.sin(angle)], axis=1) / IMG)


def row_twist():
    angle = 2.0 * np.pi / IMG * (np.arange(32)[:, None] * np.arange(128)[None, :] % IMG)
    return np.stack([np.cos(angle), np.sin(angle)], axis=1).astype(np.float32)


def col_twist():
    low, row = np.arange(8)[None, :, None], np.arange(16)[None, None, :]
    angle = 2.0 * np.pi / IMG * (low * (16 * np.arange(NV)[:, None, None] + row))
    return np.stack([np.cos(angle), np.sin(angle)], axis=1).reshape(NV, 2, 128).astype(np.float32)


def repeat_table():
    return np.tile(np.eye(32), (1, 8)).astype(bf16)


def wavelet_tables():
    up = np.zeros((512, 256))
    down = np.zeros((384, 256))
    rows_up = np.zeros((2, 16, 32))
    rows_down = np.zeros((16, 24))
    for tap in range(8):
        for side, taps in ((0, low_taps), (1, high_taps)):
            for k in range(128):
                down[2 * k + tap, 128 * side + k] = taps[tap]
            for k in range(-128, 128):
                if 0 <= 2 * k + tap < 256:
                    up[256 * side + 128 + k, 2 * k + tap] = taps[tap]
            for k in range(8):
                rows_down[8 * side + k, 2 * k + tap] = taps[tap]
            for k in range(-3, 8):
                if 0 <= 2 * k + tap < 16:
                    for part in range(2):
                        spot = 8 * side + k if k >= 0 else 16 + 3 * (part + 2 * side) + k + 3
                        rows_up[part, 2 * k + tap, spot] = taps[tap]
    sides = np.zeros((48, 32))
    sides[0:32] = rows_up.reshape(32, 32)
    sides[32:48, 0:24] = rows_down
    return tuple(part for table in (up, down, sides) for part in halves_of(table))


def lane_order():
    place = np.zeros((128, 128), np.float32)
    for t in range(128):
        place[t // 64 * 64 + (t % 8) * 8 + t // 8 % 8, t] = 1.0
    return place.astype(bf16)


def times(pair, cosine, sine):
    re, im = pair
    if abs(sine) < 1e-12:
        if cosine > 0:
            return pair
        return (-re, None if im is None else -im)
    if abs(cosine) < 1e-12:
        if im is None:
            return (None, re if sine > 0 else -re)
        return (-im, re) if sine > 0 else (im, -re)
    cosine, sine = np.float32(cosine), np.float32(sine)
    if im is None:
        return (re * cosine, re * sine)
    return (re * cosine - im * sine, re * sine + im * cosine)


def plus(a, b):
    if a is None:
        return b
    return a if b is None else a + b


def minus(a, b):
    if b is None:
        return a
    return -b if a is None else a - b


def small_dft(values, sign):
    count = len(values)
    if count == 1:
        return values
    even = small_dft(values[0::2], sign)
    odd = small_dft(values[1::2], sign)
    out = [None] * count
    for k in range(count // 2):
        angle = sign * 2.0 * math.pi * k / count
        turned = times(odd[k], math.cos(angle), math.sin(angle))
        out[k] = (plus(even[k][0], turned[0]), plus(even[k][1], turned[1]))
        out[k + count // 2] = (minus(even[k][0], turned[0]), minus(even[k][1], turned[1]))
    return out


def swap_groups(arrays, width=16):
    arrays = list(arrays)
    axis = arrays[0].ndim - 1
    lane = lax.broadcasted_iota(jnp.int32, arrays[0].shape, axis)
    bit = 1
    while bit < len(arrays):
        shift = width * bit
        upper = (lane // shift) % 2 == 1
        for j in range(len(arrays)):
            other = j | bit
            if other == j:
                continue
            low, high = arrays[j], arrays[other]
            arrays[j] = jnp.where(upper, pltpu.roll(high, shift, axis), low)
            arrays[other] = jnp.where(upper, high, pltpu.roll(low, 128 - shift, axis))
        bit *= 2
    return arrays


def dot(a, b):
    return jnp.dot(a, b, preferred_element_type=f32)


def dot_nt(a, b):
    return lax.dot_general(a, b, (((1,), (1,)), ((), ())), preferred_element_type=f32)


def halves(value):
    high = value.astype(bf16)
    return high, (value - high.astype(f32)).astype(bf16)


def by_table(value, high, low):
    value_high, value_low = halves(value)
    return dot(value_high, high) + dot(value_low, high) + dot(value_high, low)


def table_by(high, low, value):
    value_high, value_low = halves(value)
    return dot(high, value_high) + dot(high, value_low) + dot(low, value_high)


def dropped(value):
    return value - value.astype(bf16).astype(f32)


def greet(vis_me, band_me, neighbours):
    barrier = pltpu.get_barrier_semaphore()

    def vis_signal(d, carry):
        pl.semaphore_signal(
            barrier, inc=1, device_id={"vis": vis_me ^ d}, device_id_type=MESH_ID
        )
        return carry

    def band_signal(d, carry):
        pl.semaphore_signal(
            barrier, inc=1, device_id={"band": band_me ^ d}, device_id_type=MESH_ID
        )
        return carry

    for neighbour in neighbours:
        pl.semaphore_signal(barrier, inc=1, device_id=neighbour, device_id_type=MESH_ID)
    lax.fori_loop(1, NV, vis_signal, 0)
    lax.fori_loop(1, NB, band_signal, 0)
    return barrier


def far_first(n, count):
    if count == NV:
        z, y = n // 8, n // 2 % 4
        return n % 2 + 2 * (z ^ z // 2) + 8 * (y ^ y // 2)
    x = n % 4
    return (x ^ x // 2) + n // 4 * 4


def launch(r, name, part, axis, count, me, same=False, shared=1):
    sent, landed, sems = r["sent_" + name], r["got_" + name].at[part], r["sem_" + name]
    if not same:
        sent = sent.at[part]

    def body(step, carry):
        peer = me ^ far_first(count - step, count)
        pltpu.make_async_remote_copy(
            src_ref=sent if same else sent.at[peer // shared],
            dst_ref=landed.at[me],
            send_sem=sems.at[2 * part],
            recv_sem=sems.at[2 * part + 1],
            device_id={axis: peer},
            device_id_type=MESH_ID,
        ).start()
        return carry

    lax.fori_loop(1, count, body, 0)
    landed[me] = sent[...] if same else sent[me // shared]


def rest_copy(r, part, low, me):
    return pltpu.make_async_remote_copy(
        src_ref=r["sent_l"].at[part, low],
        dst_ref=r["got_l"].at[part, me],
        send_sem=r["sem_l"].at[2 * part],
        recv_sem=r["sem_l"].at[2 * part + 1],
        device_id={"vis": 4 * low},
        device_id_type=MESH_ID,
    )


def launch_rest(r, part, me):
    for low in range(8):

        @pl.when(me != 4 * low)
        def _():
            rest_copy(r, part, low, me).start()

        @pl.when(me == 4 * low)
        def _():
            r["got_l"][part, me] = r["sent_l"][part, low]


def rest_arrived(r, part, me):
    @pl.when(me % 4 == 0)
    def _():
        finish(r, "l", part, NV, 1)


def rest_drained(r, part, me):
    finish(r, "l", part, 8, 0)

    @pl.when(me % 4 != 0)
    def _():
        finish(r, "l", part, 2, 0)


def to_neighbour(sent, landed, sems, neighbour):
    copy = pltpu.make_async_remote_copy(
        src_ref=sent,
        dst_ref=landed,
        send_sem=sems.at[0],
        recv_sem=sems.at[1],
        device_id=neighbour,
        device_id_type=MESH_ID,
    )
    copy.start()
    return copy


def finish(r, name, part, count, side):
    landed = r["got_" + name].at[part]
    landed = landed.at[pl.ds(0, count - 1)]
    pltpu.make_async_copy(landed, landed, r["sem_" + name].at[2 * part + side]).wait()


def arrived(r, name, part, count):
    finish(r, name, part, count, 1)
    return r["got_" + name].at[part]


def step_kernel(*refs):
    names = INPUTS + OUTPUTS + list(SCRATCH)
    r = dict(zip(names, refs))
    vis_me, band_me = lax.axis_index("vis"), lax.axis_index("band")
    me = band_me * NV + vis_me
    following = (me + 1) % (NB * NV)
    preceding = (me + NB * NV - 1) % (NB * NV)
    following = {"band": following // NV, "vis": following % NV}
    preceding = {"band": preceding // NV, "vis": preceding % NV}
    copies = {}
    for place, name in enumerate(STAGED):
        copies[name] = pltpu.make_async_copy(r[name], r["here_" + name], r["sem_in"].at[place])
        copies[name].start()

    def staged(name):
        if name in copies:
            copies.pop(name).wait()
        return r["here_" + name]

    barrier = greet(vis_me, band_me, (following, preceding))

    to_row = (
        lax.broadcasted_iota(jnp.int32, (256, 32), 0) // 8
        == lax.broadcasted_iota(jnp.int32, (256, 32), 1)
    ).astype(f32).astype(bf16)
    column = r["rows"][...]
    facts = jnp.concatenate(
        [
            (column % 32 * 16 + column // 32 - 256).astype(f32),
            r["counts"][...].astype(f32),
            jnp.zeros((123, 32), f32),
        ],
        axis=0,
    ).astype(bf16)
    eye = (
        lax.broadcasted_iota(jnp.int32, (32, 32), 0)
        == lax.broadcasted_iota(jnp.int32, (32, 32), 1)
    ).astype(f32).astype(bf16)
    facts = dot_nt(eye, facts)
    place = (column % 32 * 16 + column // 32 - 256).astype(f32)
    r["sent_i"][...] = jnp.concatenate([place[n : n + 1] for n in range(4)], axis=1)
    row, col = (lax.broadcasted_iota(jnp.int32, (256, 256), n) for n in range(2))
    source = row // 8 % 8 * 32 + row % 2 * 16 + row // 64 * 4 + row % 8 // 2
    r["reorder"][...] = (col == source).astype(f32).astype(bf16)
    source = col // 8 % 8 * 32 + col % 2 * 16 + col // 64 * 4 + col % 8 // 2
    backwards = (row == source).astype(f32).astype(bf16)
    r["blocks"][...] = jnp.zeros((4, 128, 1024), bf16)
    row_slot = lax.broadcasted_iota(jnp.int32, (256, 128), 0) % 8 // 2
    fact = lax.broadcasted_iota(jnp.int32, (256, 128), 1)

    def per_row(table, choice):
        wide = dot(to_row, table.astype(bf16))
        return jnp.sum(jnp.where(fact == choice, wide, 0.0), axis=1, keepdims=True)

    count = per_row(facts, 4)
    live = jnp.broadcast_to(count, (256, 32)) > (
        lax.broadcasted_iota(jnp.int32, (256, 32), 0) % 8 // 2
    ).astype(f32)
    live = jnp.where(live, 1.0, 0.0)
    vis_state = r["vis_state"][...].reshape(256, 32)
    vis_data = r["vis_data"][...].reshape(256, 32)
    data_square = jnp.sum(live * vis_data * vis_data)

    weights = dot((live * vis_state).astype(bf16), r["repeat"][...]).reshape(NV, 8, 256)
    wide_row = lax.broadcasted_iota(jnp.int32, (NV, 8, 256), 1)
    wide_lane = lax.broadcasted_iota(jnp.int32, (NV, 8, 256), 2)
    crossed = jnp.where(
        wide_row % 2 == 0, pltpu.roll(weights, 7, 1), -pltpu.roll(weights, 1, 1)
    )
    weights = jnp.where(wide_lane // 32 % 2 == 0, weights, crossed)
    r["weights"][...] = jnp.where(wide_lane // 64 == wide_row // 2, weights, 0.0).astype(bf16)
    twist_col = r["twist_col"]
    eye = (
        lax.broadcasted_iota(jnp.int32, (128, 128), 0)
        == lax.broadcasted_iota(jnp.int32, (128, 128), 1)
    )
    for c in range(2):
        one = jnp.broadcast_to(r["twists"][vis_me, c : c + 1, :], (128, 128))
        one = jnp.sum(jnp.where(eye, one, 0.0), axis=1, keepdims=True)
        twist_col[:, c] = jnp.broadcast_to(one, (128, 128)).reshape(8, 16, 128)

    order = r["order"]
    kernels = staged("kernels")
    contrib = jnp.concatenate(
        [dot(r["weights"][q], kernels[q]) for q in range(NV)], axis=0
    ).astype(bf16)
    contrib = dot(backwards, dot_nt(contrib, order[...]).astype(bf16))
    groups = swap_groups([contrib[16 * n : 16 * n + 16] for n in range(16)], 8)
    for part in range(2):
        for low in range(8):
            r["sent_b"][part, low] = groups[8 * part + low].astype(bf16)
    coef = staged("coef")
    for part in range(4):
        r["coef_rows"][3 * part : 3 * part + 3] = coef[part, 5:8, :]
    r["coef_rows"][12:16] = jnp.zeros((4, 2048), f32)
    r["got_l"][...] = jnp.zeros((2, NV, 8, 128), bf16)

    pl.semaphore_wait(barrier, NV + NB)
    launch(r, "i", 0, "vis", NV, vis_me, same=True)
    for part in range(2):
        launch(r, "b", part, "vis", NV, vis_me, shared=4)
    coef_copy = to_neighbour(r["coef_rows"], r["got_coef"], r["sem_coef"], following)
    positions = arrived(r, "i", 0, NV)[...].reshape(NV, 128)

    to_row = (
        lax.broadcasted_iota(jnp.int32, (128, 32), 0) // 4
        == lax.broadcasted_iota(jnp.int32, (128, 32), 1)
    ).astype(f32).astype(bf16)
    row, lane = (lax.broadcasted_iota(jnp.int32, (128, 128), n) for n in range(2))
    wide = jnp.where(lane // 32 == row % 4, dot(to_row, positions.astype(bf16)), 0.0)
    wide = wide + pltpu.roll(wide, 64, 1)
    wide = wide + pltpu.roll(wide, 32, 1)
    here = (lane + 128 * (vis_me % 4) - 256).astype(f32)
    for q in range(NV):
        hot = jnp.broadcast_to(wide[:, q : q + 1], (128, 128)) == here
        cols = slice(128 * (q % 8), 128 * (q % 8) + 128)
        r["hots"][q // 8, :, cols] = hot.astype(f32).astype(bf16)

    sky = staged("sky")
    sides_hi, sides_lo = r["sides_hi"], r["sides_lo"]
    up_hi, up_lo = staged("up_hi"), staged("up_lo")
    coef_copy.wait_recv()
    rows_up = []
    for part in range(2):
        rows = slice(16 * part, 16 * part + 16)
        stack = jnp.concatenate([coef[part], coef[part + 2], r["got_coef"][...]], axis=0)
        rows_up.append(table_by(sides_hi[rows, :], sides_lo[rows, :], stack))
    stack = []
    for n in range(16):
        parts = []
        for field in rows_up:
            for block in ((n + 15) % 16, n):
                parts.append(field[:, 128 * block : 128 * block + 128])
        stack.append(jnp.concatenate(parts, axis=1))
    smooth = by_table(jnp.concatenate(stack, axis=0), up_hi[...], up_lo[...])
    raw = r["raw_here"]
    for n in range(16):
        cols = slice(256 * n, 256 * n + 256)
        raw[:, cols] = sky[:, cols] - smooth[16 * n : 16 * n + 16]

    table_hi, table_lo = staged("table_hi"), staged("table_lo")
    upper = lax.broadcasted_iota(jnp.int32, (16, 8, 128), 1) < 4

    def spread_of(landed):
        return jnp.concatenate(
            [landed[:, 0].reshape(256, 128), landed[:, 1].reshape(256, 128)], axis=1
        )

    def gridded(landed):
        reals, imags = [], []
        for n in (0, 2):
            both = landed[:, 4 * n : 4 * n + 8, :].astype(f32).reshape(16, 2, 8, 128)
            even, odd = both[:, 0], both[:, 1]
            for slots in (
                jnp.where(upper, even, pltpu.roll(odd, 4, 1)),
                jnp.where(upper, pltpu.roll(even, 4, 1), odd),
            ):
                total = lax.dot_general(
                    slots.reshape(128, 128).astype(bf16),
                    r["hots"][len(reals) // 8],
                    (((0,), (0,)), ((), ())),
                    preferred_element_type=f32,
                )
                for q in range(8):
                    cols = slice(128 * q, 128 * q + 128)
                    reals.append(total[16 * q : 16 * q + 8, cols])
                    imags.append(total[16 * q + 8 : 16 * q + 16, cols])
        reals, imags = jnp.concatenate(reals, axis=0), jnp.concatenate(imags, axis=0)
        return jnp.concatenate([reals, imags], axis=1).astype(bf16)

    first = gridded(arrived(r, "b", 0, NV))
    ahead = dot(table_hi[:, 0:256], first) + dot(table_lo[:, 0:256], first)
    second = gridded(arrived(r, "b", 1, NV))
    for part in range(2):
        both = []
        for side in range(2):
            rows = slice(512 * side + 256 * part, 512 * side + 256 * part + 256)
            both.append(
                ahead[rows] + dot(table_hi[rows, 256:512], second)
                + dot(table_lo[rows, 256:512], second)
            )
        re = both[0][:, :128] - both[1][:, 128:]
        im = both[1][:, :128] + both[0][:, 128:]
        r["sent_c"][part, :, 0] = re.reshape(NV, 8, 128).astype(bf16)
        r["sent_c"][part, :, 1] = im.reshape(NV, 8, 128).astype(bf16)
        launch(r, "c", part, "vis", NV, vis_me)

    sent_d = r["sent_d"]
    for part in range(2):
        got_c = arrived(r, "c", part, NV)
        rows = slice(8 * part, 8 * part + 8)
        for g in range(4):
            values = []
            for low in range(8):
                re = got_c[low * 4 + g, 0].astype(f32)
                im = got_c[low * 4 + g, 1].astype(f32)
                cosine, sine = twist_col[low, 0, rows], twist_col[low, 1, rows]
                values.append((re * cosine - im * sine, re * sine + im * cosine))
            values = small_dft(values, 1.0)
            for b in range(NB):
                for c in range(2):
                    sent_d[part, b, c, :, 128 * g : 128 * g + 128] = values[b][c].astype(
                        sent_d.dtype
                    )
        launch(r, "d", part, "band", NB, band_me)

    mid, twist_row, extrap, sent_e = r["mid"], r["twist_row"], r["extrap"], r["sent_e"]

    first_lane = lax.broadcasted_iota(jnp.int32, (8, 128), 1) == 0
    second_lane = lax.broadcasted_iota(jnp.int32, (8, 128), 1) == 1

    def lane_product(part):
        return by_table(
            mid[part].reshape(512, 128), r["lane_hi"][...], r["lane_lo"][...]
        ).reshape(32, 2, 8, 256)

    for part in range(2):
        rows = slice(8 * part, 8 * part + 8)
        got_d = arrived(r, "d", part, NB)
        for g in range(4):
            for c in range(2):
                parts = swap_groups(
                    [got_d[b, c, :, 128 * g : 128 * g + 128].astype(f32) for b in range(NB)]
                )
                for a in range(8):
                    mid[part, g * 8 + a, c] = parts[a]
        lanes = lane_product(part)
        values = []
        for a in range(32):
            re = lanes[a, 0, :, :128] - lanes[a, 1, :, 128:]
            im = lanes[a, 0, :, 128:] + lanes[a, 1, :, :128]
            cosine, sine = twist_row[a, 0:1], twist_row[a, 1:2]
            values.append((re * cosine - im * sine, re * sine + im * cosine))
        values = small_dft(values, 1.0)
        for n in range(32):
            cols = slice(128 * n, 128 * n + 128)
            now = jnp.maximum(raw[rows, cols] - values[n][0], 0.0)
            raw[rows, cols] = now
            extrap[part, :, cols] = 2.0 * now - sky[rows, cols]
        values = [(extrap[part, :, 128 * n : 128 * n + 128], None) for n in range(32)]
        values = small_dft(values, -1.0)
        for a in range(32):
            re, im = values[a]
            cosine, sine = twist_row[a, 0:1], twist_row[a, 1:2]
            if im is None:
                mid[part, a, 0] = re * cosine
                mid[part, a, 1] = -re * sine
            else:
                mid[part, a, 0] = re * cosine + im * sine
                mid[part, a, 1] = im * cosine - re * sine
        lanes = lane_product(part)
        for g in range(4):
            cols = slice(128 * g, 128 * g + 128)
            reals, imags = [], []
            for a in range(8):
                re, im = lanes[g * 8 + a, 0], lanes[g * 8 + a, 1]
                reals.append(re[:, :128] + im[:, 128:])
                imags.append(im[:, :128] - re[:, 128:])
            reals, imags = swap_groups(reals), swap_groups(imags)
            if g == 0:
                imags[0] = jnp.where(first_lane, dropped(reals[0]), imags[0])
            for b in range(NB):
                sent_e[part, b, 0, :, cols] = reals[b].astype(bf16)
                sent_e[part, b, 1, :, cols] = imags[b].astype(bf16)
        launch(r, "e", part, "band", NB, band_me)
    out_image = pltpu.make_async_copy(raw, r["image"], r["sem_out"].at[0])
    out_image.start()

    sent_f = r["sent_f"]
    column_zero = jnp.where(first_lane, jnp.where(band_me == 0, 1.0, 0.0), 0.0)
    for part in range(2):
        got_e = arrived(r, "e", part, NB)
        rows = slice(8 * part, 8 * part + 8)
        for g in range(4):
            values = []
            for b in range(NB):
                re, im = (
                    got_e[b, c, :, 128 * g : 128 * g + 128].astype(f32) for c in range(2)
                )
                if g == 0:
                    re, im = re + im * column_zero, im * (1.0 - column_zero)
                values.append((re, im))
            values = small_dft(values, -1.0)
            for low in range(8):
                re, im = values[low]
                cosine, sine = twist_col[low, 0, rows], twist_col[low, 1, rows]
                re, im = re * cosine + im * sine, im * cosine - re * sine
                sent_f[part, low * 4 + g, 0] = re.astype(bf16)
                sent_f[part, low * 4 + g, 1] = im.astype(bf16)
                if g == 0:
                    rest = jnp.where(first_lane, dropped(re), 0.0)
                    rest = jnp.where(second_lane, pltpu.roll(dropped(im), 1, 1), rest)
                    r["sent_l"][part, low] = rest.astype(bf16)
        launch(r, "f", part, "vis", NV, vis_me)
        launch_rest(r, part, vis_me)
    image_copy = to_neighbour(extrap.at[0], r["got_rows"], r["sem_rows"], preceding)

    def through(rows, cols, spread, rest):
        wide = dot(table_hi[rows, cols], spread) + dot(table_lo[rows, cols], spread)
        rest = dot(table_hi[rows, cols], rest)
        one = lax.broadcasted_iota(jnp.int32, rest.shape, 1) == 0
        return wide + jnp.concatenate(
            [jnp.where(one, rest, 0.0), jnp.where(one, pltpu.roll(rest, 127, 1), 0.0)], axis=1
        )

    def rest_of(part):
        rest_arrived(r, part, vis_me)
        return r["got_l"][part].astype(f32).reshape(256, 128).astype(bf16)

    first = spread_of(arrived(r, "f", 0, NV))
    ahead = through(slice(0, 1024), slice(0, 256), first, rest_of(0))
    second = spread_of(arrived(r, "f", 1, NV))
    rest = rest_of(1)
    for part in range(2):
        both = []
        for side in range(2):
            rows = slice(512 * side + 256 * part, 512 * side + 256 * part + 256)
            both.append(ahead[rows] + through(rows, slice(256, 512), second, rest))
        re = both[0][:, :128] + both[1][:, 128:]
        im = both[0][:, 128:] - both[1][:, :128]
        for q in range(NV):
            rows, cols = (slice(n * (q % 8), n * (q % 8) + n) for n in (16, 128))
            r["blocks"][q // 8, rows, cols] = jnp.concatenate(
                [re[8 * q : 8 * q + 8], im[8 * q : 8 * q + 8]], axis=0
            ).astype(bf16)
        picked = [
            dot_nt(r["hots"][n], r["blocks"][n]).reshape(16, 8, 128) for n in range(4)
        ]
        chunks = []
        for n in (0, 2):
            one, two = picked[n], picked[n + 1]
            even = jnp.where(upper, one, pltpu.roll(two, 4, 1))
            odd = jnp.where(upper, pltpu.roll(one, 4, 1), two)
            chunks.append(jnp.stack([even, odd], axis=1).reshape(NV, 8, 128))
        r["sent_g"][part] = jnp.concatenate(chunks, axis=1).astype(bf16)
        launch(r, "g", part, "vis", NV, vis_me)

    down_hi, down_lo = staged("down_hi"), staged("down_lo")
    image_copy.wait_recv()
    fields = jnp.concatenate([extrap[0], extrap[1], r["got_rows"][...]], axis=0)
    fields = table_by(sides_hi[32:48, 0:24], sides_lo[32:48, 0:24], fields)
    stack = []
    for n in range(16):
        if n < 15:
            stack.append(fields[:, 256 * n : 256 * n + 384])
        else:
            stack.append(jnp.concatenate([fields[:, 3840:4096], fields[:, 0:128]], axis=1))
    found = by_table(jnp.concatenate(stack, axis=0), down_hi[...], down_lo[...])
    coeffs = r["coeffs_here"]
    for n in range(16):
        cols = slice(128 * n, 128 * n + 128)
        block = found[16 * n : 16 * n + 16]
        coeffs[0, :, cols] = coef[0, :, cols] + block[0:8, :128]
        coeffs[1, :, cols] = coef[1, :, cols] + block[0:8, 128:]
        coeffs[2, :, cols] = coef[2, :, cols] + block[8:16, :128]
        coeffs[3, :, cols] = coef[3, :, cols] + block[8:16, 128:]
    abs_total = jnp.sum(jnp.abs(found))
    out_coeffs = pltpu.make_async_copy(coeffs, r["coeffs"], r["sem_out"].at[1])
    out_coeffs.start()
    values = []
    for part in range(2):
        got_g = arrived(r, "g", part, NV)
        for low in range(8):
            first, second, third, fourth = (got_g[4 * low + g].astype(f32) for g in range(4))
            values.append((first + second) + (third + fourth))
    tiles = jnp.concatenate(swap_groups(values, 8), axis=0).astype(bf16)
    tiles = dot(r["reorder"][...], tiles).astype(bf16)
    tiles = dot(tiles, order[...]).reshape(NV, 8, 128).astype(bf16)
    products = jnp.stack([dot_nt(tiles[q], kernels[q]) for q in range(NV)])
    products = jnp.where(wide_lane // 64 == wide_row // 2, products, 0.0)
    products = products[:, :, 0:128] + products[:, :, 128:256]
    products = products + pltpu.roll(products, 64, 2)
    other = pltpu.roll(products, 96, 2)
    row = lax.broadcasted_iota(jnp.int32, (NV, 8, 128), 1)
    products = products + jnp.where(
        row % 2 == 0, -pltpu.roll(other, 7, 1), pltpu.roll(other, 1, 1)
    )
    predicted = products.reshape(256, 128)[:, 0:32]
    residual = live * (vis_state + predicted - vis_data)
    resid_square = jnp.sum(residual * residual)
    r["residual"][...] = residual.reshape(NV, 4, 2, 32)

    sent_t, sent_u = r["sent_t"], r["sent_u"]
    spot = lax.broadcasted_iota(jnp.int32, (1, 128), 1)
    sent_t[...] = jnp.where(
        spot == 0, abs_total, jnp.where(spot == 1, resid_square, data_square)
    )
    launch(r, "t", 0, "vis", NV, vis_me, same=True)
    sent_u[...] = jnp.sum(arrived(r, "t", 0, NV)[...], axis=0)
    launch(r, "u", 0, "band", NB, band_me, same=True)
    totals = jnp.sum(arrived(r, "u", 0, NB)[...], axis=0)
    r["totals"][...] = totals

    for copy in (coef_copy, image_copy):
        copy.wait_send()
    out_image.wait()
    out_coeffs.wait()
    for name in "bcdefgitu":
        for part in range(2 if name in "bcdefg" else 1):
            finish(r, name, part, NB if name in "deu" else NV, 0)
    for part in range(2):
        rest_drained(r, part, vis_me)


STAGED = ["kernels", "coef", "sky", "up_hi", "up_lo", "table_hi", "table_lo", "down_hi", "down_lo"]
INPUTS = STAGED + [
    "vis_state", "vis_data", "rows", "counts", "repeat", "lane_hi", "lane_lo",
    "twist_row", "twists", "order", "sides_hi", "sides_lo",
]
OUTPUTS = ["image", "coeffs", "residual", "totals"]
VIS_TILE = (2, NV, 2, 8, 128)
BAND_TILE = (2, NB, 2, 8, 512)
SCRATCH = dict(
    here_kernels=((NV, 256, 128), bf16),
    here_coef=((4, 8, 2048), f32),
    here_sky=((16, IMG), f32),
    here_up_hi=((512, 256), bf16),
    here_up_lo=((512, 256), bf16),
    here_table_hi=((1024, 512), bf16),
    here_table_lo=((1024, 512), bf16),
    here_down_hi=((384, 256), bf16),
    here_down_lo=((384, 256), bf16),
    sent_i=((1, 128), f32), got_i=((1, NV, 1, 128), f32),
    sent_b=((2, 8, 16, 128), bf16), got_b=((2, NV, 16, 128), bf16),
    sent_c=(VIS_TILE, bf16), got_c=(VIS_TILE, bf16),
    sent_d=(BAND_TILE, bf16), got_d=(BAND_TILE, bf16),
    sent_e=(BAND_TILE, bf16), got_e=(BAND_TILE, bf16),
    sent_f=(VIS_TILE, bf16), got_f=(VIS_TILE, bf16),
    sent_l=((2, 8, 8, 128), bf16), got_l=((2, NV, 8, 128), bf16),
    sent_g=((2, NV, 16, 128), bf16), got_g=((2, NV, 16, 128), bf16),
    hots=((4, 128, 1024), bf16), blocks=((4, 128, 1024), bf16), reorder=((256, 256), bf16),
    sent_t=((1, 128), f32), got_t=((1, NV, 1, 128), f32),
    sent_u=((1, 128), f32), got_u=((1, NB, 1, 128), f32),
    weights=((NV, 8, 256), bf16), twist_col=((8, 2, 16, 128), f32), coef_rows=((16, 2048), f32),
    got_coef=((16, 2048), f32), got_rows=((8, IMG), f32),
    raw_here=((16, IMG), f32), extrap=((2, 8, IMG), f32), coeffs_here=((4, 8, 2048), f32),
    mid=((2, 32, 2, 8, 128), f32),
    **{"sem_" + n: 4 for n in list("bcdefgiltu") + ["coef", "rows", "out"]},
    sem_in=len(STAGED),
)


def step(inputs):
    anywhere = pl.BlockSpec(memory_space=pl.ANY)
    vmem = pl.BlockSpec(memory_space=pltpu.VMEM)
    scratch = []
    for what in SCRATCH.values():
        if isinstance(what, int):
            scratch.append(pltpu.SemaphoreType.DMA((what,)))
        else:
            scratch.append(pltpu.VMEM(*what))
    return pl.pallas_call(
        step_kernel,
        out_shape=(
            jax.ShapeDtypeStruct((16, IMG), f32),
            jax.ShapeDtypeStruct((4, 8, 2048), f32),
            jax.ShapeDtypeStruct((NV, 4, 2, 32), f32),
            jax.ShapeDtypeStruct((1, 128), f32),
        ),
        in_specs=[anywhere if name in STAGED else vmem for name in INPUTS],
        out_specs=(anywhere, anywhere, vmem, vmem),
        scratch_shapes=scratch,
        compiler_params=pltpu.CompilerParams(
            collective_id=0, has_side_effects=True, vmem_limit_bytes=56 * 2**20
        ),
    )(*[inputs[name] for name in INPUTS])


def closing_kernel(*refs):
    given, out, here, sems = refs[0:4], refs[4:7], refs[7:11], refs[11]
    copies = [pltpu.make_async_copy(given[n], here[n], sems.at[n]) for n in range(4)]
    for copy in copies:
        copy.start()

    def hand_out(n):
        copies[n] = pltpu.make_async_copy(here[n], out[n], sems.at[n])
        copies[n].start()

    spot = lax.broadcasted_iota(jnp.int32, (1, 128), 1)
    copies.pop().wait()
    copies[0].wait()
    hand_out(0)
    abs_total, resid_square, data_square = (
        jnp.sum(jnp.where(spot == n, here[3][...], 0.0), axis=1, keepdims=True)
        for n in range(3)
    )
    limit = jnp.broadcast_to(0.5 * abs_total / (IMG * IMG), (8, 2048))
    copies[1].wait()
    for part in range(4):
        here[1][part] = jnp.maximum(jnp.minimum(here[1][part], limit), -limit)
    hand_out(1)
    radius = 0.5 * jnp.sqrt(data_square + 1e-06)
    size = jnp.sqrt(resid_square + 1e-06)
    factor = 1.0 - jnp.minimum(1.0, radius / size)
    copies[2].wait()
    here[2][...] = here[2][...] * jnp.broadcast_to(factor.reshape(1, 1, 1, 1), (NV, 4, 2, 32))
    hand_out(2)
    for copy in copies:
        copy.wait()


def closing(results):
    anywhere = pl.BlockSpec(memory_space=pl.ANY)
    return pl.pallas_call(
        closing_kernel,
        out_shape=tuple(jax.ShapeDtypeStruct(x.shape, x.dtype) for x in results[:3]),
        in_specs=[anywhere] * 4,
        out_specs=(anywhere,) * 3,
        scratch_shapes=[pltpu.VMEM(x.shape, x.dtype) for x in results]
        + [pltpu.SemaphoreType.DMA((4,))],
    )(*results)


def local(sky_image, coef_dual, vis_dual, visibilities, kernel_blocks, tile_rows, tile_counts):
    names = (
        "table_hi", "table_lo", "lane_hi", "lane_lo",
        "up_hi", "up_lo", "down_hi", "down_lo", "sides_hi", "sides_lo",
    )
    inputs = dict(zip(names, dft512_tables() + dft128_tables() + wavelet_tables()))
    inputs.update(
        twist_row=row_twist(), twists=col_twist(), order=lane_order(), repeat=repeat_table()
    )
    inputs = {name: jnp.asarray(table) for name, table in inputs.items()}
    inputs.update(
        kernels=kernel_blocks.reshape(NV, 256, 128),
        coef=coef_dual,
        sky=sky_image,
        vis_state=vis_dual.reshape(NV, 4, 2, 32),
        vis_data=visibilities.reshape(NV, 4, 2, 32),
        rows=tile_rows.reshape(NV, 4).T,
        counts=tile_counts.reshape(1, NV),
    )
    image, coeffs, vis_new = closing(step(inputs))
    return (image, coeffs, vis_new.reshape(1, 1, NV, 4, 2, 32))


def solution(mesh):
    return jax.shard_map(
        local,
        mesh=mesh,
        in_specs=(
            P(("band", "vis"), None),
            P(None, ("band", "vis"), None),
            P("band", "vis", None, None, None, None),
            P("band", "vis", None, None, None, None),
            P("band", "vis", None, None, None, None, None),
            P("band", "vis", None, None),
            P("band", "vis", None),
        ),
        out_specs=(
            P(("band", "vis"), None),
            P(None, ("band", "vis"), None),
            P("band", "vis", None, None, None, None),
        ),
        check_vma=False,
    )
```
